32 devices in a mesh: graph: 32 (over z, y, x, core).
Axes of the slice: x: 2, y: 2, z: 4, core: 2. Of those that a mesh axis runs over, the one named last changes fastest.
Arguments:
- node_feats: bfloat16 [65536, 500], P('graph')
- w_one: float32 [500, 256], replicated
- w_two: float32 [256, 7], replicated
- send_idx: int32 [64, 1024], P('graph')
- edge_src: int32 [262144], P('graph')
- edge_dst: int32 [262144], P('graph')
- edge_w: float32 [262144], P('graph')
- labels: int32 [65536], P('graph')
- label_mask: int32 [65536], P('graph')
Outputs:
- output 1: float32 [], replicated
- output 2: float32 [500, 256], replicated
- output 3: float32 [256, 7], replicated
All inputs are finite; a program needn't handle non-finite values.
Results may differ from the reference program's by a relative error of at most 0.001.
Values are sent between devices in bfloat16 or wider.
A program may use at most 1 GiB of HBM per device.

```python
import jax
import jax.numpy as jnp
from jax import lax

GRAPH = 32
N_LOC = 2048
HALO = 1024
EDGES = 8192
F_IN = 500
F_HID = 256
CLASSES = 7


def draw_structure(key):
    sub_keys = jax.random.split(key, 9)
    halo_pct = jax.random.randint(sub_keys[0], (GRAPH, 1), 5, 21, jnp.int32)
    pick_draw = jax.random.randint(sub_keys[1], (GRAPH, EDGES), 0, 100, jnp.int32)
    own_src = jax.random.randint(sub_keys[2], (GRAPH, EDGES), 0, N_LOC, jnp.int32)
    halo_src = jax.random.randint(sub_keys[3], (GRAPH, EDGES), N_LOC, N_LOC + 2 * HALO, jnp.int32)
    edge_src = jnp.where(pick_draw < halo_pct, halo_src, own_src)
    edge_dst = jax.random.randint(sub_keys[4], (GRAPH, EDGES), 0, N_LOC, jnp.int32)
    live_count = jax.random.randint(sub_keys[5], (GRAPH, 1), EDGES // 4, EDGES + 1, jnp.int32)
    is_live = jnp.arange(EDGES)[None, :] < live_count
    send_idx = jax.random.randint(sub_keys[6], (GRAPH * 2, HALO), 0, N_LOC, jnp.int32)
    labels = jax.random.randint(sub_keys[7], (GRAPH * N_LOC,), 0, CLASSES, jnp.int32)
    label_mask = jax.random.randint(sub_keys[8], (GRAPH * N_LOC,), 0, 2, jnp.int32)
    return edge_src, edge_dst, is_live, send_idx, labels, label_mask


def normalise(raw_weight, edge_dst):
    weight_sum = jax.vmap(lambda w_g, dst_g: jax.ops.segment_sum(w_g, dst_g, num_segments=N_LOC))(raw_weight, edge_dst)
    node_sum = jnp.take_along_axis(weight_sum, edge_dst, axis=1)
    return raw_weight / jnp.maximum(node_sum, 1e-6)


def setup_inputs(seed: int = 0) -> dict:
    key_list = jax.random.split(jax.random.key(seed), 5)
    edge_src, edge_dst, is_live, send_idx, labels, label_mask = draw_structure(key_list[0])
    deg_gain = EDGES / N_LOC
    node_feats = jax.random.normal(key_list[1], (GRAPH * N_LOC, F_IN), jnp.float32)
    w_one = jax.random.normal(key_list[2], (F_IN, F_HID), jnp.float32) * (deg_gain / F_IN) ** 0.5
    w_two = jax.random.normal(key_list[3], (F_HID, CLASSES), jnp.float32) * (deg_gain / F_HID) ** 0.5
    raw_weight = jax.random.uniform(key_list[4], (GRAPH, EDGES), jnp.float32, 0.5, 1.5) * is_live
    edge_w = normalise(raw_weight, edge_dst)
    return {"node_feats": node_feats.astype(jnp.bfloat16), "w_one": w_one, "w_two": w_two, "send_idx": send_idx, "edge_src": edge_src.reshape(-1), "edge_dst": edge_dst.reshape(-1), "edge_w": edge_w.reshape(-1), "labels": labels, "label_mask": label_mask}


def halo_extend(node_table, send_rows):
    pick_rows = jax.vmap(lambda table_g, idx_g: table_g[idx_g])
    from_prev = pick_rows(jnp.roll(node_table, 1, axis=0), jnp.roll(send_rows[:, 1], 1, axis=0))
    from_next = pick_rows(jnp.roll(node_table, -1, axis=0), jnp.roll(send_rows[:, 0], -1, axis=0))
    return jnp.concatenate([node_table, from_prev, from_next], axis=1)


def aggregate(ext_table, src_dev, dst_dev, w_dev):
    def one_device(args_g):
        ext_g, src_g, dst_g, w_g = args_g
        return jax.ops.segment_sum(w_g[:, None] * ext_g[src_g].astype(jnp.float32), dst_g, num_segments=N_LOC)
    return lax.map(one_device, (ext_table, src_dev, dst_dev, w_dev))


def scatter_back(grad_rows, send_rows, src_dev, dst_dev, w_dev):
    def one_device(args_g):
        grad_g, src_g, dst_g, w_g = args_g
        return jax.ops.segment_sum(w_g[:, None] * grad_g[dst_g], src_g, num_segments=N_LOC + 2 * HALO)
    ext_grad = lax.map(one_device, (grad_rows, src_dev, dst_dev, w_dev))
    back_prev = jnp.roll(ext_grad[:, N_LOC:N_LOC + HALO], -1, axis=0)
    back_next = jnp.roll(ext_grad[:, N_LOC + HALO:], 1, axis=0)
    row_ids = jnp.concatenate([send_rows[:, 1], send_rows[:, 0]], axis=1)
    ret_vals = jnp.concatenate([back_prev, back_next], axis=1)
    returned = jax.vmap(lambda vals_g, ids_g: jax.ops.segment_sum(vals_g, ids_g, num_segments=N_LOC))(ret_vals, row_ids)
    return ext_grad[:, :N_LOC] + returned


def reference(node_feats, w_one, w_two, send_idx, edge_src, edge_dst, edge_w, labels, label_mask):
    send_rows = send_idx.reshape(GRAPH, 2, HALO)
    src_dev = edge_src.reshape(GRAPH, EDGES)
    dst_dev = edge_dst.reshape(GRAPH, EDGES)
    w_dev = edge_w.reshape(GRAPH, EDGES)
    w_one_b = w_one.astype(jnp.bfloat16)
    w_two_b = w_two.astype(jnp.bfloat16)
    tab_one = jnp.dot(node_feats, w_one_b, preferred_element_type=jnp.float32).astype(jnp.bfloat16)
    pre_one = aggregate(halo_extend(tab_one.reshape(GRAPH, N_LOC, F_HID), send_rows), src_dev, dst_dev, w_dev).reshape(GRAPH * N_LOC, F_HID)
    hidden = jnp.maximum(pre_one, 0.0).astype(jnp.bfloat16)
    tab_two = jnp.dot(hidden, w_two_b, preferred_element_type=jnp.float32).astype(jnp.bfloat16)
    logits = aggregate(halo_extend(tab_two.reshape(GRAPH, N_LOC, CLASSES), send_rows), src_dev, dst_dev, w_dev).reshape(GRAPH * N_LOC, CLASSES)
    mask_f = label_mask.astype(jnp.float32)
    label_count = jnp.maximum(jnp.sum(mask_f), 1.0)
    log_norm = jax.nn.logsumexp(logits, axis=1)
    one_hot = (labels[:, None] == jnp.arange(CLASSES)[None, :]).astype(jnp.float32)
    picked = jnp.sum(logits * one_hot, axis=1)
    mean_loss = jnp.sum(mask_f * (log_norm - picked)) / label_count
    d_logits = (jnp.exp(logits - log_norm[:, None]) - one_hot) * (mask_f / label_count)[:, None]
    d_tab_two = scatter_back(d_logits.reshape(GRAPH, N_LOC, CLASSES), send_rows, src_dev, dst_dev, w_dev).reshape(GRAPH * N_LOC, CLASSES).astype(jnp.bfloat16)
    grad_two = jnp.dot(hidden.T, d_tab_two, preferred_element_type=jnp.float32)
    d_hidden = jnp.dot(d_tab_two, w_two_b.T, preferred_element_type=jnp.float32)
    d_pre = jnp.where(pre_one > 0.0, d_hidden, 0.0)
    d_tab_one = scatter_back(d_pre.reshape(GRAPH, N_LOC, F_HID), send_rows, src_dev, dst_dev, w_dev).reshape(GRAPH * N_LOC, F_HID).astype(jnp.bfloat16)
    grad_one = jnp.dot(node_feats.T, d_tab_one, preferred_element_type=jnp.float32)
    return mean_loss, grad_one, grad_two
```

```python
import functools

import jax
import jax.numpy as jnp
from jax import lax
from jax.experimental import pallas as pl
from jax.experimental.pallas import tpu as pltpu
from jax.sharding import PartitionSpec as P

GRAPH_AXIS = "graph"
MESH = pl.DeviceIdType.MESH
LANES = 128
CLASS_ROWS = 8
VMEM_BYTES = 60 * 2**20
F32 = jnp.float32
BF16 = jnp.bfloat16
NT = (((1,), (1,)), ((), ()))


def vmem():
    return pl.BlockSpec(memory_space=pltpu.VMEM)


def smem():
    return pl.BlockSpec(memory_space=pltpu.SMEM)


def flip(me, bit):
    return me + bit * (1 - 2 * ((me // bit) % 2))


def meet(partners):
    barrier = pltpu.get_barrier_semaphore()
    for dev in partners:
        pl.semaphore_signal(barrier, inc=1, device_id=(dev,), device_id_type=MESH)
    pl.semaphore_wait(barrier, len(partners))


def remote(src, dst, sems, slot, dev):
    return pltpu.make_async_remote_copy(
        src_ref=src, dst_ref=dst, send_sem=sems.at[0, slot], recv_sem=sems.at[1, slot],
        device_id=(dev,), device_id_type=MESH)


def three_pieces(val):
    top = val.astype(BF16).astype(F32)
    rest = val - top
    mid = rest.astype(BF16).astype(F32)
    return top, mid, rest - mid


def k1_body(num_dev, bits, x_ref, w_ref, send_ref, mask_ref, own_ref, halo_ref, cnt_ref,
            stage, cnt_send, cnt_recv, sems, cnt_sems):
    me = lax.axis_index(GRAPH_AXIS)
    nxt, prv = (me + 1) % num_dev, (me + num_dev - 1) % num_dev
    partners = [flip(me, b) for b in bits]
    meet([nxt, prv] + partners)
    rows = own_ref.shape[0]
    halo = send_ref.shape[1]
    own_ref[...] = jnp.dot(x_ref[...], w_ref[...].astype(BF16), preferred_element_type=F32).astype(BF16)

    blocks = halo // LANES
    ids = jnp.concatenate([send_ref[r:r + 1, b * LANES:(b + 1) * LANES] for r in range(2) for b in range(blocks)], axis=0)
    ids_col = jnp.transpose(ids)
    node = lax.broadcasted_iota(jnp.int32, (LANES, rows), 1)
    copies = []
    half = halo // 2
    for part in range(2):
        for r in (1, 0):
            for b in range(part * blocks // 2, (part + 1) * blocks // 2):
                col = ids_col[:, r * blocks + b:r * blocks + b + 1]
                pick = (node == col).astype(F32).astype(BF16)
                stage[pl.ds(r * halo + b * LANES, LANES), :] = jnp.dot(
                    pick, own_ref[...], preferred_element_type=F32).astype(BF16)
            dst_row = (1 - r) * halo + part * half
            copy = remote(stage.at[pl.ds(r * halo + part * half, half), :], halo_ref.at[pl.ds(dst_row, half), :],
                          sems, 2 * part + r, nxt if r == 1 else prv)
            copy.start()
            copies.append(copy)

    total = jnp.sum(jnp.sum(mask_ref[...].astype(F32), axis=1, keepdims=True), axis=0, keepdims=True)
    total = jnp.broadcast_to(total, cnt_ref.shape)
    for i, dev in enumerate(partners):
        cnt_send[i] = total
        copy = remote(cnt_send.at[i], cnt_recv.at[i], cnt_sems, i, dev)
        copy.start()
        copy.wait()
        total = total + cnt_recv[i]
    cnt_ref[...] = jnp.maximum(total, 1.0)
    for copy in copies:
        copy.wait()


def spread_weights(w_ref, wide):
    wt = jnp.transpose(w_ref[...])
    for b in range(w_ref.shape[0]):
        wide[pl.ds(b * LANES, LANES), :] = jnp.broadcast_to(wt[:, b:b + 1], (LANES, LANES))


def row_loop(pair_ref, wide, table, bufs, swap, unroll):
    def clear(i, carry):
        for buf in bufs:
            buf[pl.ds(i * 64, 64), :] = jnp.zeros((64, LANES), F32)
        return carry

    lax.fori_loop(0, bufs[0].shape[0] // 64, clear, 0)
    num = len(bufs)

    def step(i, carry):
        base = i * unroll
        for first in range(0, unroll, num):
            pairs = [pair_ref[base + first + j] for j in range(num)]
            low = [pl.multiple_of(p & 0xFFFF, 2) for p in pairs]
            high = [pl.multiple_of(lax.shift_right_logical(p, 16), 2) for p in pairs]
            take, put = (high, low) if swap else (low, high)
            vals = [wide[pl.ds(base + first + j, 1), :] * table[pl.ds(take[j], 2), :] for j in range(num)]
            old = [bufs[j][pl.ds(put[j], 2), :] for j in range(num)]
            for j in range(num):
                bufs[j][pl.ds(put[j], 2), :] = old[j] + vals[j]
        return carry

    lax.fori_loop(0, wide.shape[0] // unroll, step, 0)


def to_rows(src_ref, table, first_row):
    def body(i, carry):
        blk = src_ref[pl.ds(pl.multiple_of(i * LANES, LANES), LANES), :].astype(F32)
        for h in range(2):
            table[pl.ds(2 * first_row + 2 * i * LANES + h, LANES, stride=2), :] = blk[:, h * LANES:(h + 1) * LANES]
        return carry

    lax.fori_loop(0, src_ref.shape[0] // LANES, body, 0)


def sum_rows(bufs, blk):
    halves = []
    for h in range(2):
        parts = [buf[pl.ds(2 * blk * LANES + h, LANES, stride=2), :] for buf in bufs]
        while len(parts) > 1:
            parts = [a + b for a, b in zip(parts[::2], parts[1::2])]
        halves.append(parts[0])
    return jnp.concatenate(halves, axis=1)


def k2_body(unroll, own_ref, halo_ref, pair_ref, w_ref, w2t_ref, hid_ref, pos_ref, tab_ref, table, wide, *bufs):
    spread_weights(w_ref, wide)
    to_rows(own_ref, table, 0)
    to_rows(halo_ref, table, own_ref.shape[0])
    row_loop(pair_ref, wide, table, bufs, False, unroll)

    def finish(i, carry):
        pre = sum_rows(bufs, i)
        hid = jnp.maximum(pre, 0.0).astype(BF16)
        at = pl.ds(pl.multiple_of(i * LANES, LANES), LANES)
        hid_ref[at, :] = hid
        pos_ref[at, :] = (pre > 0.0).astype(F32).astype(BF16)
        t2 = lax.dot_general(w2t_ref[...], hid, NT, preferred_element_type=F32)
        tab_ref[pl.ds(pl.multiple_of(i * CLASS_ROWS, CLASS_ROWS), CLASS_ROWS), :] = t2.astype(BF16).astype(F32)
        return carry

    lax.fori_loop(0, hid_ref.shape[0] // LANES, finish, 0)


def k4_body(unroll, dy_ref, pair_ref, w_ref, ext_ref, table, wide, *bufs):
    spread_weights(w_ref, wide)
    to_rows(dy_ref, table, 0)
    row_loop(pair_ref, wide, table, bufs, True, unroll)

    def finish(i, carry):
        ext_ref[pl.ds(pl.multiple_of(i * LANES, LANES), LANES), :] = sum_rows(bufs, i)
        return carry

    lax.fori_loop(0, ext_ref.shape[0] // LANES, finish, 0)


def wide_row(ref, first):
    blk = ref[pl.ds(first, 8), :]
    return jnp.concatenate([blk[j:j + 1, :] for j in range(8)], axis=1)


def lo_hot(idx):
    lo = idx & (LANES - 1)
    node = lax.broadcasted_iota(jnp.int32, (LANES, idx.shape[1]), 0)
    return (node == lo).astype(F32).astype(BF16)


def hi_of(idx):
    return jnp.broadcast_to(lax.shift_right_logical(idx, 7), (CLASS_ROWS, idx.shape[1]))


def pick_cols(table_b, pieces, idx, hot):
    cols = jnp.dot(table_b, hot, preferred_element_type=F32)
    rows = table_b.shape[0] // pieces
    hi = hi_of(idx)
    out = jnp.zeros(hi.shape, F32)
    for h in range(rows // CLASS_ROWS):
        part = cols[h * CLASS_ROWS:(h + 1) * CLASS_ROWS]
        for p in range(1, pieces):
            part = part + cols[p * rows + h * CLASS_ROWS:p * rows + (h + 1) * CLASS_ROWS]
        out = out + jnp.where(hi == h, part, 0.0)
    return out


def add_cols(val, idx, hot, num_hi):
    hi = hi_of(idx)
    pieces = three_pieces(val)
    rows = []
    for h in range(0, num_hi, 2):
        both = [jnp.where(hi == h + k, p, 0.0) for k in range(2) for p in pieces]
        rows.append(jnp.concatenate(both, axis=0).astype(BF16))
    return lax.dot_general(jnp.concatenate(rows, axis=0), hot, NT, preferred_element_type=F32)


def join_pieces(acc, num_hi):
    out = []
    for h in range(num_hi):
        a = acc[h * 24:h * 24 + 24, :]
        out.append(a[0:8] + a[8:16] + a[16:24])
    return out


def stack_pieces(val):
    return jnp.concatenate(three_pieces(val), axis=0).astype(BF16)


def k3_body(num_dev, tab_ref, send_ref, src_ref, dst_ref, w_ref, lab_ref, mask_ref, cnt_ref, hid_ref, pos_ref, w2t_ref,
            dy_ref, misc_ref, ext_b, fwd_send, fwd_recv, bwd_send, bwd_recv, acc_z, acc_s, acc_r, dz_b, sems):
    me = lax.axis_index(GRAPH_AXIS)
    nxt, prv = (me + 1) % num_dev, (me + num_dev - 1) % num_dev
    meet([nxt, prv])
    own_hi = tab_ref.shape[0] // CLASS_ROWS
    halo = send_ref.shape[1]
    halo_hi = halo // LANES
    all_hi = own_hi + 2 * halo_hi
    own_b = tab_ref[...].astype(BF16)
    ext_b[pl.ds(0, own_hi * CLASS_ROWS), :] = own_b
    hot_send = [lo_hot(send_ref[r:r + 1, :]) for r in range(2)]
    copies = []
    for r in (1, 0):
        val = pick_cols(own_b, 1, send_ref[r:r + 1, :], hot_send[r])
        fwd_send[r] = jnp.concatenate([val, jnp.zeros_like(val)], axis=0).astype(BF16)
        copy = remote(fwd_send.at[r], fwd_recv.at[1 - r], sems, r, nxt if r == 1 else prv)
        copy.start()
        copies.append(copy)
    acc_z[...] = jnp.zeros_like(acc_z)
    acc_s[...] = jnp.zeros_like(acc_s)
    for copy in copies:
        copy.wait()
    for r in range(2):
        got = fwd_recv[r].astype(F32)
        for j in range(0, halo_hi, 2):
            two = jnp.concatenate([got[0:8, (j + k) * LANES:(j + k + 1) * LANES] for k in range(2)], axis=0)
            ext_b[pl.ds((own_hi + r * halo_hi + j) * CLASS_ROWS, 16), :] = two.astype(BF16)

    steps = src_ref.shape[0] // 8

    def forward(i, carry):
        first = pl.multiple_of(i * 8, 8)
        src, dst = wide_row(src_ref, first), wide_row(dst_ref, first)
        val = pick_cols(ext_b[...], 1, src, lo_hot(src)) * wide_row(w_ref, first)
        acc_z[...] += add_cols(val, dst, lo_hot(dst), own_hi)
        return carry

    lax.fori_loop(0, steps, forward, 0)

    logits = join_pieces(acc_z[...], own_hi)
    cls = lax.broadcasted_iota(jnp.int32, (CLASS_ROWS, LANES), 0)
    count = cnt_ref[0:1, :]
    loss = jnp.zeros((1, LANES), F32)
    d_log = []
    for h in range(own_hi):
        z = jnp.where(cls < 7, logits[h], -jnp.inf)
        top = jnp.max(z, axis=0, keepdims=True)
        norm = jnp.log(jnp.sum(jnp.exp(z - top), axis=0, keepdims=True)) + top
        hot = cls == lab_ref[h:h + 1, :]
        mask = mask_ref[h:h + 1, :].astype(F32)
        picked = jnp.sum(jnp.where(hot, logits[h], 0.0), axis=0, keepdims=True)
        loss = loss + mask * (norm - picked)
        d_log.append((jnp.exp(z - norm) - hot.astype(F32)) * (mask / count))
    dz_b[...] = stack_pieces(jnp.concatenate(d_log, axis=0))

    def backward(i, carry):
        first = pl.multiple_of(i * 8, 8)
        src, dst = wide_row(src_ref, first), wide_row(dst_ref, first)
        val = pick_cols(dz_b[...], 3, dst, lo_hot(dst)) * wide_row(w_ref, first)
        acc_s[...] += add_cols(val, src, lo_hot(src), all_hi)
        return carry

    lax.fori_loop(0, steps, backward, 0)

    d_ext = join_pieces(acc_s[...], all_hi)
    copies = []
    for r in range(2):
        for j in range(halo_hi):
            bwd_send[r, :, j * LANES:(j + 1) * LANES] = d_ext[own_hi + r * halo_hi + j]
        copy = remote(bwd_send.at[r], bwd_recv.at[1 - r], sems, 2 + r, prv if r == 0 else nxt)
        copy.start()
        copies.append(copy)
    for copy in copies:
        copy.wait()
    for r in range(2):
        part = add_cols(bwd_recv[r], send_ref[r:r + 1, :], hot_send[r], own_hi)
        acc_r[...] = part if r == 0 else acc_r[...] + part
    back = join_pieces(acc_r[...], own_hi)
    grad = jnp.zeros((CLASS_ROWS, hid_ref.shape[1]), F32)
    for h in range(own_hi):
        d_tab = d_ext[h] + back[h]
        d_tab_b = d_tab.astype(BF16)
        at = pl.ds(h * LANES, LANES)
        grad = grad + jnp.dot(d_tab_b, hid_ref[at, :], preferred_element_type=F32)
        d_hid = jnp.dot(jnp.transpose(d_tab).astype(BF16), w2t_ref[...], preferred_element_type=F32)
        dy_ref[at, :] = jnp.where(pos_ref[at, :].astype(F32) > 0.0, d_hid, 0.0)
    misc_ref[0:8, :] = grad
    total = jnp.sum(loss, axis=1, keepdims=True) / count[:, 0:1]
    misc_ref[8:16, :] = jnp.broadcast_to(total, (8, misc_ref.shape[1]))


def k5_body(num_dev, bits, x_ref, ext_ref, send_ref, misc_ref, grad_ref, tail_ref,
            xt, hot, recv, back, part, full, *rest):
    landing, (sems, sum_sems) = rest[:len(bits)], rest[len(bits):]
    me = lax.axis_index(GRAPH_AXIS)
    nxt, prv = (me + 1) % num_dev, (me + num_dev - 1) % num_dev
    partners = [flip(me, b) for b in bits]
    meet([nxt, prv] + partners)
    rows, feats = x_ref.shape
    halo = send_ref.shape[1]
    chunks = 4
    size = halo // chunks
    copies = []
    for q in range(chunks):
        for r in range(2):
            copy = remote(ext_ref.at[pl.ds(rows + r * halo + q * size, size), :],
                          recv.at[pl.ds((1 - r) * halo + q * size, size), :], sems, 2 * q + r, prv if r == 0 else nxt)
            copy.start()
            copies.append(copy)
    node = lax.broadcasted_iota(jnp.int32, (rows, size), 0)
    for r in range(2):
        for q in range(chunks):
            ids = send_ref[r:r + 1, q * size:(q + 1) * size]
            hot[:, r * halo + q * size:r * halo + (q + 1) * size] = (node == ids).astype(F32).astype(BF16)
    for b in range(4):
        lo, hi = b * LANES, min((b + 1) * LANES, feats)
        blk = x_ref[:, lo:hi].astype(F32)
        if hi - lo < LANES:
            blk = jnp.concatenate([blk, jnp.zeros((rows, LANES - (hi - lo)), F32)], axis=1)
        xt[lo:lo + LANES, :] = jnp.transpose(blk).astype(BF16)
    back[...] = ext_ref[pl.ds(0, rows), :]
    tile = 256
    for q in range(chunks):
        for r in range(2):
            copies[2 * q + r].wait()
        for r in range(2):
            first = r * halo + q * size
            val = recv[pl.ds(first, size), :]
            pieces = [p.astype(BF16) for p in three_pieces(val)]

            def add(i, carry):
                at = pl.ds(pl.multiple_of(i * tile, tile), tile)
                pick = hot[at, first:first + size]
                total = back[at, :]
                for p in pieces:
                    total = total + jnp.dot(pick, p, preferred_element_type=F32)
                back[at, :] = total
                return carry

            lax.fori_loop(0, rows // tile, add, 0)
    d_tab = back[...].astype(BF16)
    part[...] = jnp.dot(xt[...], d_tab, preferred_element_type=F32)
    part[feats:feats + 9, :] = misc_ref[0:9, :]

    offset = 0
    size = part.shape[0]
    for i, (bit, dev) in enumerate(zip(bits, partners)):
        size //= 2
        mine = (me // bit) % 2
        give = pl.multiple_of(offset + (1 - mine) * size, size)
        keep = pl.multiple_of(offset + mine * size, size)
        copy = remote(part.at[pl.ds(give, size), :], landing[i], sum_sems, i, dev)
        copy.start()
        copy.wait()
        part[pl.ds(keep, size), :] += landing[i][...]
        offset = keep
    full[pl.ds(offset, size), :] = part[pl.ds(offset, size), :]
    for i in range(len(bits) - 1, -1, -1):
        copy = remote(full.at[pl.ds(offset, size), :], full.at[pl.ds(offset, size), :], sum_sems, len(bits) + i, partners[i])
        copy.start()
        copy.wait()
        offset = pl.multiple_of(offset - ((me // bits[i]) % 2) * size, size)
        size *= 2
    grad_ref[...] = full[0:feats, :]
    tail_ref[...] = full[feats - 4:feats + 12, :]


def solution(mesh):
    num_dev = mesh.shape[GRAPH_AXIS]
    bits = []
    while 2 ** len(bits) < num_dev:
        bits.append(2 ** len(bits))

    def params(cid=None):
        if cid is None:
            return pltpu.CompilerParams(vmem_limit_bytes=VMEM_BYTES)
        return pltpu.CompilerParams(vmem_limit_bytes=VMEM_BYTES, collective_id=cid, has_side_effects=True)

    def device_step(node_feats, w_one, w_two, send_rows, edge_src, edge_dst, edge_w, labels, label_mask):
        rows, feats = node_feats.shape
        width = w_one.shape[1]
        classes = w_two.shape[1]
        halo = send_rows.shape[1]
        edges = edge_src.shape[0]
        own_hi, all_hi = rows // LANES, (rows + 2 * halo) // LANES
        w2t = jnp.zeros((CLASS_ROWS, width), BF16).at[:classes].set(w_two.astype(BF16).T)
        pair = edge_src * 2 + edge_dst * (2 << 16)
        src2, dst2, w2 = (a.reshape(edges // LANES, LANES) for a in (edge_src, edge_dst, edge_w))
        lab2, mask2 = labels.reshape(own_hi, LANES), label_mask.reshape(own_hi, LANES)

        own, halo_rows, count = pl.pallas_call(
            functools.partial(k1_body, num_dev, bits),
            out_shape=(jax.ShapeDtypeStruct((rows, width), BF16), jax.ShapeDtypeStruct((2 * halo, width), BF16),
                       jax.ShapeDtypeStruct((8, LANES), F32)),
            in_specs=[vmem()] * 4, out_specs=(vmem(),) * 3,
            scratch_shapes=[pltpu.VMEM((2 * halo, width), BF16), pltpu.VMEM((len(bits), 8, LANES), F32),
                            pltpu.VMEM((len(bits), 8, LANES), F32), pltpu.SemaphoreType.DMA((2, 4)),
                            pltpu.SemaphoreType.DMA((2, len(bits)))],
            compiler_params=params(0), name="transform_and_halo",
        )(node_feats, w_one, send_rows, mask2)

        hid, pos, tab = pl.pallas_call(
            functools.partial(k2_body, 32),
            out_shape=(jax.ShapeDtypeStruct((rows, width), BF16), jax.ShapeDtypeStruct((rows, width), BF16),
                       jax.ShapeDtypeStruct((own_hi * CLASS_ROWS, LANES), F32)),
            in_specs=[vmem(), vmem(), smem(), vmem(), vmem()], out_specs=(vmem(),) * 3,
            scratch_shapes=[pltpu.VMEM((2 * (rows + 2 * halo), LANES), F32), pltpu.VMEM((edges, LANES), F32)]
            + [pltpu.VMEM((2 * rows, LANES), F32)] * 8,
            compiler_params=params(), name="aggregate_one",
        )(own, halo_rows, pair, w2, w2t)

        d_pre, misc = pl.pallas_call(
            functools.partial(k3_body, num_dev),
            out_shape=(jax.ShapeDtypeStruct((rows, width), F32), jax.ShapeDtypeStruct((16, width), F32)),
            in_specs=[vmem()] * 11, out_specs=(vmem(),) * 2,
            scratch_shapes=[pltpu.VMEM((all_hi * CLASS_ROWS, LANES), BF16), pltpu.VMEM((2, 16, halo), BF16),
                            pltpu.VMEM((2, 16, halo), BF16), pltpu.VMEM((2, CLASS_ROWS, halo), F32),
                            pltpu.VMEM((2, CLASS_ROWS, halo), F32), pltpu.VMEM((own_hi * 24, LANES), F32),
                            pltpu.VMEM((all_hi * 24, LANES), F32), pltpu.VMEM((own_hi * 24, LANES), F32),
                            pltpu.VMEM((3 * own_hi * CLASS_ROWS, LANES), BF16), pltpu.SemaphoreType.DMA((2, 4))],
            compiler_params=params(1), name="layer_two",
        )(tab, send_rows, src2, dst2, w2, lab2, mask2, count, hid, pos, w2t)

        ext = pl.pallas_call(
            functools.partial(k4_body, 32),
            out_shape=jax.ShapeDtypeStruct((rows + 2 * halo, width), F32),
            in_specs=[vmem(), smem(), vmem()], out_specs=vmem(),
            scratch_shapes=[pltpu.VMEM((2 * rows, LANES), F32), pltpu.VMEM((edges, LANES), F32)]
            + [pltpu.VMEM((2 * (rows + 2 * halo), LANES), F32)] * 8,
            compiler_params=params(), name="scatter_one",
        )(d_pre, pair, w2)

        sum_rows_pad = 512
        landing = [pltpu.VMEM((sum_rows_pad >> (i + 1), width), F32) for i in range(len(bits))]
        grad_one, tail = pl.pallas_call(
            functools.partial(k5_body, num_dev, bits),
            out_shape=(jax.ShapeDtypeStruct((feats, width), F32), jax.ShapeDtypeStruct((16, width), F32)),
            in_specs=[vmem()] * 4, out_specs=(vmem(),) * 2,
            scratch_shapes=[pltpu.VMEM((sum_rows_pad, rows), BF16), pltpu.VMEM((rows, 2 * halo), BF16),
                            pltpu.VMEM((2 * halo, width), F32), pltpu.VMEM((rows, width), F32),
                            pltpu.VMEM((sum_rows_pad, width), F32), pltpu.VMEM((sum_rows_pad, width), F32)]
            + landing + [pltpu.SemaphoreType.DMA((2, 8)), pltpu.SemaphoreType.DMA((2, 2 * len(bits)))],
            compiler_params=params(2), name="weight_gradient",
        )(node_feats, ext, send_rows, misc)
        return tail[12, 0], grad_one, tail[4:4 + classes].T

    row_spec = P(GRAPH_AXIS)
    return jax.shard_map(device_step, mesh=mesh,
                         in_specs=(row_spec, P(), P(), row_spec, row_spec, row_spec, row_spec, row_spec, row_spec),
                         out_specs=(P(), P(), P()), check_vma=False)
```

```python
import functools

import jax
import jax.numpy as jnp
from jax import lax
from jax.experimental import pallas as pl
from jax.experimental.pallas import tpu as pltpu
from jax.sharding import PartitionSpec as P

GRAPH_AXIS = "graph"
MESH = pl.DeviceIdType.MESH
LANES = 128
CLASS_ROWS = 8
VMEM_BYTES = 60 * 2**20
F32 = jnp.float32
BF16 = jnp.bfloat16
NT = (((1,), (1,)), ((), ()))
TN = (((0,), (0,)), ((), ()))


def vmem():
    return pl.BlockSpec(memory_space=pltpu.VMEM)


def smem():
    return pl.BlockSpec(memory_space=pltpu.SMEM)


PLANE = 8
LIST_ROWS = 80
BLOCK = 32
NUM_BUFS = 4


def ring_peers(num_dev):
    me = lax.axis_index(GRAPH_AXIS)
    return me, (me + 1) % num_dev, (me + num_dev - 1) % num_dev


def layer_peers(me, num_dev):
    return [(me + PLANE * k) % num_dev for k in range(1, num_dev // PLANE)]


def class_weights(w_ref):
    w = w_ref[...]
    return jnp.concatenate([w, jnp.zeros((CLASS_ROWS - w.shape[0], w.shape[1]), F32)], axis=0).astype(BF16)


def meet(partners):
    barrier = pltpu.get_barrier_semaphore()
    for dev in partners:
        pl.semaphore_signal(barrier, inc=1, device_id=(dev,), device_id_type=MESH)
    pl.semaphore_wait(barrier, len(partners))


def remote(src, dst, sems, slot, dev):
    return pltpu.make_async_remote_copy(
        src_ref=src, dst_ref=dst, send_sem=sems.at[0, slot], recv_sem=sems.at[1, slot],
        device_id=(dev,), device_id_type=MESH)


def three_pieces(val):
    top = val.astype(BF16).astype(F32)
    rest = val - top
    mid = rest.astype(BF16).astype(F32)
    return top, mid, rest - mid


def wide_row(ref, first):
    blk = ref[pl.ds(first, 8), :]
    return jnp.concatenate([blk[j:j + 1, :] for j in range(8)], axis=1)


def lo_hot(idx):
    lo = idx & (LANES - 1)
    node = lax.broadcasted_iota(jnp.int32, (LANES, idx.shape[1]), 0)
    return (node == lo).astype(F32).astype(BF16)


def list_places(src_ref, w_ref, rows, halo, pos, num_ref):
    src, live = src_ref[...], w_ref[...] != 0.0
    n_rows = src.shape[0]
    tri = (lax.broadcasted_iota(jnp.int32, (LANES, LANES), 0) <= lax.broadcasted_iota(jnp.int32, (LANES, LANES), 1))
    tri = tri.astype(F32).astype(BF16)
    low = (lax.broadcasted_iota(jnp.int32, (n_rows, n_rows), 1) < lax.broadcasted_iota(jnp.int32, (n_rows, n_rows), 0))
    low = low.astype(F32).astype(BF16)
    place = jnp.full(src.shape, LIST_ROWS * LANES, jnp.int32)
    start = jnp.zeros((1, 1), jnp.int32)
    lane = lax.broadcasted_iota(jnp.int32, num_ref.shape, 1)
    num = jnp.zeros(num_ref.shape, jnp.int32)
    kinds = (src < rows, (src >= rows) & (src < rows + halo), src >= rows + halo)
    for k, kind in enumerate(kinds):
        kind = kind & live
        flag = kind.astype(F32)
        inner = jnp.dot(flag.astype(BF16), tri, preferred_element_type=F32)
        row_sum = jnp.broadcast_to(jnp.sum(flag, axis=1, keepdims=True), flag.shape)
        before = jnp.dot(low, row_sum.astype(BF16), preferred_element_type=F32)
        rank = (inner + before).astype(jnp.int32) - 1
        place = jnp.where(kind, start + rank, place)
        total = jnp.sum(jnp.sum(flag, axis=1, keepdims=True), axis=0, keepdims=True).astype(jnp.int32)
        blocks = lax.shift_right_logical(total + (BLOCK - 1), BLOCK.bit_length() - 1)
        start = start + blocks * BLOCK
        num = jnp.where(lane == k, blocks, num)
    pos[...] = place
    num_ref[...] = num


def k1_body(num_dev, xt_ref, w_ref, send_ref, mask_ref, src_ref, dst_ref, ew_ref,
            own_ref, halo_ref, cnt_ref, lsrc_ref, ldst_ref, ltgt_ref, lw_ref, num_ref,
            stage, peer, cnt_send, cnt_recv, pos, acc, sems, peer_sems, cnt_sems):
    me, nxt, prv = ring_peers(num_dev)
    layer = [me - me % PLANE + (me % PLANE + k) % PLANE for k in range(1, PLANE)]
    meet([nxt, prv] + layer)
    rows = own_ref.shape[0]
    halo = send_ref.shape[1]
    total = jnp.sum(jnp.sum(mask_ref[...].astype(F32), axis=1, keepdims=True), axis=0, keepdims=True)
    cnt_send[...] = jnp.broadcast_to(total, cnt_send.shape)
    small = [remote(send_ref, peer.at[0], peer_sems, 0, nxt), remote(send_ref, peer.at[1], peer_sems, 1, prv)]
    small += [remote(cnt_send, cnt_recv.at[k], cnt_sems, k, dev) for k, dev in enumerate(layer)]
    for copy in small:
        copy.start()
    own_t = lax.dot_general(w_ref[...].astype(BF16), xt_ref[...], TN, preferred_element_type=F32)
    own_ref[...] = jnp.transpose(own_t).astype(BF16)

    blocks = halo // LANES
    ids = jnp.concatenate([send_ref[r:r + 1, b * LANES:(b + 1) * LANES] for r in range(2) for b in range(blocks)], axis=0)
    ids_col = jnp.transpose(ids)
    node = lax.broadcasted_iota(jnp.int32, (LANES, rows), 1)
    copies = []
    half = halo // 2
    for part in range(2):
        for r in (1, 0):
            for b in range(part * blocks // 2, (part + 1) * blocks // 2):
                col = ids_col[:, r * blocks + b:r * blocks + b + 1]
                pick = (node == col).astype(F32).astype(BF16)
                stage[pl.ds(r * halo + b * LANES, LANES), :] = jnp.dot(
                    pick, own_ref[...], preferred_element_type=F32).astype(BF16)
            dst_row = (1 - r) * halo + part * half
            copy = remote(stage.at[pl.ds(r * halo + part * half, half), :], halo_ref.at[pl.ds(dst_row, half), :],
                          sems, 2 * part + r, nxt if r == 1 else prv)
            copy.start()
            copies.append(copy)

    list_places(src_ref, ew_ref, rows, halo, pos, num_ref)
    for copy in small:
        copy.wait()
    for k in range(len(layer)):
        total = total + cnt_recv[k][0:1, 0:1]
    cnt_ref[...] = jnp.broadcast_to(total, cnt_ref.shape)
    theirs = jnp.concatenate([peer[s][1 - s:2 - s, b * LANES:(b + 1) * LANES] for s in range(2) for b in range(blocks)], axis=0)
    theirs = jnp.concatenate([lax.shift_right_logical(theirs, 4), theirs & 15], axis=0).astype(F32).astype(BF16)
    acc[...] = jnp.zeros_like(acc)

    def sort(i, carry):
        first = pl.multiple_of(i * 8, 8)
        src, dst, wgt, place = (wide_row(ref, first) for ref in (src_ref, dst_ref, ew_ref, pos))
        n = src.shape[1]
        at = jnp.maximum(src - rows, 0)
        cols = jnp.dot(theirs, lo_hot(at), preferred_element_type=F32)
        cols = cols[0:2 * blocks] * 16.0 + cols[2 * blocks:4 * blocks]
        mine = lax.broadcasted_iota(jnp.int32, cols.shape, 0) == lax.shift_right_logical(at, 7)
        tgt = jnp.sum(jnp.where(mine, cols, 0.0), axis=0, keepdims=True).astype(jnp.int32)
        tgt = jnp.where(src < rows, src, tgt)
        both = src + dst * 4096
        ints = [both & 255, lax.shift_right_logical(both, 8) & 255, lax.shift_right_logical(both, 16),
                tgt & 255, lax.shift_right_logical(tgt, 8)]
        cargo = [v.astype(F32) for v in ints] + list(three_pieces(wgt))
        here = lax.broadcasted_iota(jnp.int32, (LIST_ROWS, n), 0) == lax.shift_right_logical(place, 7)
        lhs = jnp.concatenate([jnp.where(here, v, 0.0).astype(BF16) for v in cargo], axis=0)
        acc[...] += lax.dot_general(lhs, lo_hot(place), NT, preferred_element_type=F32)
        return carry

    lax.fori_loop(0, src_ref.shape[0] // 8, sort, 0)
    got = [acc[p * LIST_ROWS:(p + 1) * LIST_ROWS, :] for p in range(8)]
    ints = [g.astype(jnp.int32) for g in got[:5]]
    both = ints[0] + ints[1] * 256 + ints[2] * 65536
    lsrc_ref[...] = (both & 4095) * 2
    ldst_ref[...] = lax.shift_right_logical(both, 12) * 2
    ltgt_ref[...] = (ints[3] + ints[4] * 256) * 2
    lw_ref[...] = got[5] + got[6] + got[7]
    for copy in copies:
        copy.wait()


def spread_weights(w_ref, wide, first, last):
    def body(b, carry):
        row = jnp.broadcast_to(w_ref[pl.ds(b, 1), :], (LANES, LANES))
        wide[pl.ds(pl.multiple_of(b * LANES, LANES), LANES), :] = jnp.transpose(row)
        return carry

    lax.fori_loop(first, last, body, 0)


def clear_rows(bufs):
    def body(i, carry):
        for buf in bufs:
            buf[pl.ds(pl.multiple_of(i * 64, 64), 64), :] = jnp.zeros((64, LANES), F32)
        return carry

    lax.fori_loop(0, bufs[0].shape[0] // 64, body, 0)


def row_loop(take_ref, put_ref, wide, table, bufs, first, last):
    num = len(bufs)

    def step(i, carry):
        base = i * BLOCK
        for lead in range(0, BLOCK, num):
            take = [pl.multiple_of(take_ref[base + lead + j], 2) for j in range(num)]
            put = [pl.multiple_of(put_ref[base + lead + j], 2) for j in range(num)]
            vals = [wide[pl.ds(base + lead + j, 1), :] * table[pl.ds(take[j], 2), :] for j in range(num)]
            old = [bufs[j][pl.ds(put[j], 2), :] for j in range(num)]
            for j in range(num):
                bufs[j][pl.ds(put[j], 2), :] = old[j] + vals[j]
        return carry

    lax.fori_loop(first, last, step, 0)


def list_rows(first, last):
    return first * BLOCK // LANES, (last * BLOCK + LANES - 1) // LANES


def to_rows(blk, table, first_row):
    for h in range(2):
        table[pl.ds(2 * first_row + h, blk.shape[0], stride=2), :] = blk[:, h * LANES:(h + 1) * LANES]


def sum_rows(bufs, blk):
    halves = []
    for h in range(2):
        parts = [buf[pl.ds(2 * blk * LANES + h, LANES, stride=2), :] for buf in bufs]
        while len(parts) > 1:
            parts = [a + b for a, b in zip(parts[::2], parts[1::2])]
        halves.append(parts[0])
    return jnp.concatenate(halves, axis=1)


def k2_body(own_ref, halo_ref, lsrc_ref, ldst_ref, num_ref, lw_ref, w2_ref, hid_ref, pos_ref, tab_ref, table, wide, *bufs):
    end = num_ref[0, 0] + num_ref[0, 1] + num_ref[0, 2]
    spread_weights(lw_ref, wide, *list_rows(0, end))
    rows = own_ref.shape[0]

    def widen(i, carry):
        at = pl.ds(pl.multiple_of(i * LANES, LANES), LANES)
        to_rows(own_ref[at, :].astype(F32), table, i * LANES)
        to_rows(halo_ref[at, :].astype(F32), table, rows + i * LANES)
        return carry

    lax.fori_loop(0, rows // LANES, widen, 0)
    clear_rows(bufs)
    row_loop(lsrc_ref, ldst_ref, wide, table, bufs, 0, end)
    w2t = class_weights(w2_ref)

    def finish(i, carry):
        pre = sum_rows(bufs, i)
        hid = jnp.maximum(pre, 0.0).astype(BF16)
        at = pl.ds(pl.multiple_of(i * LANES, LANES), LANES)
        hid_ref[at, :] = hid
        pos_ref[at, :] = (pre > 0.0).astype(F32).astype(BF16)
        t2 = lax.dot_general(w2t, hid, NT, preferred_element_type=F32)
        tab_ref[pl.ds(pl.multiple_of(i * CLASS_ROWS, CLASS_ROWS), CLASS_ROWS), :] = t2.astype(BF16).astype(F32)
        return carry

    lax.fori_loop(0, rows // LANES, finish, 0)


def k4_body(own_list, prev_list, next_list, pos_own_ref, pos_halo_ref, dt_own_ref, dt_halo_ref, w2_ref, xt_ref, misc_ref,
            out_ref, dt_wide, tables, wide, d_tab, *bufs):
    w2t = class_weights(w2_ref)
    rows = pos_own_ref.shape[0]
    clear_rows(bufs)
    sides = ((own_list, dt_own_ref, pos_own_ref, 0), (prev_list, dt_halo_ref.at[0], pos_halo_ref.at[0], 2),
             (next_list, dt_halo_ref.at[1], pos_halo_ref.at[1], 1))
    for (take_ref, put_ref, num_ref, lw_ref), dt_ref, pos_ref, kind in sides:
        dt_wide[...] = dt_ref[...].astype(F32)

        def widen(i, carry):
            dt = dt_wide[pl.ds(pl.multiple_of(i * CLASS_ROWS, CLASS_ROWS), CLASS_ROWS), :]
            d_hid = jnp.dot(jnp.transpose(dt).astype(BF16), w2t, preferred_element_type=F32)
            at = pl.ds(pl.multiple_of(i * LANES, LANES), LANES)
            to_rows(jnp.where(pos_ref[at, :].astype(F32) > 0.0, d_hid, 0.0), tables, i * LANES)
            return carry

        lax.fori_loop(0, rows // LANES, widen, 0)
        first = 0
        for k in range(kind):
            first = first + num_ref[0, k]
        last = first + num_ref[0, kind]
        spread_weights(lw_ref, wide, *list_rows(first, last))
        row_loop(take_ref, put_ref, wide, tables, bufs, first, last)

    def finish(i, carry):
        d_tab[pl.ds(pl.multiple_of(i * LANES, LANES), LANES), :] = sum_rows(bufs, i).astype(BF16)
        return carry

    lax.fori_loop(0, rows // LANES, finish, 0)
    feats = xt_ref.shape[0]
    out_ref[0:feats, :] = jnp.dot(xt_ref[...], d_tab[...], preferred_element_type=F32)
    out_ref[feats:feats + 12, :] = misc_ref[0:12, :]


def hi_of(idx):
    return jnp.broadcast_to(lax.shift_right_logical(idx, 7), (CLASS_ROWS, idx.shape[1]))


def pick_cols(table_b, pieces, idx, hot):
    cols = jnp.dot(table_b, hot, preferred_element_type=F32)
    rows = table_b.shape[0] // pieces
    hi = hi_of(idx)
    out = jnp.zeros(hi.shape, F32)
    for h in range(rows // CLASS_ROWS):
        part = cols[h * CLASS_ROWS:(h + 1) * CLASS_ROWS]
        for p in range(1, pieces):
            part = part + cols[p * rows + h * CLASS_ROWS:p * rows + (h + 1) * CLASS_ROWS]
        out = out + jnp.where(hi == h, part, 0.0)
    return out


def add_cols(val, idx, hot, num_hi):
    hi = hi_of(idx)
    pieces = three_pieces(val)
    rows = []
    for h in range(0, num_hi, 2):
        both = [jnp.where(hi == h + k, p, 0.0) for k in range(2) for p in pieces]
        rows.append(jnp.concatenate(both, axis=0).astype(BF16))
    return lax.dot_general(jnp.concatenate(rows, axis=0), hot, NT, preferred_element_type=F32)


def join_pieces(acc, num_hi):
    out = []
    for h in range(num_hi):
        a = acc[h * 24:h * 24 + 24, :]
        out.append(a[0:8] + a[8:16] + a[16:24])
    return out


def stack_pieces(val):
    return jnp.concatenate(three_pieces(val), axis=0).astype(BF16)


def k3_body(num_dev, tab_ref, send_ref, src_ref, dst_ref, w_ref, lab_ref, mask_ref, cnt_ref, hid_ref, pos_ref,
            ldst_ref, ltgt_ref, lw_ref, num_ref,
            dt_ref, misc_ref, dt_halo_ref, pos_halo_ref, hdst_ref, htgt_ref, hw_ref, hnum_ref,
            ext_b, fwd_send, fwd_recv, bwd_send, bwd_recv, acc_z, acc_s, acc_r, dz_b, cnt_recv,
            sems, cnt_sems, list_sems, pos_sems):
    me, nxt, prv = ring_peers(num_dev)
    layers = layer_peers(me, num_dev)
    meet([nxt, prv] + layers)
    counts = [remote(cnt_ref, cnt_recv.at[k], cnt_sems, k, dev) for k, dev in enumerate(layers)]
    for copy in counts:
        copy.start()
    late = []

    def send_late(pairs, pool, first):
        for k, (src, dst) in enumerate(pairs):
            for s, dev in enumerate((nxt, prv)):
                copy = remote(src, dst(s), pool, 2 * (first + k) + s, dev)
                copy.start()
                late.append(copy)

    chunk = pos_ref.shape[0] // 4

    def send_pos(q):
        at = pl.ds(q * chunk, chunk)
        send_late([(pos_ref.at[at, :], lambda s: pos_halo_ref.at[s, at, :])], pos_sems, q)

    own_hi = tab_ref.shape[0] // CLASS_ROWS
    halo = send_ref.shape[1]
    halo_hi = halo // LANES
    all_hi = own_hi + 2 * halo_hi
    own_b = tab_ref[...].astype(BF16)
    ext_b[pl.ds(0, own_hi * CLASS_ROWS), :] = own_b
    hot_send = [lo_hot(send_ref[r:r + 1, :]) for r in range(2)]
    copies = []
    for r in (1, 0):
        val = pick_cols(own_b, 1, send_ref[r:r + 1, :], hot_send[r])
        fwd_send[r] = jnp.concatenate([val, jnp.zeros_like(val)], axis=0).astype(BF16)
        copy = remote(fwd_send.at[r], fwd_recv.at[1 - r], sems, r, nxt if r == 1 else prv)
        copy.start()
        copies.append(copy)
    send_late([(ldst_ref, lambda s: hdst_ref.at[s]), (ltgt_ref, lambda s: htgt_ref.at[s]),
               (lw_ref, lambda s: hw_ref.at[s]), (num_ref, lambda s: hnum_ref.at[s])], list_sems, 0)
    send_pos(0)
    send_pos(1)
    acc_z[...] = jnp.zeros_like(acc_z)
    acc_s[...] = jnp.zeros_like(acc_s)
    for copy in copies:
        copy.wait()
    for r in range(2):
        got = fwd_recv[r].astype(F32)
        for j in range(0, halo_hi, 2):
            two = jnp.concatenate([got[0:8, (j + k) * LANES:(j + k + 1) * LANES] for k in range(2)], axis=0)
            ext_b[pl.ds((own_hi + r * halo_hi + j) * CLASS_ROWS, 16), :] = two.astype(BF16)

    steps = src_ref.shape[0] // 8

    def forward(i, carry):
        first = pl.multiple_of(i * 8, 8)
        src, dst = wide_row(src_ref, first), wide_row(dst_ref, first)
        val = pick_cols(ext_b[...], 1, src, lo_hot(src)) * wide_row(w_ref, first)
        acc_z[...] += add_cols(val, dst, lo_hot(dst), own_hi)
        return carry

    lax.fori_loop(0, steps, forward, 0)

    logits = join_pieces(acc_z[...], own_hi)
    cls = lax.broadcasted_iota(jnp.int32, (CLASS_ROWS, LANES), 0)
    count = cnt_ref[0:1, :]
    for k, copy in enumerate(counts):
        copy.wait()
        count = count + cnt_recv[k][0:1, :]
    count = jnp.maximum(count, 1.0)
    loss = jnp.zeros((1, LANES), F32)
    d_log = []
    for h in range(own_hi):
        z = jnp.where(cls < 7, logits[h], -jnp.inf)
        top = jnp.max(z, axis=0, keepdims=True)
        norm = jnp.log(jnp.sum(jnp.exp(z - top), axis=0, keepdims=True)) + top
        hot = cls == lab_ref[h:h + 1, :]
        mask = mask_ref[h:h + 1, :].astype(F32)
        picked = jnp.sum(jnp.where(hot, logits[h], 0.0), axis=0, keepdims=True)
        loss = loss + mask * (norm - picked)
        d_log.append((jnp.exp(z - norm) - hot.astype(F32)) * (mask / count))
    dz_b[...] = stack_pieces(jnp.concatenate(d_log, axis=0))

    def backward(i, carry):
        first = pl.multiple_of(i * 8, 8)
        src, dst = wide_row(src_ref, first), wide_row(dst_ref, first)
        val = pick_cols(dz_b[...], 3, dst, lo_hot(dst)) * wide_row(w_ref, first)
        acc_s[...] += add_cols(val, src, lo_hot(src), all_hi)
        return carry

    lax.fori_loop(0, steps, backward, 0)

    d_ext = join_pieces(acc_s[...], all_hi)
    copies = []
    for r in range(2):
        for j in range(halo_hi):
            bwd_send[r, :, j * LANES:(j + 1) * LANES] = d_ext[own_hi + r * halo_hi + j]
        copy = remote(bwd_send.at[r], bwd_recv.at[1 - r], sems, 2 + r, prv if r == 0 else nxt)
        copy.start()
        copies.append(copy)
    send_pos(2)
    for copy in copies:
        copy.wait()
    for r in range(2):
        part = add_cols(bwd_recv[r], send_ref[r:r + 1, :], hot_send[r], own_hi)
        acc_r[...] = part if r == 0 else acc_r[...] + part
    back = join_pieces(acc_r[...], own_hi)
    d_tab = [d_ext[h] + back[h] for h in range(own_hi)]
    dt_ref[...] = jnp.concatenate(d_tab, axis=0).astype(BF16)
    send_late([(dt_ref, lambda s: dt_halo_ref.at[s])], list_sems, 4)
    send_pos(3)
    grad = jnp.zeros((CLASS_ROWS, hid_ref.shape[1]), F32)
    for h in range(own_hi):
        grad = grad + jnp.dot(d_tab[h].astype(BF16), hid_ref[pl.ds(h * LANES, LANES), :], preferred_element_type=F32)
    misc_ref[0:8, :] = grad
    total = jnp.sum(loss, axis=1, keepdims=True) / count[:, 0:1]
    misc_ref[8:16, :] = jnp.broadcast_to(total, (8, misc_ref.shape[1]))
    for copy in late:
        copy.wait()


def k5_body(num_dev, part_ref, full_ref, land_core, land_chip, land_z, by_core, by_chip, sems):
    me = lax.axis_index(GRAPH_AXIS)
    core, chip, z = me % 2, (me // 2) % 4, me // PLANE
    other = me + 1 - 2 * core
    chips = [me + 2 * ((chip + k) % 4 - chip) for k in range(1, 4)]
    layers = layer_peers(me, num_dev)
    num_z = num_dev // PLANE
    meet([other] + chips + layers)
    rows = part_ref.shape[0]
    n1, n2, n3 = rows // 2, rows // 8, rows // 8 // num_z
    slot = 0
    keep = pl.multiple_of(core * n1, n1)
    copy = remote(part_ref.at[pl.ds(pl.multiple_of((1 - core) * n1, n1), n1), :], land_core, sems, slot, other)
    copy.start()
    copy.wait()
    by_core[...] = part_ref[pl.ds(keep, n1), :] + land_core[...]

    slot = 1
    copies = []
    for k, dev in enumerate(chips):
        at = pl.multiple_of(((chip + k + 1) % 4) * n2, n2)
        copies.append(remote(by_core.at[pl.ds(at, n2), :], land_chip.at[k], sems, slot + k, dev))
        copies[-1].start()
    total = by_core[pl.ds(pl.multiple_of(chip * n2, n2), n2), :]
    for k, copy in enumerate(copies):
        copy.wait()
        total = total + land_chip[k]
    by_chip[...] = total

    slot = 4
    copies = []
    for k, dev in enumerate(layers):
        at = pl.multiple_of(((z + k + 1) % num_z) * n3, n3)
        copies.append(remote(by_chip.at[pl.ds(at, n3), :], land_z.at[k], sems, slot + k, dev))
        copies[-1].start()
    total = by_chip[pl.ds(pl.multiple_of(z * n3, n3), n3), :]
    for k, copy in enumerate(copies):
        copy.wait()
        total = total + land_z[k]
    first = pl.multiple_of(core * n1 + chip * n2 + z * n3, n3)
    full_ref[pl.ds(first, n3), :] = total

    slot = 4 + len(layers)
    for at, size, devs in ((first, n3, layers), (core * n1 + chip * n2, n2, chips), (core * n1, n1, [other])):
        own = full_ref.at[pl.ds(pl.multiple_of(at, size), size), :]
        copies = [remote(own, own, sems, slot + k, dev) for k, dev in enumerate(devs)]
        slot += len(devs)
        for copy in copies:
            copy.start()
        for copy in copies:
            copy.wait()


def k6_body(full_ref, loss_ref, one_ref, two_ref):
    feats, classes = one_ref.shape[0], two_ref.shape[0]
    one_ref[...] = full_ref[0:feats, :]
    two_ref[...] = full_ref[feats:feats + classes, :]
    loss_ref[...] = full_ref[feats + 8:feats + 9, 0:1]


def solution(mesh):
    num_dev = mesh.shape[GRAPH_AXIS]

    def params(cid=None):
        if cid is None:
            return pltpu.CompilerParams(vmem_limit_bytes=VMEM_BYTES)
        return pltpu.CompilerParams(vmem_limit_bytes=VMEM_BYTES, collective_id=cid, has_side_effects=True)

    def arr(dtype, *shape):
        return jax.ShapeDtypeStruct(shape, dtype)

    def scr(dtype, *shape):
        return pltpu.VMEM(shape, dtype)

    def dma(count):
        return pltpu.SemaphoreType.DMA((2, count))

    I32 = jnp.int32

    def device_step(node_feats, w_one, w_two, send_rows, edge_src, edge_dst, edge_w, labels, label_mask):
        rows, feats = node_feats.shape
        width = w_one.shape[1]
        halo = send_rows.shape[1]
        edges = edge_src.shape[0]
        own_hi, all_hi = rows // LANES, (rows + 2 * halo) // LANES
        feats_t, w2 = node_feats.T, w_two.T
        src2, dst2, ew2 = (a.reshape(edges // LANES, LANES) for a in (edge_src, edge_dst, edge_w))
        lab2, mask2 = labels.reshape(own_hi, LANES), label_mask.reshape(own_hi, LANES)
        listed = (LIST_ROWS, LANES)
        entries = LIST_ROWS * LANES

        own, halo_rows, count, lsrc, ldst, ltgt, lw, num = pl.pallas_call(
            functools.partial(k1_body, num_dev),
            out_shape=(arr(BF16, rows, width), arr(BF16, 2 * halo, width), arr(F32, 8, LANES), arr(I32, *listed),
                       arr(I32, *listed), arr(I32, *listed), arr(F32, *listed), arr(I32, 8, LANES)),
            in_specs=[vmem()] * 7, out_specs=(vmem(),) * 8,
            scratch_shapes=[scr(BF16, 2 * halo, width), scr(I32, 2, 2, halo), scr(F32, 8, LANES),
                            scr(F32, PLANE - 1, 8, LANES), scr(I32, edges // LANES, LANES), scr(F32, 8 * LIST_ROWS, LANES),
                            dma(4), dma(2), dma(PLANE - 1)],
            compiler_params=params(0), name="transform_and_halo",
        )(feats_t, w_one, send_rows, mask2, src2, dst2, ew2)

        hid, pos, tab = pl.pallas_call(
            k2_body,
            out_shape=(arr(BF16, rows, width), arr(BF16, rows, width), arr(F32, own_hi * CLASS_ROWS, LANES)),
            in_specs=[vmem(), vmem(), smem(), smem(), smem(), vmem(), vmem()], out_specs=(vmem(),) * 3,
            scratch_shapes=[scr(F32, 2 * (rows + 2 * halo), LANES), scr(F32, entries, LANES)]
            + [scr(F32, 2 * rows, LANES)] * NUM_BUFS,
            compiler_params=params(), name="aggregate_one",
        )(own, halo_rows, lsrc.reshape(entries), ldst.reshape(entries), num, lw, w2)

        num_z = num_dev // PLANE
        d_tab, misc, d_tab_halo, pos_halo, hdst, htgt, hw, hnum = pl.pallas_call(
            functools.partial(k3_body, num_dev),
            out_shape=(arr(BF16, own_hi * CLASS_ROWS, LANES), arr(F32, 16, width), arr(BF16, 2, own_hi * CLASS_ROWS, LANES),
                       arr(BF16, 2, rows, width), arr(I32, 2, *listed), arr(I32, 2, *listed), arr(F32, 2, *listed),
                       arr(I32, 2, 8, LANES)),
            in_specs=[vmem()] * 14, out_specs=(vmem(),) * 8,
            scratch_shapes=[scr(BF16, all_hi * CLASS_ROWS, LANES), scr(BF16, 2, 16, halo), scr(BF16, 2, 16, halo),
                            scr(F32, 2, CLASS_ROWS, halo), scr(F32, 2, CLASS_ROWS, halo), scr(F32, own_hi * 24, LANES),
                            scr(F32, all_hi * 24, LANES), scr(F32, own_hi * 24, LANES),
                            scr(BF16, 3 * own_hi * CLASS_ROWS, LANES), scr(F32, num_z - 1, 8, LANES),
                            dma(4), dma(num_z - 1), dma(10), dma(8)],
            compiler_params=params(1), name="layer_two",
        )(tab, send_rows, src2, dst2, ew2, lab2, mask2, count, hid, pos, ldst, ltgt, lw, num)

        def k4(own_take, own_put, own_num, own_w, p_take, p_put, p_num, p_w, n_take, n_put, n_num, n_w, *rest):
            k4_body((own_take, own_put, own_num, own_w), (p_take, p_put, p_num, p_w), (n_take, n_put, n_num, n_w), *rest)

        sum_rows_pad = 512
        part = pl.pallas_call(
            k4,
            out_shape=arr(F32, sum_rows_pad, width),
            in_specs=[smem(), smem(), smem(), vmem()] * 3 + [vmem()] * 7, out_specs=vmem(),
            scratch_shapes=[scr(F32, own_hi * CLASS_ROWS, LANES), scr(F32, 2 * rows, LANES), scr(F32, entries, LANES),
                            scr(BF16, rows, width)] + [scr(F32, 2 * rows, LANES)] * NUM_BUFS,
            compiler_params=params(), name="scatter_one",
        )(ldst.reshape(entries), ltgt.reshape(entries), num, lw,
          hdst[0].reshape(entries), htgt[0].reshape(entries), hnum[0], hw[0],
          hdst[1].reshape(entries), htgt[1].reshape(entries), hnum[1], hw[1],
          pos, pos_halo, d_tab, d_tab_halo, w2, feats_t, misc)

        n1, n2 = sum_rows_pad // 2, sum_rows_pad // 8
        n3 = n2 // num_z
        full = pl.pallas_call(
            functools.partial(k5_body, num_dev),
            out_shape=arr(F32, sum_rows_pad, width),
            in_specs=[vmem()], out_specs=vmem(),
            scratch_shapes=[scr(F32, n1, width), scr(F32, 3, n2, width), scr(F32, num_z - 1, n3, width),
                            scr(F32, n1, width), scr(F32, n2, width), dma(2 * (1 + 3 + num_z - 1))],
            compiler_params=params(2), name="sum_gradients",
        )(part)
        loss, grad_one, grad_two = pl.pallas_call(
            k6_body,
            out_shape=(arr(F32, 1, 1), arr(F32, feats, width), arr(F32, w2.shape[0], width)),
            in_specs=[vmem()], out_specs=(vmem(),) * 3, compiler_params=params(), name="outputs",
        )(full)
        return loss.reshape(()), grad_one, grad_two.T

    row_spec = P(GRAPH_AXIS)
    return jax.shard_map(device_step, mesh=mesh,
                         in_specs=(row_spec, P(), P(), row_spec, row_spec, row_spec, row_spec, row_spec, row_spec),
                         out_specs=(P(), P(), P()), check_vma=False)
```

```python
import functools

import jax
import jax.numpy as jnp
from jax import lax
from jax.experimental import pallas as pl
from jax.experimental.pallas import tpu as pltpu
from jax.sharding import PartitionSpec as P

GRAPH_AXIS = "graph"
MESH = pl.DeviceIdType.MESH
LANES = 128
CLASS_ROWS = 8
VMEM_BYTES = 60 * 2**20
F32 = jnp.float32
BF16 = jnp.bfloat16
NT = (((1,), (1,)), ((), ()))
TN = (((0,), (0,)), ((), ()))


def vmem():
    return pl.BlockSpec(memory_space=pltpu.VMEM)


def smem():
    return pl.BlockSpec(memory_space=pltpu.SMEM)


PLANE = 8
LIST_ROWS = 80
BLOCK = 32
NUM_BUFS = 4


def ring_peers(num_dev):
    me = lax.axis_index(GRAPH_AXIS)
    return me, (me + 1) % num_dev, (me + num_dev - 1) % num_dev


def layer_peers(me, num_dev):
    return [(me + PLANE * k) % num_dev for k in range(1, num_dev // PLANE)]


def class_weights(w_ref):
    w = w_ref[...]
    return jnp.concatenate([w, jnp.zeros((CLASS_ROWS - w.shape[0], w.shape[1]), F32)], axis=0).astype(BF16)


def meet(partners):
    barrier = pltpu.get_barrier_semaphore()
    for dev in partners:
        pl.semaphore_signal(barrier, inc=1, device_id=(dev,), device_id_type=MESH)
    pl.semaphore_wait(barrier, len(partners))


def remote(src, dst, sems, slot, dev):
    return pltpu.make_async_remote_copy(
        src_ref=src, dst_ref=dst, send_sem=sems.at[0, slot], recv_sem=sems.at[1, slot],
        device_id=(dev,), device_id_type=MESH)


def three_pieces(val):
    top = val.astype(BF16).astype(F32)
    rest = val - top
    mid = rest.astype(BF16).astype(F32)
    return top, mid, rest - mid


def wide_row(ref, first):
    blk = ref[pl.ds(first, 8), :]
    return jnp.concatenate([blk[j:j + 1, :] for j in range(8)], axis=1)


def lo_hot(idx):
    lo = idx & (LANES - 1)
    node = lax.broadcasted_iota(jnp.int32, (LANES, idx.shape[1]), 0)
    return (node == lo).astype(F32).astype(BF16)


def list_places(src_ref, w_ref, rows, halo, pos, num_ref):
    src, live = src_ref[...], w_ref[...] != 0.0
    n_rows = src.shape[0]
    tri = (lax.broadcasted_iota(jnp.int32, (LANES, LANES), 0) <= lax.broadcasted_iota(jnp.int32, (LANES, LANES), 1))
    tri = tri.astype(F32).astype(BF16)
    low = (lax.broadcasted_iota(jnp.int32, (n_rows, n_rows), 1) < lax.broadcasted_iota(jnp.int32, (n_rows, n_rows), 0))
    low = low.astype(F32).astype(BF16)
    place = jnp.full(src.shape, LIST_ROWS * LANES, jnp.int32)
    start = jnp.zeros((1, 1), jnp.int32)
    lane = lax.broadcasted_iota(jnp.int32, num_ref.shape, 1)
    num = jnp.zeros(num_ref.shape, jnp.int32)
    kinds = (src < rows, (src >= rows) & (src < rows + halo), src >= rows + halo)
    for k, kind in enumerate(kinds):
        kind = kind & live
        flag = kind.astype(F32)
        inner = jnp.dot(flag.astype(BF16), tri, preferred_element_type=F32)
        row_sum = jnp.broadcast_to(jnp.sum(flag, axis=1, keepdims=True), flag.shape)
        before = jnp.dot(low, row_sum.astype(BF16), preferred_element_type=F32)
        rank = (inner + before).astype(jnp.int32) - 1
        place = jnp.where(kind, start + rank, place)
        total = jnp.sum(jnp.sum(flag, axis=1, keepdims=True), axis=0, keepdims=True).astype(jnp.int32)
        blocks = lax.shift_right_logical(total + (BLOCK - 1), BLOCK.bit_length() - 1)
        start = start + blocks * BLOCK
        num = jnp.where(lane == k, blocks, num)
    pos[...] = place
    num_ref[...] = num


def k1_body(num_dev, xt_ref, w_ref, send_ref, mask_ref, src_ref, dst_ref, ew_ref,
            own_ref, halo_ref, cnt_ref, lsrc_ref, ldst_ref, ltgt_ref, lpair_ref, lw_ref, num_ref,
            own_t_b, stage, peer, cnt_send, cnt_recv, pos, acc, sems, peer_sems, cnt_sems):
    me, nxt, prv = ring_peers(num_dev)
    layer = [me - me % PLANE + (me % PLANE + k) % PLANE for k in range(1, PLANE)]
    meet([nxt, prv] + layer)
    rows = own_ref.shape[0]
    halo = send_ref.shape[1]
    total = jnp.sum(jnp.sum(mask_ref[...].astype(F32), axis=1, keepdims=True), axis=0, keepdims=True)
    cnt_send[...] = jnp.broadcast_to(total, cnt_send.shape)
    small = [remote(send_ref, peer.at[0], peer_sems, 0, nxt), remote(send_ref, peer.at[1], peer_sems, 1, prv)]
    small += [remote(cnt_send, cnt_recv.at[k], cnt_sems, k, dev) for k, dev in enumerate(layer)]
    for copy in small:
        copy.start()
    own_t = lax.dot_general(w_ref[...].astype(BF16), xt_ref[...], TN, preferred_element_type=F32)
    own_t_b[...] = own_t.astype(BF16)

    blocks = halo // LANES
    ids = jnp.concatenate([send_ref[r:r + 1, b * LANES:(b + 1) * LANES] for r in range(2) for b in range(blocks)], axis=0)
    ids_col = jnp.transpose(ids)
    node = lax.broadcasted_iota(jnp.int32, (LANES, rows), 1)
    copies = []
    half = halo // 2
    for part in range(2):
        for r in (1, 0):
            for b in range(part * blocks // 2, (part + 1) * blocks // 2):
                col = ids_col[:, r * blocks + b:r * blocks + b + 1]
                pick = (node == col).astype(F32).astype(BF16)
                stage[pl.ds(r * halo + b * LANES, LANES), :] = lax.dot_general(
                    pick, own_t_b[...], NT, preferred_element_type=F32).astype(BF16)
            dst_row = (1 - r) * halo + part * half
            copy = remote(stage.at[pl.ds(r * halo + part * half, half), :], halo_ref.at[pl.ds(dst_row, half), :],
                          sems, 2 * part + r, nxt if r == 1 else prv)
            copy.start()
            copies.append(copy)

    own_ref[...] = jnp.transpose(own_t_b[...])
    list_places(src_ref, ew_ref, rows, halo, pos, num_ref)
    for copy in small:
        copy.wait()
    for k in range(len(layer)):
        total = total + cnt_recv[k][0:1, 0:1]
    cnt_ref[...] = jnp.broadcast_to(total, cnt_ref.shape)
    theirs = jnp.concatenate([peer[s][1 - s:2 - s, b * LANES:(b + 1) * LANES] for s in range(2) for b in range(blocks)], axis=0)
    theirs = jnp.concatenate([lax.shift_right_logical(theirs, 4), theirs & 15], axis=0).astype(F32).astype(BF16)
    acc[...] = jnp.zeros_like(acc)

    def sort(i, carry):
        first = pl.multiple_of(i * 8, 8)
        src, dst, wgt, place = (wide_row(ref, first) for ref in (src_ref, dst_ref, ew_ref, pos))
        n = src.shape[1]
        at = jnp.maximum(src - rows, 0)
        cols = jnp.dot(theirs, lo_hot(at), preferred_element_type=F32)
        cols = cols[0:2 * blocks] * 16.0 + cols[2 * blocks:4 * blocks]
        mine = lax.broadcasted_iota(jnp.int32, cols.shape, 0) == lax.shift_right_logical(at, 7)
        tgt = jnp.sum(jnp.where(mine, cols, 0.0), axis=0, keepdims=True).astype(jnp.int32)
        tgt = jnp.where(src < rows, src, tgt)
        both = src + dst * 4096
        ints = [both & 255, lax.shift_right_logical(both, 8) & 255, lax.shift_right_logical(both, 16),
                tgt & 255, lax.shift_right_logical(tgt, 8)]
        cargo = [v.astype(F32) for v in ints] + list(three_pieces(wgt))
        here = lax.broadcasted_iota(jnp.int32, (LIST_ROWS, n), 0) == lax.shift_right_logical(place, 7)
        lhs = jnp.concatenate([jnp.where(here, v, 0.0).astype(BF16) for v in cargo], axis=0)
        acc[...] += lax.dot_general(lhs, lo_hot(place), NT, preferred_element_type=F32)
        return carry

    lax.fori_loop(0, src_ref.shape[0] // 8, sort, 0)
    got = [acc[p * LIST_ROWS:(p + 1) * LIST_ROWS, :] for p in range(8)]
    ints = [g.astype(jnp.int32) for g in got[:5]]
    both = ints[0] + ints[1] * 256 + ints[2] * 65536
    dst, tgt = lax.shift_right_logical(both, 12) * 2, (ints[3] + ints[4] * 256) * 2
    lsrc_ref[...] = (both & 4095) * 2
    ldst_ref[...] = dst
    ltgt_ref[...] = tgt
    lpair_ref[...] = dst + tgt * 65536
    lw_ref[...] = got[5] + got[6] + got[7]
    for copy in copies:
        copy.wait()


def spread_weights(w_ref, wide, first, last):
    def body(g, carry):
        cols = jnp.transpose(w_ref[pl.ds(pl.multiple_of(g * 8, 8), 8), :])
        for j in range(8):
            at = pl.ds(pl.multiple_of(g * 8 * LANES + j * LANES, LANES), LANES)
            wide[at, :] = jnp.broadcast_to(cols[:, j:j + 1], (LANES, LANES))
        return carry

    lax.fori_loop(first // 8, (last + 7) // 8, body, 0)


def clear_rows(bufs):
    def body(i, carry):
        for buf in bufs:
            buf[pl.ds(pl.multiple_of(i * 64, 64), 64), :] = jnp.zeros((64, LANES), F32)
        return carry

    lax.fori_loop(0, bufs[0].shape[0] // 64, body, 0)


def row_loop(take_ref, put_ref, wide, table, bufs, first, last):
    num = len(bufs)

    def step(i, carry):
        base = i * BLOCK
        for lead in range(0, BLOCK, num):
            take = [pl.multiple_of(take_ref[base + lead + j], 2) for j in range(num)]
            put = [pl.multiple_of(put_ref[base + lead + j], 2) for j in range(num)]
            vals = [wide[pl.ds(base + lead + j, 1), :] * table[pl.ds(take[j], 2), :] for j in range(num)]
            old = [bufs[j][pl.ds(put[j], 2), :] for j in range(num)]
            for j in range(num):
                bufs[j][pl.ds(put[j], 2), :] = old[j] + vals[j]
        return carry

    lax.fori_loop(first, last, step, 0)


def list_rows(first, last):
    return first * BLOCK // LANES, (last * BLOCK + LANES - 1) // LANES


def to_rows(blk, table, first_row):
    for h in range(2):
        table[pl.ds(2 * first_row + h, blk.shape[0], stride=2), :] = blk[:, h * LANES:(h + 1) * LANES]


def sum_rows(bufs, blk):
    halves = []
    for h in range(2):
        parts = [buf[pl.ds(2 * blk * LANES + h, LANES, stride=2), :] for buf in bufs]
        while len(parts) > 1:
            parts = [a + b for a, b in zip(parts[::2], parts[1::2])]
        halves.append(parts[0])
    return jnp.concatenate(halves, axis=1)


def k2_body(own_ref, halo_ref, lsrc_ref, ldst_ref, num_ref, lw_ref, w2_ref, hid_ref, pos_ref, tab_ref, table, wide, *bufs):
    end = num_ref[0, 0] + num_ref[0, 1] + num_ref[0, 2]
    spread_weights(lw_ref, wide, *list_rows(0, end))
    rows = own_ref.shape[0]

    def widen(i, carry):
        at = pl.ds(pl.multiple_of(i * LANES, LANES), LANES)
        to_rows(own_ref[at, :].astype(F32), table, i * LANES)
        to_rows(halo_ref[at, :].astype(F32), table, rows + i * LANES)
        return carry

    lax.fori_loop(0, rows // LANES, widen, 0)
    clear_rows(bufs)
    row_loop(lsrc_ref, ldst_ref, wide, table, bufs, 0, end)
    w2t = class_weights(w2_ref)

    def finish(i, carry):
        pre = sum_rows(bufs, i)
        hid = jnp.maximum(pre, 0.0).astype(BF16)
        at = pl.ds(pl.multiple_of(i * LANES, LANES), LANES)
        hid_ref[at, :] = hid
        pos_ref[at, :] = (pre > 0.0).astype(F32).astype(BF16)
        t2 = lax.dot_general(w2t, hid, NT, preferred_element_type=F32)
        tab_ref[pl.ds(pl.multiple_of(i * CLASS_ROWS, CLASS_ROWS), CLASS_ROWS), :] = t2.astype(BF16).astype(F32)
        return carry

    lax.fori_loop(0, rows // LANES, finish, 0)


def k4_body(own_list, prev_list, next_list, pos_own_ref, pos_prev_ref, pos_next_ref, dt_own_ref, dt_prev_ref, dt_next_ref,
            w2_ref, xt_ref, misc_ref,
            out_ref, tables, wide, d_tab, *bufs):
    w2t = class_weights(w2_ref).astype(F32)
    rows = pos_own_ref.shape[0]
    w2_all = jnp.concatenate([w2t] * (rows // LANES), axis=0)
    group = lax.shift_right_logical(lax.broadcasted_iota(jnp.int32, w2_all.shape, 0), 3)
    clear_rows(bufs)
    sides = ((own_list, dt_own_ref, pos_own_ref, 0), (prev_list, dt_prev_ref, pos_prev_ref, 2),
             (next_list, dt_next_ref, pos_next_ref, 1))
    for (take_ref, put_ref, num_ref, lw_ref), dt_ref, pos_ref, kind in sides:
        dt_cols = jnp.transpose(dt_ref[...].astype(F32)).astype(BF16)

        def widen(i, carry):
            d_hid = jnp.dot(dt_cols, jnp.where(group == i, w2_all, 0.0).astype(BF16), preferred_element_type=F32)
            at = pl.ds(pl.multiple_of(i * LANES, LANES), LANES)
            to_rows(jnp.where(pos_ref[at, :].astype(F32) > 0.0, d_hid, 0.0), tables, i * LANES)
            return carry

        lax.fori_loop(0, rows // LANES, widen, 0)
        first = 0
        for k in range(kind):
            first = first + num_ref[0, k]
        last = first + num_ref[0, kind]
        spread_weights(lw_ref, wide, *list_rows(first, last))
        row_loop(take_ref, put_ref, wide, tables, bufs, first, last)

    def finish(i, carry):
        d_tab[pl.ds(pl.multiple_of(i * LANES, LANES), LANES), :] = sum_rows(bufs, i).astype(BF16)
        return carry

    lax.fori_loop(0, rows // LANES, finish, 0)
    feats = xt_ref.shape[0]
    out_ref[0:feats, :] = jnp.dot(xt_ref[...], d_tab[...], preferred_element_type=F32)
    out_ref[feats:feats + 12, :] = misc_ref[0:12, :]


def hi_of(idx):
    return jnp.broadcast_to(lax.shift_right_logical(idx, 7), (CLASS_ROWS, idx.shape[1]))


def pick_cols(table_b, pieces, idx, hot):
    cols = jnp.dot(table_b, hot, preferred_element_type=F32)
    rows = table_b.shape[0] // pieces
    hi = hi_of(idx)
    out = jnp.zeros(hi.shape, F32)
    for h in range(rows // CLASS_ROWS):
        part = cols[h * CLASS_ROWS:(h + 1) * CLASS_ROWS]
        for p in range(1, pieces):
            part = part + cols[p * rows + h * CLASS_ROWS:p * rows + (h + 1) * CLASS_ROWS]
        out = out + jnp.where(hi == h, part, 0.0)
    return out


def add_cols(val, idx, hot, num_hi):
    hi = hi_of(idx)
    pieces = three_pieces(val)
    rows = []
    for h in range(0, num_hi, 2):
        both = [jnp.where(hi == h + k, p, 0.0) for k in range(2) for p in pieces]
        rows.append(jnp.concatenate(both, axis=0).astype(BF16))
    return lax.dot_general(jnp.concatenate(rows, axis=0), hot, NT, preferred_element_type=F32)


def join_pieces(acc, num_hi):
    out = []
    for h in range(num_hi):
        a = acc[h * 24:h * 24 + 24, :]
        out.append(a[0:8] + a[8:16] + a[16:24])
    return out


def stack_pieces(val):
    return jnp.concatenate(three_pieces(val), axis=0).astype(BF16)


def k3_body(num_dev, tab_ref, send_ref, src_ref, dst_ref, w_ref, lab_ref, mask_ref, cnt_ref, hid_ref, pos_ref,
            lpair_ref, lw_ref, num_ref,
            dt_ref, misc_ref, dt_prev_ref, dt_next_ref, pos_prev_ref, pos_next_ref, dst_prev_ref, dst_next_ref,
            tgt_prev_ref, tgt_next_ref, w_prev_ref, w_next_ref, num_prev_ref, num_next_ref, pairs,
            ext_b, fwd_send, fwd_recv, bwd_send, bwd_recv, acc_z, acc_s, acc_r, dz_b, cnt_recv,
            sems, cnt_sems, list_sems, pos_sems):
    me, nxt, prv = ring_peers(num_dev)
    layers = layer_peers(me, num_dev)
    meet([nxt, prv] + layers)
    counts = [remote(cnt_ref, cnt_recv.at[k], cnt_sems, k, dev) for k, dev in enumerate(layers)]
    for copy in counts:
        copy.start()
    late = []

    def send_late(pairs, pool, first):
        for k, (src, dst) in enumerate(pairs):
            for s, dev in enumerate((nxt, prv)):
                copy = remote(src, dst[s], pool, 2 * (first + k) + s, dev)
                copy.start()
                late.append(copy)

    chunk = pos_ref.shape[0] // 4

    def send_pos(q):
        at = pl.ds(q * chunk, chunk)
        send_late([(pos_ref.at[at, :], [pos_prev_ref.at[at, :], pos_next_ref.at[at, :]])], pos_sems, q)

    own_hi = tab_ref.shape[0] // CLASS_ROWS
    halo = send_ref.shape[1]
    halo_hi = halo // LANES
    all_hi = own_hi + 2 * halo_hi
    own_b = tab_ref[...].astype(BF16)
    ext_b[pl.ds(0, own_hi * CLASS_ROWS), :] = own_b
    hot_send = [lo_hot(send_ref[r:r + 1, :]) for r in range(2)]
    copies = []
    for r in (1, 0):
        val = pick_cols(own_b, 1, send_ref[r:r + 1, :], hot_send[r])
        fwd_send[r] = jnp.concatenate([val, jnp.zeros_like(val)], axis=0).astype(BF16)
        copy = remote(fwd_send.at[r], fwd_recv.at[1 - r], sems, r, nxt if r == 1 else prv)
        copy.start()
        copies.append(copy)
    send_late([(lpair_ref, [pairs.at[0], pairs.at[1]]), (lw_ref, [w_prev_ref, w_next_ref]),
               (num_ref, [num_prev_ref, num_next_ref])], list_sems, 0)
    send_pos(0)
    send_pos(1)
    acc_z[...] = jnp.zeros_like(acc_z)
    acc_s[...] = jnp.zeros_like(acc_s)
    for copy in copies:
        copy.wait()
    for r in range(2):
        got = fwd_recv[r].astype(F32)
        for j in range(0, halo_hi, 2):
            two = jnp.concatenate([got[0:8, (j + k) * LANES:(j + k + 1) * LANES] for k in range(2)], axis=0)
            ext_b[pl.ds((own_hi + r * halo_hi + j) * CLASS_ROWS, 16), :] = two.astype(BF16)

    steps = src_ref.shape[0] // 8

    def forward(i, carry):
        first = pl.multiple_of(i * 8, 8)
        src, dst = wide_row(src_ref, first), wide_row(dst_ref, first)
        val = pick_cols(ext_b[...], 1, src, lo_hot(src)) * wide_row(w_ref, first)
        acc_z[...] += add_cols(val, dst, lo_hot(dst), own_hi)
        return carry

    lax.fori_loop(0, steps, forward, 0)

    logits = join_pieces(acc_z[...], own_hi)
    cls = lax.broadcasted_iota(jnp.int32, (CLASS_ROWS, LANES), 0)
    count = cnt_ref[0:1, :]
    for k, copy in enumerate(counts):
        copy.wait()
        count = count + cnt_recv[k][0:1, :]
    count = jnp.maximum(count, 1.0)
    loss = jnp.zeros((1, LANES), F32)
    d_log = []
    for h in range(own_hi):
        z = jnp.where(cls < 7, logits[h], -jnp.inf)
        top = jnp.max(z, axis=0, keepdims=True)
        norm = jnp.log(jnp.sum(jnp.exp(z - top), axis=0, keepdims=True)) + top
        hot = cls == lab_ref[h:h + 1, :]
        mask = mask_ref[h:h + 1, :].astype(F32)
        picked = jnp.sum(jnp.where(hot, logits[h], 0.0), axis=0, keepdims=True)
        loss = loss + mask * (norm - picked)
        d_log.append((jnp.exp(z - norm) - hot.astype(F32)) * (mask / count))
    dz_b[...] = stack_pieces(jnp.concatenate(d_log, axis=0))

    def backward(i, carry):
        first = pl.multiple_of(i * 8, 8)
        src, dst = wide_row(src_ref, first), wide_row(dst_ref, first)
        val = pick_cols(dz_b[...], 3, dst, lo_hot(dst)) * wide_row(w_ref, first)
        acc_s[...] += add_cols(val, src, lo_hot(src), all_hi)
        return carry

    lax.fori_loop(0, steps, backward, 0)

    d_ext = join_pieces(acc_s[...], all_hi)
    copies = []
    for r in range(2):
        for j in range(halo_hi):
            bwd_send[r, :, j * LANES:(j + 1) * LANES] = d_ext[own_hi + r * halo_hi + j]
        copy = remote(bwd_send.at[r], bwd_recv.at[1 - r], sems, 2 + r, prv if r == 0 else nxt)
        copy.start()
        copies.append(copy)
    send_pos(2)
    for copy in copies:
        copy.wait()
    for r in range(2):
        part = add_cols(bwd_recv[r], send_ref[r:r + 1, :], hot_send[r], own_hi)
        acc_r[...] = part if r == 0 else acc_r[...] + part
    back = join_pieces(acc_r[...], own_hi)
    d_tab = [d_ext[h] + back[h] for h in range(own_hi)]
    dt_ref[...] = jnp.concatenate(d_tab, axis=0).astype(BF16)
    send_late([(dt_ref, [dt_prev_ref, dt_next_ref])], list_sems, 3)
    send_pos(3)
    grad = jnp.zeros((CLASS_ROWS, hid_ref.shape[1]), F32)
    for h in range(own_hi):
        grad = grad + jnp.dot(d_tab[h].astype(BF16), hid_ref[pl.ds(h * LANES, LANES), :], preferred_element_type=F32)
    misc_ref[0:8, :] = grad
    total = jnp.sum(loss, axis=1, keepdims=True) / count[:, 0:1]
    misc_ref[8:16, :] = jnp.broadcast_to(total, (8, misc_ref.shape[1]))
    for copy in late:
        copy.wait()
    for s, (dst_ref_, tgt_ref_) in enumerate(((dst_prev_ref, tgt_prev_ref), (dst_next_ref, tgt_next_ref))):
        dst_ref_[...] = pairs[s] & 0xFFFF
        tgt_ref_[...] = lax.shift_right_logical(pairs[s], 16)


def k5_body(num_dev, part_ref, full_ref, land_core, land_chip, land_z, by_core, by_chip, sems):
    me = lax.axis_index(GRAPH_AXIS)
    core, chip, z = me % 2, (me // 2) % 4, me // PLANE
    other = me + 1 - 2 * core
    chips = [me + 2 * ((chip + k) % 4 - chip) for k in range(1, 4)]
    layers = layer_peers(me, num_dev)
    num_z = num_dev // PLANE
    meet([other] + chips + layers)
    rows, width = part_ref.shape
    n1, n2, n3 = rows // 2, rows // 8, rows // 8 // num_z
    parts = [pl.ds(c * LANES, LANES) for c in range(width // LANES)]
    used = [0]

    def send(pairs):
        out = []
        for src, dst, dev in pairs:
            out.append(remote(src, dst, sems, used[0], dev))
            used[0] += 1
        for copy in out:
            copy.start()
        return out

    def wait(copies):
        for copy in copies:
            copy.wait()

    def at(first, size):
        return pl.ds(pl.multiple_of(first, size), size)

    flying = [send([(part_ref.at[at((1 - core) * n1, n1), c], land_core.at[:, c], other)]) for c in parts]
    for i, c in enumerate(parts):
        wait(flying[i])
        by_core[:, c] = part_ref[at(core * n1, n1), c] + land_core[:, c]
        flying[i] = send([(by_core.at[at((chip + k + 1) % 4 * n2, n2), c], land_chip.at[k, :, c], dev)
                          for k, dev in enumerate(chips)])
    for i, c in enumerate(parts):
        wait(flying[i])
        total = by_core[at(chip * n2, n2), c]
        for k in range(len(chips)):
            total = total + land_chip[k, :, c]
        by_chip[:, c] = total
        flying[i] = send([(by_chip.at[at((z + k + 1) % num_z * n3, n3), c], land_z.at[k, :, c], dev)
                          for k, dev in enumerate(layers)])
    first = core * n1 + chip * n2 + z * n3
    gathers = ((first, n3, layers), (core * n1 + chip * n2, n2, chips), (core * n1, n1, [other]))

    def gather(level, c):
        first, size, devs = gathers[level]
        own = full_ref.at[at(first, size), c]
        return send([(own, own, dev) for dev in devs])

    for i, c in enumerate(parts):
        wait(flying[i])
        total = by_chip[at(z * n3, n3), c]
        for k in range(len(layers)):
            total = total + land_z[k, :, c]
        full_ref[at(first, n3), c] = total
        flying[i] = gather(0, c)
    for level in (1, 2):
        for i, c in enumerate(parts):
            wait(flying[i])
            flying[i] = gather(level, c)
    for copies in flying:
        wait(copies)


def k6_body(full_ref, loss_ref, one_ref, two_ref):
    feats, classes = one_ref.shape[0], two_ref.shape[0]
    one_ref[...] = full_ref[0:feats, :]
    two_ref[...] = full_ref[feats:feats + classes, :]
    loss_ref[...] = full_ref[feats + 8:feats + 9, 0:1]


def solution(mesh):
    num_dev = mesh.shape[GRAPH_AXIS]

    def params(cid=None):
        if cid is None:
            return pltpu.CompilerParams(vmem_limit_bytes=VMEM_BYTES)
        return pltpu.CompilerParams(vmem_limit_bytes=VMEM_BYTES, collective_id=cid, has_side_effects=True)

    def arr(dtype, *shape):
        return jax.ShapeDtypeStruct(shape, dtype)

    def scr(dtype, *shape):
        return pltpu.VMEM(shape, dtype)

    def dma(count):
        return pltpu.SemaphoreType.DMA((2, count))

    I32 = jnp.int32

    def device_step(node_feats, w_one, w_two, send_rows, edge_src, edge_dst, edge_w, labels, label_mask):
        rows, feats = node_feats.shape
        width = w_one.shape[1]
        halo = send_rows.shape[1]
        edges = edge_src.shape[0]
        own_hi, all_hi = rows // LANES, (rows + 2 * halo) // LANES
        feats_t, w2 = node_feats.T, w_two.T
        src2, dst2, ew2 = (a.reshape(edges // LANES, LANES) for a in (edge_src, edge_dst, edge_w))
        lab2, mask2 = labels.reshape(own_hi, LANES), label_mask.reshape(own_hi, LANES)
        listed = (LIST_ROWS, LANES)
        entries = LIST_ROWS * LANES

        own, halo_rows, count, lsrc, ldst, ltgt, lpair, lw, num = pl.pallas_call(
            functools.partial(k1_body, num_dev),
            out_shape=(arr(BF16, rows, width), arr(BF16, 2 * halo, width), arr(F32, 8, LANES), arr(I32, *listed),
                       arr(I32, *listed), arr(I32, *listed), arr(I32, *listed), arr(F32, *listed), arr(I32, 8, LANES)),
            in_specs=[vmem()] * 7, out_specs=(vmem(),) * 9,
            scratch_shapes=[scr(BF16, width, rows), scr(BF16, 2 * halo, width), scr(I32, 2, 2, halo), scr(F32, 8, LANES),
                            scr(F32, PLANE - 1, 8, LANES), scr(I32, edges // LANES, LANES), scr(F32, 8 * LIST_ROWS, LANES),
                            dma(4), dma(2), dma(PLANE - 1)],
            compiler_params=params(0), name="transform_and_halo",
        )(feats_t, w_one, send_rows, mask2, src2, dst2, ew2)

        hid, pos, tab = pl.pallas_call(
            k2_body,
            out_shape=(arr(BF16, rows, width), arr(BF16, rows, width), arr(F32, own_hi * CLASS_ROWS, LANES)),
            in_specs=[vmem(), vmem(), smem(), smem(), smem(), vmem(), vmem()], out_specs=(vmem(),) * 3,
            scratch_shapes=[scr(F32, 2 * (rows + 2 * halo), LANES), scr(F32, entries, LANES)]
            + [scr(F32, 2 * rows, LANES)] * NUM_BUFS,
            compiler_params=params(), name="aggregate_one",
        )(own, halo_rows, lsrc.reshape(entries), ldst.reshape(entries), num, lw, w2)

        num_z = num_dev // PLANE
        tab_b = arr(BF16, own_hi * CLASS_ROWS, LANES)
        (d_tab, misc, d_prev, d_next, pos_prev, pos_next, dst_prev, dst_next, tgt_prev, tgt_next, w_prev, w_next,
         num_prev, num_next) = pl.pallas_call(
            functools.partial(k3_body, num_dev),
            out_shape=(tab_b, arr(F32, 16, width), tab_b, tab_b, arr(BF16, rows, width), arr(BF16, rows, width),
                       arr(I32, *listed), arr(I32, *listed), arr(I32, *listed), arr(I32, *listed),
                       arr(F32, *listed), arr(F32, *listed), arr(I32, 8, LANES), arr(I32, 8, LANES)),
            in_specs=[vmem()] * 13, out_specs=(vmem(),) * 14,
            scratch_shapes=[scr(I32, 2, *listed), scr(BF16, all_hi * CLASS_ROWS, LANES), scr(BF16, 2, 16, halo),
                            scr(BF16, 2, 16, halo), scr(F32, 2, CLASS_ROWS, halo), scr(F32, 2, CLASS_ROWS, halo),
                            scr(F32, own_hi * 24, LANES), scr(F32, all_hi * 24, LANES), scr(F32, own_hi * 24, LANES),
                            scr(BF16, 3 * own_hi * CLASS_ROWS, LANES), scr(F32, num_z - 1, 8, LANES),
                            dma(4), dma(num_z - 1), dma(8), dma(8)],
            compiler_params=params(1), name="layer_two",
        )(tab, send_rows, src2, dst2, ew2, lab2, mask2, count, hid, pos, lpair, lw, num)

        def k4(own_take, own_put, own_num, own_w, p_take, p_put, p_num, p_w, n_take, n_put, n_num, n_w, *rest):
            k4_body((own_take, own_put, own_num, own_w), (p_take, p_put, p_num, p_w), (n_take, n_put, n_num, n_w), *rest)

        sum_rows_pad = 512
        part = pl.pallas_call(
            k4,
            out_shape=arr(F32, sum_rows_pad, width),
            in_specs=[smem(), smem(), smem(), vmem()] * 3 + [vmem()] * 9, out_specs=vmem(),
            scratch_shapes=[scr(F32, 2 * rows, LANES), scr(F32, entries, LANES), scr(BF16, rows, width)] + [scr(F32, 2 * rows, LANES)] * NUM_BUFS,
            compiler_params=params(), name="scatter_one",
        )(ldst.reshape(entries), ltgt.reshape(entries), num, lw,
          dst_prev.reshape(entries), tgt_prev.reshape(entries), num_prev, w_prev,
          dst_next.reshape(entries), tgt_next.reshape(entries), num_next, w_next,
          pos, pos_prev, pos_next, d_tab, d_prev, d_next, w2, feats_t, misc)

        n1, n2 = sum_rows_pad // 2, sum_rows_pad // 8
        n3 = n2 // num_z
        full = pl.pallas_call(
            functools.partial(k5_body, num_dev),
            out_shape=arr(F32, sum_rows_pad, width),
            in_specs=[vmem()], out_specs=vmem(),
            scratch_shapes=[scr(F32, n1, width), scr(F32, 3, n2, width), scr(F32, num_z - 1, n3, width),
                            scr(F32, n1, width), scr(F32, n2, width), dma(4 * (1 + 3 + num_z - 1))],
            compiler_params=params(2), name="sum_gradients",
        )(part)
        loss, grad_one, grad_two = pl.pallas_call(
            k6_body,
            out_shape=(arr(F32, 1, 1), arr(F32, feats, width), arr(F32, w2.shape[0], width)),
            in_specs=[vmem()], out_specs=(vmem(),) * 3, compiler_params=params(), name="outputs",
        )(full)
        return loss.reshape(()), grad_one, grad_two.T

    row_spec = P(GRAPH_AXIS)
    return jax.shard_map(device_step, mesh=mesh,
                         in_specs=(row_spec, P(), P(), row_spec, row_spec, row_spec, row_spec, row_spec, row_spec),
                         out_specs=(P(), P(), P()), check_vma=False)
```

```python
import functools

import jax
import jax.numpy as jnp
from jax import lax
from jax.experimental import pallas as pl
from jax.experimental.pallas import tpu as pltpu
from jax.sharding import PartitionSpec as P

GRAPH_AXIS = "graph"
MESH = pl.DeviceIdType.MESH
LANES = 128
CLASS_ROWS = 8
VMEM_BYTES = 28 * 2**20
F32 = jnp.float32
BF16 = jnp.bfloat16
NT = (((1,), (1,)), ((), ()))
TN = (((0,), (0,)), ((), ()))


def vmem():
    return pl.BlockSpec(memory_space=pltpu.VMEM)


def hbm():
    return pl.BlockSpec(memory_space=pl.ANY)


def smem():
    return pl.BlockSpec(memory_space=pltpu.SMEM)


PLANE = 8
LIST_ROWS = 80
BLOCK = 128
NUM_BUFS = 4
CHUNK = 1024


def ring_peers(num_dev):
    me = lax.axis_index(GRAPH_AXIS)
    return me, (me + 1) % num_dev, (me + num_dev - 1) % num_dev


def layer_peers(me, num_dev):
    return [(me + PLANE * k) % num_dev for k in range(1, num_dev // PLANE)]


def class_weights(w_ref):
    w = w_ref[...]
    return jnp.concatenate([w, jnp.zeros((CLASS_ROWS - w.shape[0], w.shape[1]), F32)], axis=0).astype(BF16)


def meet(partners):
    barrier = pltpu.get_barrier_semaphore()
    for dev in partners:
        pl.semaphore_signal(barrier, inc=1, device_id=(dev,), device_id_type=MESH)
    pl.semaphore_wait(barrier, len(partners))


def remote(src, dst, sems, slot, dev):
    return pltpu.make_async_remote_copy(
        src_ref=src, dst_ref=dst, send_sem=sems.at[0, slot], recv_sem=sems.at[1, slot],
        device_id=(dev,), device_id_type=MESH)


def three_pieces(val):
    top = val.astype(BF16).astype(F32)
    rest = val - top
    mid = rest.astype(BF16).astype(F32)
    return top, mid, rest - mid


def wide_row(ref, first):
    blk = ref[pl.ds(first, 8), :]
    return jnp.concatenate([blk[j:j + 1, :] for j in range(8)], axis=1)


def lo_hot(idx):
    lo = idx & (LANES - 1)
    node = lax.broadcasted_iota(jnp.int32, (LANES, idx.shape[1]), 0)
    return (node == lo).astype(F32).astype(BF16)


def list_places(src_ref, w_ref, rows, halo, pos, num_ref):
    src, live = src_ref[...], w_ref[...] != 0.0
    n_rows = src.shape[0]
    tri = (lax.broadcasted_iota(jnp.int32, (LANES, LANES), 0) <= lax.broadcasted_iota(jnp.int32, (LANES, LANES), 1))
    tri = tri.astype(F32).astype(BF16)
    low = (lax.broadcasted_iota(jnp.int32, (n_rows, n_rows), 1) < lax.broadcasted_iota(jnp.int32, (n_rows, n_rows), 0))
    low = low.astype(F32).astype(BF16)
    place = jnp.full(src.shape, LIST_ROWS * LANES, jnp.int32)
    start = jnp.zeros((1, 1), jnp.int32)
    lane = lax.broadcasted_iota(jnp.int32, num_ref.shape, 1)
    num = jnp.zeros(num_ref.shape, jnp.int32)
    kinds = (src < rows, (src >= rows) & (src < rows + halo), src >= rows + halo)
    for k, kind in enumerate(kinds):
        kind = kind & live
        flag = kind.astype(F32)
        inner = jnp.dot(flag.astype(BF16), tri, preferred_element_type=F32)
        row_sum = jnp.broadcast_to(jnp.sum(flag, axis=1, keepdims=True), flag.shape)
        before = jnp.dot(low, row_sum.astype(BF16), preferred_element_type=F32)
        rank = (inner + before).astype(jnp.int32) - 1
        place = jnp.where(kind, start + rank, place)
        total = jnp.sum(jnp.sum(flag, axis=1, keepdims=True), axis=0, keepdims=True).astype(jnp.int32)
        blocks = lax.shift_right_logical(total + (BLOCK - 1), BLOCK.bit_length() - 1)
        start = start + blocks * BLOCK
        num = jnp.where(lane == k, blocks, num)
    pos[...] = place
    num_ref[...] = num


def k1_body(xt_hbm, w_hbm, send_hbm, own_t_ref, to_next_ref, to_prev_ref, xt_ref, w_ref, send_ref, sems):
    copies = [pltpu.make_async_copy(a, b, sems.at[k])
              for k, (a, b) in enumerate(((send_hbm, send_ref), (w_hbm, w_ref), (xt_hbm, xt_ref)))]
    for copy in copies:
        copy.start()
    copies[0].wait()
    halo = send_ref.shape[1]
    rows = xt_ref.shape[1]
    blocks = halo // LANES
    ids = jnp.concatenate([send_ref[r:r + 1, b * LANES:(b + 1) * LANES] for r in range(2) for b in range(blocks)], axis=0)
    ids_col = jnp.transpose(ids)
    copies[1].wait()
    w_b = w_ref[...].astype(BF16)
    copies[2].wait()
    own_t_ref[...] = lax.dot_general(w_b, xt_ref[...], TN, preferred_element_type=F32).astype(BF16)
    node = lax.broadcasted_iota(jnp.int32, (LANES, rows), 1)
    for r, out in ((1, to_next_ref), (0, to_prev_ref)):
        for b in range(blocks):
            pick = (node == ids_col[:, r * blocks + b:r * blocks + b + 1]).astype(F32).astype(BF16)
            out[b * LANES:(b + 1) * LANES, :] = lax.dot_general(
                pick, own_t_ref[...], NT, preferred_element_type=F32).astype(BF16)


def sort_edges(src_ref, dst_ref, ew_ref, rows, halo, pos, acc, lsrc_ref, ldst_ref, lpair_ref, lw_ref, num_ref):
    list_places(src_ref, ew_ref, rows, halo, pos, num_ref)
    acc[...] = jnp.zeros_like(acc)

    def sort(i, carry):
        first = pl.multiple_of(i * 8, 8)
        src, dst, wgt, place = (wide_row(ref, first) for ref in (src_ref, dst_ref, ew_ref, pos))
        both = src + dst * 4096
        ints = [both & 255, lax.shift_right_logical(both, 8) & 255, lax.shift_right_logical(both, 16)]
        cargo = [v.astype(F32) for v in ints] + list(three_pieces(wgt))
        here = lax.broadcasted_iota(jnp.int32, (LIST_ROWS, src.shape[1]), 0) == lax.shift_right_logical(place, 7)
        lhs = jnp.concatenate([jnp.where(here, v, 0.0).astype(BF16) for v in cargo], axis=0)
        acc[...] += lax.dot_general(lhs, lo_hot(place), NT, preferred_element_type=F32)
        return carry

    lax.fori_loop(0, src_ref.shape[0] // 8, sort, 0)
    got = [acc[p * LIST_ROWS:(p + 1) * LIST_ROWS, :] for p in range(6)]
    ints = [g.astype(jnp.int32) for g in got[:3]]
    both = ints[0] + ints[1] * 256 + ints[2] * 65536
    src, dst = both & 4095, lax.shift_right_logical(both, 12) * 2
    src = jnp.where(src < rows, src, src - rows)
    lsrc_ref[...] = src * 2
    ldst_ref[...] = dst
    lpair_ref[...] = dst + src * 65536
    lw_ref[...] = got[3] + got[4] + got[5]


def spread_weights(w_ref, wide, first, last):
    def body(g, carry):
        cols = jnp.transpose(w_ref[pl.ds(pl.multiple_of(g * 8, 8), 8), :])
        for j in range(8):
            at = pl.ds(pl.multiple_of(g * 8 * LANES + j * LANES, LANES), LANES)
            wide[at, :] = jnp.broadcast_to(cols[:, j:j + 1], (LANES, LANES))
        return carry

    lax.fori_loop(first // 8, (last + 7) // 8, body, 0)


def clear_rows(bufs):
    def body(i, carry):
        for buf in bufs:
            buf[pl.ds(pl.multiple_of(i * 64, 64), 64), :] = jnp.zeros((64, LANES), F32)
        return carry

    lax.fori_loop(0, bufs[0].shape[0] // 64, body, 0)


def chunk_copies(lists, fast, sems, c):
    at = pl.ds(pl.multiple_of(c * 8, 8), CHUNK // LANES)
    return [pltpu.make_async_copy(a.at[at, :], b.at[at, :], sems.at[k, c]) for k, (a, b) in enumerate(zip(lists, fast))]


def chunks_of(first, last):
    per = CHUNK // BLOCK
    return first // per, (last + per - 1) // per


def start_lists(lists, fast, sems, first, last):
    def body(c, carry):
        for copy in chunk_copies(lists, fast, sems, c):
            copy.start()
        return carry

    lax.fori_loop(*chunks_of(first, last), body, 0)


def row_loop(lists, fast, sems, wide, table, bufs, first, last, rename=None):
    num = len(bufs)
    take_ref, put_ref = fast
    per = CHUNK // BLOCK

    def step(i, carry):
        base = i * BLOCK
        for lead in range(0, BLOCK, num):
            take = [pl.multiple_of(take_ref[i, lead + j], 2) for j in range(num)]
            put = [put_ref[i, lead + j] for j in range(num)]
            if rename is not None:
                put = [rename[p] for p in put]
            put = [pl.multiple_of(p, 2) for p in put]
            vals = [wide[pl.ds(base + lead + j, 1), :] * table[pl.ds(take[j], 2), :] for j in range(num)]
            old = [bufs[j][pl.ds(put[j], 2), :] for j in range(num)]
            for j in range(num):
                bufs[j][pl.ds(put[j], 2), :] = old[j] + vals[j]
        return carry

    def chunk(c, carry):
        for copy in chunk_copies(lists, fast, sems, c):
            copy.wait()
        return lax.fori_loop(jnp.maximum(first, c * per), jnp.minimum(last, c * per + per), step, carry)

    lax.fori_loop(*chunks_of(first, last), chunk, 0)


def list_rows(first, last):
    return first * BLOCK // LANES, (last * BLOCK + LANES - 1) // LANES


def to_rows(blk, table, first_row):
    for h in range(2):
        table[pl.ds(2 * first_row + h, blk.shape[0], stride=2), :] = blk[:, h * LANES:(h + 1) * LANES]


def sum_rows(bufs, blk):
    halves = []
    for h in range(2):
        parts = [buf[pl.ds(2 * blk * LANES + h, LANES, stride=2), :] for buf in bufs]
        while len(parts) > 1:
            parts = [a + b for a, b in zip(parts[::2], parts[1::2])]
        halves.append(parts[0])
    return jnp.concatenate(halves, axis=1)


def k2a_body(own_t_ref, src_ref, dst_ref, ew_ref, part_ref, lsrc_ref, ldst_ref, lpair_ref, lw_ref, num_ref,
             pos, acc, table, wide, num_fast, src_fast, dst_fast, num_sem, sems, *bufs):
    rows = part_ref.shape[0]
    sort_edges(src_ref, dst_ref, ew_ref, rows, rows // 2, pos, acc, lsrc_ref, ldst_ref, lpair_ref, lw_ref, num_ref)

    def widen(i, carry):
        at = pl.ds(pl.multiple_of(i * LANES, LANES), LANES)
        to_rows(jnp.transpose(own_t_ref[:, at].astype(F32)), table, i * LANES)
        return carry

    lax.fori_loop(0, rows // LANES, widen, 0)
    clear_rows(bufs)
    copy = pltpu.make_async_copy(num_ref, num_fast, num_sem)
    copy.start()
    copy.wait()
    end = num_fast[0, 0]
    lists, fast = (lsrc_ref, ldst_ref), (src_fast, dst_fast)
    start_lists(lists, fast, sems, 0, end)
    spread_weights(lw_ref, wide, *list_rows(0, end))
    row_loop(lists, fast, sems, wide, table, bufs, 0, end)

    def finish(i, carry):
        part_ref[pl.ds(pl.multiple_of(i * LANES, LANES), LANES), :] = sum_rows(bufs, i)
        return carry

    lax.fori_loop(0, rows // LANES, finish, 0)


def k2b_body(part_ref, prev_ref, next_ref, lsrc_ref, ldst_ref, num_ref, lw_ref, w2_ref,
             hid_ref, pos_a_ref, pos_b_ref, tab_ref, table, wide, src_fast, dst_fast, sems, *bufs):
    first = num_ref[0, 0]
    end = first + num_ref[0, 1] + num_ref[0, 2]
    lists, fast = (lsrc_ref, ldst_ref), (src_fast, dst_fast)
    start_lists(lists, fast, sems, first, end)
    spread_weights(lw_ref, wide, *list_rows(first, end))
    halo = prev_ref.shape[0]

    def widen(i, carry):
        at = pl.ds(pl.multiple_of(i * LANES, LANES), LANES)
        to_rows(prev_ref[at, :].astype(F32), table, i * LANES)
        to_rows(next_ref[at, :].astype(F32), table, halo + i * LANES)
        return carry

    lax.fori_loop(0, halo // LANES, widen, 0)
    clear_rows(bufs)
    row_loop(lists, fast, sems, wide, table, bufs, first, end)
    w2t = class_weights(w2_ref)

    for side, pos_ref in enumerate((pos_a_ref, pos_b_ref)):
        lead = side * pos_ref.shape[0] // LANES

        def finish(j, carry):
            i = lead + j
            at = pl.ds(pl.multiple_of(i * LANES, LANES), LANES)
            pre = part_ref[at, :] + sum_rows(bufs, i)
            hid = jnp.maximum(pre, 0.0).astype(BF16)
            hid_ref[at, :] = hid
            pos_ref[pl.ds(pl.multiple_of(j * LANES, LANES), LANES), :] = (pre > 0.0).astype(F32).astype(BF16)
            t2 = lax.dot_general(w2t, hid, NT, preferred_element_type=F32)
            tab_ref[pl.ds(pl.multiple_of(i * CLASS_ROWS, CLASS_ROWS), CLASS_ROWS), :] = t2.astype(BF16).astype(F32)
            return carry

        lax.fori_loop(0, pos_ref.shape[0] // LANES, finish, 0)


def stack_classes(w2_ref, blocks):
    w2_all = jnp.concatenate([class_weights(w2_ref).astype(F32)] * blocks, axis=0)
    return w2_all, lax.shift_right_logical(lax.broadcasted_iota(jnp.int32, w2_all.shape, 0), 3)


def fill_table(dt_ref, pos_refs, w2_all, group, table):
    dt_cols = jnp.transpose(dt_ref[...].astype(F32)).astype(BF16)
    for side, pos_ref in enumerate(pos_refs):
        lead = side * pos_ref.shape[0] // LANES

        def widen(j, carry):
            i = lead + j
            d_hid = jnp.dot(dt_cols, jnp.where(group == i, w2_all, 0.0).astype(BF16), preferred_element_type=F32)
            at = pl.ds(pl.multiple_of(j * LANES, LANES), LANES)
            to_rows(jnp.where(pos_ref[at, :].astype(F32) > 0.0, d_hid, 0.0), table, i * LANES)
            return carry

        lax.fori_loop(0, pos_ref.shape[0] // LANES, widen, 0)


def k4a_body(ldst_ref, lsrc_ref, num_ref, lw_ref, pos_a_ref, pos_b_ref, dt_ref, w2_ref, part_ref,
             table, wide, take_fast, put_fast, sems, *bufs):
    rows = part_ref.shape[0]
    lists, fast, end = (ldst_ref, lsrc_ref), (take_fast, put_fast), num_ref[0, 0]
    start_lists(lists, fast, sems, 0, end)
    w2_all, group = stack_classes(w2_ref, rows // LANES)
    clear_rows(bufs)
    fill_table(dt_ref, (pos_a_ref, pos_b_ref), w2_all, group, table)
    spread_weights(lw_ref, wide, *list_rows(0, end))
    row_loop(lists, fast, sems, wide, table, bufs, 0, end)

    def finish(i, carry):
        part_ref[pl.ds(pl.multiple_of(i * LANES, LANES), LANES), :] = sum_rows(bufs, i)
        return carry

    lax.fori_loop(0, rows // LANES, finish, 0)


def k4b_body(part_ref, num_ref, names_ref, prev_dst, prev_src, prev_w, next_dst, next_src, next_w,
             prev_dt, prev_a, prev_b, next_dt, next_a, next_b, w2_ref, xt_ref, misc_ref, out_ref,
             table, wide, d_tab, *rest):
    fasts, pools, bufs = (rest[0:2], rest[2:4]), rest[4:6], rest[6:]
    rows = part_ref.shape[0]
    sides = (((prev_dst, prev_src), prev_w, prev_dt, (prev_a, prev_b), 1, 2),
             ((next_dst, next_src), next_w, next_dt, (next_a, next_b), 2, 1))
    spans = []
    for (lists, _, _, _, row, kind), fast, pool in zip(sides, fasts, pools):
        first = num_ref[row, 0]
        if kind == 2:
            first = first + num_ref[row, 1]
        spans.append((first, first + num_ref[row, kind]))
        start_lists(lists, fast, pool, *spans[-1])
    w2_all, group = stack_classes(w2_ref, rows // LANES)
    clear_rows(bufs)
    for (lists, w_ref, dt_ref, pos_refs, _, _), fast, pool, span in zip(sides, fasts, pools, spans):
        fill_table(dt_ref, pos_refs, w2_all, group, table)
        spread_weights(w_ref, wide, *list_rows(*span))
        row_loop(lists, fast, pool, wide, table, bufs, *span, rename=names_ref)

    def finish(i, carry):
        at = pl.ds(pl.multiple_of(i * LANES, LANES), LANES)
        d_tab[at, :] = (part_ref[at, :] + sum_rows(bufs, i)).astype(BF16)
        return carry

    lax.fori_loop(0, rows // LANES, finish, 0)
    feats = xt_ref.shape[0]
    out_ref[0:feats, :] = jnp.dot(xt_ref[...], d_tab[...], preferred_element_type=F32)
    out_ref[feats:feats + 12, :] = misc_ref[0:12, :]


def hi_of(idx):
    return jnp.broadcast_to(lax.shift_right_logical(idx, 7), (CLASS_ROWS, idx.shape[1]))


def pick_cols(table_b, pieces, idx, hot):
    cols = jnp.dot(table_b, hot, preferred_element_type=F32)
    rows = table_b.shape[0] // pieces
    hi = hi_of(idx)
    out = jnp.zeros(hi.shape, F32)
    for h in range(rows // CLASS_ROWS):
        part = cols[h * CLASS_ROWS:(h + 1) * CLASS_ROWS]
        for p in range(1, pieces):
            part = part + cols[p * rows + h * CLASS_ROWS:p * rows + (h + 1) * CLASS_ROWS]
        out = out + jnp.where(hi == h, part, 0.0)
    return out


def add_cols(val, idx, hot, num_hi):
    hi = hi_of(idx)
    pieces = three_pieces(val)
    rows = []
    for h in range(0, num_hi, 2):
        both = [jnp.where(hi == h + k, p, 0.0) for k in range(2) for p in pieces]
        rows.append(jnp.concatenate(both, axis=0).astype(BF16))
    return lax.dot_general(jnp.concatenate(rows, axis=0), hot, NT, preferred_element_type=F32)


def join_pieces(acc, num_hi):
    out = []
    for h in range(num_hi):
        a = acc[h * 24:h * 24 + 24, :]
        out.append(a[0:8] + a[8:16] + a[16:24])
    return out


def stack_pieces(val):
    return jnp.concatenate(three_pieces(val), axis=0).astype(BF16)


def k3_body(num_dev, tab_ref, send_ref, src_ref, dst_ref, w_ref, lab_ref, mask_ref, hid_ref, pos_ref,
            lpair_ref, lw_ref, num_ref,
            dt_ref, misc_ref, dt_prev_ref, dt_next_ref, pos_prev_ref, pos_next_ref, dst_prev_ref, dst_next_ref,
            put_prev_ref, put_next_ref, w_prev_ref, w_next_ref, nums_ref, names_ref, pairs, nums,
            ext_b, fwd_send, fwd_recv, bwd_send, bwd_recv, acc_z, acc_s, acc_r, dz_b, cnt_send, cnt_recv,
            sems, cnt_sems, list_sems, pos_sems):
    me, nxt, prv = ring_peers(num_dev)
    layers = layer_peers(me, num_dev)
    layer = [me - me % PLANE + (me % PLANE + k) % PLANE for k in range(1, PLANE)]
    meet([nxt, prv] + layer + layers)
    total = jnp.sum(jnp.sum(mask_ref[...].astype(F32), axis=1, keepdims=True), axis=0, keepdims=True)
    cnt_send[0] = jnp.broadcast_to(total, cnt_send.shape[1:])
    counts = [remote(cnt_send.at[0], cnt_recv.at[k], cnt_sems, k, dev) for k, dev in enumerate(layer)]
    for copy in counts:
        copy.start()
    late = []

    def send_late(pairs, pool, first):
        for k, (src, dst) in enumerate(pairs):
            for s, dev in enumerate((nxt, prv)):
                copy = remote(src, dst[s], pool, 2 * (first + k) + s, dev)
                copy.start()
                late.append(copy)

    chunk = pos_ref.shape[0] // 2

    def send_pos(q):
        at = pl.ds(q * chunk, chunk)
        send_late([(pos_ref.at[at, :], [pos_prev_ref.at[at, :], pos_next_ref.at[at, :]])], pos_sems, q)

    own_hi = tab_ref.shape[0] // CLASS_ROWS
    halo = send_ref.shape[1]
    halo_hi = halo // LANES
    all_hi = own_hi + 2 * halo_hi
    own_b = tab_ref[...].astype(BF16)
    ext_b[pl.ds(0, own_hi * CLASS_ROWS), :] = own_b
    hot_send = [lo_hot(send_ref[r:r + 1, :]) for r in range(2)]
    copies = []
    for r in (1, 0):
        val = pick_cols(own_b, 1, send_ref[r:r + 1, :], hot_send[r])
        fwd_send[r] = jnp.concatenate([val, jnp.zeros_like(val)], axis=0).astype(BF16)
        copy = remote(fwd_send.at[r], fwd_recv.at[1 - r], sems, r, nxt if r == 1 else prv)
        copy.start()
        copies.append(copy)
    send_late([(lpair_ref, [pairs.at[0], pairs.at[1]]), (lw_ref, [w_prev_ref, w_next_ref]),
               (num_ref, [nums.at[0], nums.at[1]])], list_sems, 0)
    for copy in counts:
        copy.wait()
    for k in range(len(layer)):
        total = total + cnt_recv[k][0:1, 0:1]
    cnt_send[1] = jnp.broadcast_to(total, cnt_send.shape[1:])
    counts = [remote(cnt_send.at[1], cnt_recv.at[len(layer) + k], cnt_sems, len(layer) + k, dev)
              for k, dev in enumerate(layers)]
    for copy in counts:
        copy.start()
    send_pos(0)
    send_pos(1)
    acc_z[...] = jnp.zeros_like(acc_z)
    acc_s[...] = jnp.zeros_like(acc_s)
    for copy in copies:
        copy.wait()
    for r in range(2):
        got = fwd_recv[r].astype(F32)
        for j in range(0, halo_hi, 2):
            two = jnp.concatenate([got[0:8, (j + k) * LANES:(j + k + 1) * LANES] for k in range(2)], axis=0)
            ext_b[pl.ds((own_hi + r * halo_hi + j) * CLASS_ROWS, 16), :] = two.astype(BF16)

    steps = src_ref.shape[0] // 8

    def forward(i, carry):
        first = pl.multiple_of(i * 8, 8)
        src, dst = wide_row(src_ref, first), wide_row(dst_ref, first)
        val = pick_cols(ext_b[...], 1, src, lo_hot(src)) * wide_row(w_ref, first)
        acc_z[...] += add_cols(val, dst, lo_hot(dst), own_hi)
        return carry

    lax.fori_loop(0, steps, forward, 0)

    logits = join_pieces(acc_z[...], own_hi)
    cls = lax.broadcasted_iota(jnp.int32, (CLASS_ROWS, LANES), 0)
    count = jnp.broadcast_to(total, (1, LANES))
    for k, copy in enumerate(counts):
        copy.wait()
        count = count + cnt_recv[len(layer) + k][0:1, :]
    count = jnp.maximum(count, 1.0)
    loss = jnp.zeros((1, LANES), F32)
    d_log = []
    for h in range(own_hi):
        z = jnp.where(cls < 7, logits[h], -jnp.inf)
        top = jnp.max(z, axis=0, keepdims=True)
        norm = jnp.log(jnp.sum(jnp.exp(z - top), axis=0, keepdims=True)) + top
        hot = cls == lab_ref[h:h + 1, :]
        mask = mask_ref[h:h + 1, :].astype(F32)
        picked = jnp.sum(jnp.where(hot, logits[h], 0.0), axis=0, keepdims=True)
        loss = loss + mask * (norm - picked)
        d_log.append((jnp.exp(z - norm) - hot.astype(F32)) * (mask / count))
    dz_b[...] = stack_pieces(jnp.concatenate(d_log, axis=0))

    def backward(i, carry):
        first = pl.multiple_of(i * 8, 8)
        src, dst = wide_row(src_ref, first), wide_row(dst_ref, first)
        val = pick_cols(dz_b[...], 3, dst, lo_hot(dst)) * wide_row(w_ref, first)
        acc_s[...] += add_cols(val, src, lo_hot(src), all_hi)
        return carry

    lax.fori_loop(0, steps, backward, 0)

    d_ext = join_pieces(acc_s[...], all_hi)
    copies = []
    for r in range(2):
        for j in range(halo_hi):
            bwd_send[r, :, j * LANES:(j + 1) * LANES] = d_ext[own_hi + r * halo_hi + j]
        copy = remote(bwd_send.at[r], bwd_recv.at[1 - r], sems, 2 + r, prv if r == 0 else nxt)
        copy.start()
        copies.append(copy)
    for copy in copies:
        copy.wait()
    for r in range(2):
        part = add_cols(bwd_recv[r], send_ref[r:r + 1, :], hot_send[r], own_hi)
        acc_r[...] = part if r == 0 else acc_r[...] + part
    back = join_pieces(acc_r[...], own_hi)
    d_tab = [d_ext[h] + back[h] for h in range(own_hi)]
    dt_ref[...] = jnp.concatenate(d_tab, axis=0).astype(BF16)
    send_late([(dt_ref, [dt_prev_ref, dt_next_ref])], list_sems, 3)
    grad = jnp.zeros((CLASS_ROWS, hid_ref.shape[1]), F32)
    for h in range(own_hi):
        grad = grad + jnp.dot(d_tab[h].astype(BF16), hid_ref[pl.ds(h * LANES, LANES), :], preferred_element_type=F32)
    misc_ref[0:8, :] = grad
    total = jnp.sum(loss, axis=1, keepdims=True) / count[:, 0:1]
    misc_ref[8:16, :] = jnp.broadcast_to(total, (8, misc_ref.shape[1]))
    for copy in late:
        copy.wait()
    for s, (to_dst, to_put) in enumerate(((dst_prev_ref, put_prev_ref), (dst_next_ref, put_next_ref))):
        to_dst[...] = pairs[s] & 0xFFFF
        to_put[...] = lax.shift_right_logical(pairs[s], 16)
    row = lax.broadcasted_iota(jnp.int32, nums_ref.shape, 0)
    nums_ref[...] = jnp.where(row == 0, num_ref[0:1, :], jnp.where(row == 1, nums[0, 0:1, :], nums[1, 0:1, :]))
    names_ref[...] = 2 * jnp.concatenate(
        [send_ref[r:r + 1, j * LANES:(j + 1) * LANES] for r in (1, 0) for j in range(halo_hi)], axis=0)


def k5_body(num_dev, part_ref, full_ref, land_core, land_chip, land_z, by_core, by_chip, sems):
    me = lax.axis_index(GRAPH_AXIS)
    core, chip, z = me % 2, (me // 2) % 4, me // PLANE
    other = me + 1 - 2 * core
    chips = [me + 2 * ((chip + k) % 4 - chip) for k in range(1, 4)]
    layers = layer_peers(me, num_dev)
    num_z = num_dev // PLANE
    meet([other] + chips + layers)
    rows, width = part_ref.shape
    n1, n2, n3 = rows // 2, rows // 8, rows // 8 // num_z
    parts = [pl.ds(c * LANES, LANES) for c in range(width // LANES)]
    used = [0]

    def send(pairs):
        out = []
        for src, dst, dev in pairs:
            out.append(remote(src, dst, sems, used[0], dev))
            used[0] += 1
        for copy in out:
            copy.start()
        return out

    def wait(copies):
        for copy in copies:
            copy.wait()

    def at(first, size):
        return pl.ds(pl.multiple_of(first, size), size)

    flying = [send([(part_ref.at[at((1 - core) * n1, n1), c], land_core.at[:, c], other)]) for c in parts]
    for i, c in enumerate(parts):
        wait(flying[i])
        by_core[:, c] = part_ref[at(core * n1, n1), c] + land_core[:, c]
        flying[i] = send([(by_core.at[at((chip + k + 1) % 4 * n2, n2), c], land_chip.at[k, :, c], dev)
                          for k, dev in enumerate(chips)])
    for i, c in enumerate(parts):
        wait(flying[i])
        total = by_core[at(chip * n2, n2), c]
        for k in range(len(chips)):
            total = total + land_chip[k, :, c]
        by_chip[:, c] = total
        flying[i] = send([(by_chip.at[at((z + k + 1) % num_z * n3, n3), c], land_z.at[k, :, c], dev)
                          for k, dev in enumerate(layers)])
    first = core * n1 + chip * n2 + z * n3
    gathers = ((first, n3, layers), (core * n1 + chip * n2, n2, chips), (core * n1, n1, [other]))

    def gather(level, c):
        first, size, devs = gathers[level]
        own = full_ref.at[at(first, size), c]
        return send([(own, own, dev) for dev in devs])

    for i, c in enumerate(parts):
        wait(flying[i])
        total = by_chip[at(z * n3, n3), c]
        for k in range(len(layers)):
            total = total + land_z[k, :, c]
        full_ref[at(first, n3), c] = total
        flying[i] = gather(0, c)
    for level in (1, 2):
        for i, c in enumerate(parts):
            wait(flying[i])
            flying[i] = gather(level, c)
    for copies in flying:
        wait(copies)


def k6_body(full_ref, loss_ref, one_ref, two_ref):
    feats, classes = one_ref.shape[0], two_ref.shape[0]
    one_ref[...] = full_ref[0:feats, :]
    two_ref[...] = full_ref[feats:feats + classes, :]
    loss_ref[...] = full_ref[feats + 8:feats + 9, 0:1]


def solution(mesh):
    num_dev = mesh.shape[GRAPH_AXIS]

    def params(cid=None):
        if cid is None:
            return pltpu.CompilerParams(vmem_limit_bytes=VMEM_BYTES)
        return pltpu.CompilerParams(vmem_limit_bytes=VMEM_BYTES, collective_id=cid, has_side_effects=True)

    def arr(dtype, *shape):
        return jax.ShapeDtypeStruct(shape, dtype)

    def scr(dtype, *shape):
        return pltpu.VMEM(shape, dtype)

    def dma(count):
        return pltpu.SemaphoreType.DMA((2, count))

    I32 = jnp.int32

    def device_step(node_feats, w_one, w_two, send_rows, edge_src, edge_dst, edge_w, labels, label_mask):
        rows, feats = node_feats.shape
        width = w_one.shape[1]
        halo = send_rows.shape[1]
        edges = edge_src.shape[0]
        own_hi, all_hi = rows // LANES, (rows + 2 * halo) // LANES
        feats_t, w2 = node_feats.T, w_two.T
        src2, dst2, ew2 = (a.reshape(edges // LANES, LANES) for a in (edge_src, edge_dst, edge_w))
        lab2, mask2 = labels.reshape(own_hi, LANES), label_mask.reshape(own_hi, LANES)
        listed = (LIST_ROWS, LANES)
        entries = LIST_ROWS * LANES
        fast_list = pltpu.SMEM(listed, I32)
        list_dma = dma(entries // CHUNK)

        half = rows // 2
        busy = pl.CostEstimate(flops=8 * 10**9, bytes_accessed=10**7, transcendentals=0)
        own_t, to_next, to_prev = pl.pallas_call(
            k1_body,
            out_shape=(arr(BF16, width, rows), arr(BF16, halo, width), arr(BF16, halo, width)),
            in_specs=[pl.BlockSpec(memory_space=pltpu.HBM)] * 3, out_specs=(vmem(),) * 3,
            scratch_shapes=[scr(BF16, feats, rows), scr(F32, feats, width), pltpu.VMEM((2, halo), I32),
                            pltpu.SemaphoreType.DMA((3,))],
            compiler_params=params(), name="transform",
        )(feats_t, w_one, send_rows)
        from_prev = lax.ppermute(to_next, GRAPH_AXIS, [(g, (g + 1) % num_dev) for g in range(num_dev)])
        from_next = lax.ppermute(to_prev, GRAPH_AXIS, [(g, (g - 1) % num_dev) for g in range(num_dev)])

        bufs = [scr(F32, 2 * rows, LANES)] * NUM_BUFS
        lists_in = (arr(I32, *listed), arr(I32, *listed), arr(I32, *listed), arr(F32, *listed), arr(I32, 8, LANES))
        part_own, lsrc, ldst, lpair, lw, num = pl.pallas_call(
            k2a_body,
            out_shape=(arr(F32, rows, width),) + lists_in,
            in_specs=[vmem()] * 4, out_specs=(vmem(),) * 6,
            scratch_shapes=[scr(I32, edges // LANES, LANES), scr(F32, 6 * LIST_ROWS, LANES), scr(F32, 2 * rows, LANES),
                            scr(F32, entries, LANES), pltpu.SMEM((8, LANES), I32), fast_list, fast_list,
                            pltpu.SemaphoreType.DMA, list_dma] + bufs,
            compiler_params=params(), cost_estimate=busy, name="aggregate_own",
        )(own_t, src2, dst2, ew2)

        hid, pos_a, pos_b, tab = pl.pallas_call(
            k2b_body,
            out_shape=(arr(BF16, rows, width), arr(BF16, half, width), arr(BF16, half, width),
                       arr(F32, own_hi * CLASS_ROWS, LANES)),
            in_specs=[vmem(), vmem(), vmem(), hbm(), hbm(), smem(), vmem(), vmem()], out_specs=(vmem(),) * 4,
            scratch_shapes=[scr(F32, 4 * halo, LANES), scr(F32, entries, LANES), fast_list, fast_list, list_dma] + bufs,
            compiler_params=params(), name="aggregate_halo",
        )(part_own, from_prev, from_next, lsrc, ldst, num, lw, w2)

        num_z = num_dev // PLANE
        tab_b = arr(BF16, own_hi * CLASS_ROWS, LANES)
        pos_half = arr(BF16, half, width)
        list_i = arr(I32, *listed)
        (d_tab, misc, d_prev, d_next, prev_a, next_a, dst_prev, dst_next, put_prev, put_next, w_prev, w_next,
         nums, names) = pl.pallas_call(
            functools.partial(k3_body, num_dev),
            out_shape=(tab_b, arr(F32, 16, width), tab_b, tab_b, pos_half, pos_half, list_i, list_i, list_i, list_i,
                       arr(F32, *listed), arr(F32, *listed), arr(I32, 8, LANES), arr(I32, 2 * halo // LANES, LANES)),
            in_specs=[vmem()] * 12, out_specs=(vmem(),) * 14,
            scratch_shapes=[scr(I32, 2, *listed), scr(I32, 2, 8, LANES), scr(BF16, all_hi * CLASS_ROWS, LANES),
                            scr(BF16, 2, 16, halo), scr(BF16, 2, 16, halo), scr(F32, 2, CLASS_ROWS, halo),
                            scr(F32, 2, CLASS_ROWS, halo), scr(F32, own_hi * 24, LANES), scr(F32, all_hi * 24, LANES),
                            scr(F32, own_hi * 24, LANES), scr(BF16, 3 * own_hi * CLASS_ROWS, LANES),
                            scr(F32, 2, 8, LANES), scr(F32, PLANE + num_z - 2, 8, LANES),
                            dma(4), dma(PLANE + num_z - 2), dma(8), dma(4)],
            compiler_params=params(1), name="layer_two",
        )(tab, send_rows, src2, dst2, ew2, lab2, mask2, hid, pos_a, lpair, lw, num)

        pos_b_late, d_tab = lax.optimization_barrier((pos_b, d_tab))
        prev_b = lax.ppermute(pos_b_late, GRAPH_AXIS, [(g, (g + 1) % num_dev) for g in range(num_dev)])
        next_b = lax.ppermute(pos_b_late, GRAPH_AXIS, [(g, (g - 1) % num_dev) for g in range(num_dev)])
        part_own = pl.pallas_call(
            k4a_body,
            out_shape=arr(F32, rows, width),
            in_specs=[hbm(), hbm(), smem()] + [vmem()] * 5, out_specs=vmem(),
            scratch_shapes=[scr(F32, 2 * rows, LANES), scr(F32, entries, LANES), fast_list, fast_list, list_dma] + bufs,
            compiler_params=params(), cost_estimate=busy, name="scatter_own",
        )(ldst, lsrc, num, lw, pos_a, pos_b, d_tab, w2)

        sum_rows_pad = 512
        part = pl.pallas_call(
            k4b_body,
            out_shape=arr(F32, sum_rows_pad, width),
            in_specs=[vmem(), smem(), smem()] + [hbm(), hbm(), vmem()] * 2 + [vmem()] * 9, out_specs=vmem(),
            scratch_shapes=[scr(F32, 2 * rows, LANES), scr(F32, entries, LANES), scr(BF16, rows, width)]
            + [fast_list] * 4 + [list_dma] * 2 + bufs,
            compiler_params=params(), name="scatter_peers",
        )(part_own, nums, names.reshape(2 * halo), dst_prev, put_prev, w_prev,
          dst_next, put_next, w_next,
          d_prev, prev_a, prev_b, d_next, next_a, next_b, w2, feats_t, misc)

        n1, n2 = sum_rows_pad // 2, sum_rows_pad // 8
        n3 = n2 // num_z
        full = pl.pallas_call(
            functools.partial(k5_body, num_dev),
            out_shape=arr(F32, sum_rows_pad, width),
            in_specs=[vmem()], out_specs=vmem(),
            scratch_shapes=[scr(F32, n1, width), scr(F32, 3, n2, width), scr(F32, num_z - 1, n3, width),
                            scr(F32, n1, width), scr(F32, n2, width), dma(4 * (1 + 3 + num_z - 1))],
            compiler_params=params(2), name="sum_gradients",
        )(part)
        loss, grad_one, grad_two = pl.pallas_call(
            k6_body,
            out_shape=(arr(F32, 1, 1), arr(F32, feats, width), arr(F32, w2.shape[0], width)),
            in_specs=[vmem()], out_specs=(vmem(),) * 3, compiler_params=params(), name="outputs",
        )(full)
        return loss.reshape(()), grad_one, grad_two.T

    row_spec = P(GRAPH_AXIS)
    return jax.shard_map(device_step, mesh=mesh,
                         in_specs=(row_spec, P(), P(), row_spec, row_spec, row_spec, row_spec, row_spec, row_spec),
                         out_specs=(P(), P(), P()), check_vma=False)
```

```python
import functools

import jax
import jax.numpy as jnp
from jax import lax
from jax.experimental import pallas as pl
from jax.experimental.pallas import tpu as pltpu
from jax.sharding import PartitionSpec as P

GRAPH_AXIS = "graph"
MESH = pl.DeviceIdType.MESH
LANES = 128
CLASS_ROWS = 8
VMEM_BYTES = 28 * 2**20
K1_VMEM = 50 * 2**20
OWN_VMEM = 34 * 2**20
F32 = jnp.float32
BF16 = jnp.bfloat16
NT = (((1,), (1,)), ((), ()))
TN = (((0,), (0,)), ((), ()))


def vmem():
    return pl.BlockSpec(memory_space=pltpu.VMEM)


def hbm():
    return pl.BlockSpec(memory_space=pl.ANY)


def smem():
    return pl.BlockSpec(memory_space=pltpu.SMEM)


PLANE = 8
LIST_ROWS = 80
BLOCK = 128
NUM_BUFS = 4
OWN_BUFS = 6
EARLY_ROWS = 768
CHUNK = 1024


def ring_peers(num_dev):
    me = lax.axis_index(GRAPH_AXIS)
    return me, (me + 1) % num_dev, (me + num_dev - 1) % num_dev


def layer_peers(me, num_dev):
    return [(me + PLANE * k) % num_dev for k in range(1, num_dev // PLANE)]


def class_weights(w_ref):
    w = w_ref[...]
    return jnp.concatenate([w, jnp.zeros((CLASS_ROWS - w.shape[0], w.shape[1]), F32)], axis=0).astype(BF16)


def meet(partners):
    barrier = pltpu.get_barrier_semaphore()
    for dev in partners:
        pl.semaphore_signal(barrier, inc=1, device_id=(dev,), device_id_type=MESH)
    pl.semaphore_wait(barrier, len(partners))


def remote(src, dst, sems, slot, dev):
    return pltpu.make_async_remote_copy(
        src_ref=src, dst_ref=dst, send_sem=sems.at[0, slot], recv_sem=sems.at[1, slot],
        device_id=(dev,), device_id_type=MESH)


def three_pieces(val):
    top = val.astype(BF16).astype(F32)
    rest = val - top
    mid = rest.astype(BF16).astype(F32)
    return top, mid, rest - mid


def wide_row(ref, first):
    blk = ref[pl.ds(first, 8), :]
    return jnp.concatenate([blk[j:j + 1, :] for j in range(8)], axis=1)


def packed(row):
    return jnp.broadcast_to(row, (16, row.shape[1])).astype(jnp.int16)


def hot_rows(row, count):
    n = row.shape[1]
    ids = lax.broadcasted_iota(jnp.int32, (count, LANES), 0).astype(jnp.int16)
    return jnp.concatenate([ids] * (n // LANES), axis=1) == jnp.concatenate([packed(row)] * (count // 16), axis=0)


def ones_at(mask):
    return jnp.where(mask, jnp.ones((), BF16), jnp.zeros((), BF16))


def lo_hot(idx):
    return ones_at(hot_rows(idx & (LANES - 1), LANES))


def list_places(src_ref, w_ref, rows, halo, pos, num_ref):
    src, live = src_ref[...], w_ref[...] != 0.0
    n_rows = src.shape[0]
    tri = (lax.broadcasted_iota(jnp.int32, (LANES, LANES), 0) <= lax.broadcasted_iota(jnp.int32, (LANES, LANES), 1))
    tri = tri.astype(F32).astype(BF16)
    low = (lax.broadcasted_iota(jnp.int32, (n_rows, n_rows), 1) < lax.broadcasted_iota(jnp.int32, (n_rows, n_rows), 0))
    low = low.astype(F32).astype(BF16)
    place = jnp.full(src.shape, LIST_ROWS * LANES, jnp.int32)
    start = jnp.zeros((1, 1), jnp.int32)
    lane = lax.broadcasted_iota(jnp.int32, num_ref.shape, 1)
    num = jnp.zeros(num_ref.shape, jnp.int32)
    kinds = (src < rows, (src >= rows) & (src < rows + halo), src >= rows + halo)
    for k, kind in enumerate(kinds):
        kind = kind & live
        flag = kind.astype(F32)
        inner = jnp.dot(flag.astype(BF16), tri, preferred_element_type=F32)
        row_sum = jnp.broadcast_to(jnp.sum(flag, axis=1, keepdims=True), flag.shape)
        before = jnp.dot(low, row_sum.astype(BF16), preferred_element_type=F32)
        rank = (inner + before).astype(jnp.int32) - 1
        place = jnp.where(kind, start + rank, place)
        total = jnp.sum(jnp.sum(flag, axis=1, keepdims=True), axis=0, keepdims=True).astype(jnp.int32)
        blocks = lax.shift_right_logical(total + (BLOCK - 1), BLOCK.bit_length() - 1)
        start = start + blocks * BLOCK
        num = jnp.where(lane == k, blocks, num)
    pos[...] = place
    num_ref[...] = num


def k1_body(xt_hbm, w_hbm, send_hbm, own_t_ref, to_next_ref, to_prev_ref, xt_ref, w_ref, send_ref, hot, sems):
    copies = [pltpu.make_async_copy(a, b, sems.at[k])
              for k, (a, b) in enumerate(((send_hbm, send_ref), (w_hbm, w_ref), (xt_hbm, xt_ref)))]
    for copy in copies:
        copy.start()
    copies[0].wait()
    halo = send_ref.shape[1]
    rows = xt_ref.shape[1]
    blocks = halo // LANES
    ids = jnp.concatenate([send_ref[r:r + 1, b * LANES:(b + 1) * LANES] for r in range(2) for b in range(blocks)], axis=0)
    ids_col = jnp.transpose(ids)
    node = lax.broadcasted_iota(jnp.int32, (LANES, rows), 1).astype(jnp.int16)
    for b in range(2 * blocks):
        col = jnp.broadcast_to(ids_col[:, b:b + 1], (LANES, LANES)).astype(jnp.int16)
        hot[b * LANES:(b + 1) * LANES, :] = ones_at(node == jnp.concatenate([col] * (rows // LANES), axis=1))
    copies[1].wait()
    w_b = w_ref[...].astype(BF16)
    copies[2].wait()
    own_t_ref[...] = lax.dot_general(w_b, xt_ref[...], TN, preferred_element_type=F32).astype(BF16)
    for r, out in ((1, to_next_ref), (0, to_prev_ref)):
        out[...] = lax.dot_general(hot[r * halo:(r + 1) * halo, :], own_t_ref[...], NT, preferred_element_type=F32).astype(BF16)


def sort_edges(src_ref, dst_ref, ew_ref, rows, halo, pos, acc, lsrc_ref, ldst_ref, lpair_ref, lw_ref, num_ref):
    list_places(src_ref, ew_ref, rows, halo, pos, num_ref)
    acc[...] = jnp.zeros_like(acc)

    def sort(i, carry):
        first = pl.multiple_of(i * 8, 8)
        src, dst, wgt, place = (wide_row(ref, first) for ref in (src_ref, dst_ref, ew_ref, pos))
        both = src + dst * 4096
        ints = [both & 255, lax.shift_right_logical(both, 8) & 255, lax.shift_right_logical(both, 16)]
        cargo = [v.astype(F32) for v in ints] + list(three_pieces(wgt))
        here = hot_rows(lax.shift_right_logical(place, 7), LIST_ROWS)
        cargo = [jnp.concatenate([jnp.broadcast_to(v, (16, v.shape[1])).astype(BF16)] * (LIST_ROWS // 16), axis=0) for v in cargo]
        lhs = jnp.concatenate([jnp.where(here, v, jnp.zeros((), BF16)) for v in cargo], axis=0)
        acc[...] += lax.dot_general(lhs, lo_hot(place), NT, preferred_element_type=F32)
        return carry

    lax.fori_loop(0, src_ref.shape[0] // 8, sort, 0)
    got = [acc[p * LIST_ROWS:(p + 1) * LIST_ROWS, :] for p in range(6)]
    ints = [g.astype(jnp.int32) for g in got[:3]]
    both = ints[0] + ints[1] * 256 + ints[2] * 65536
    src, dst = both & 4095, lax.shift_right_logical(both, 12) * 2
    src = jnp.where(src < rows, src, src - rows)
    lsrc_ref[...] = src * 2
    ldst_ref[...] = dst
    lpair_ref[...] = dst + src * 65536
    lw_ref[...] = got[3] + got[4] + got[5]


def spread_weights(w_ref, wide, first, last):
    def body(g, carry):
        cols = jnp.transpose(w_ref[pl.ds(pl.multiple_of(g * 8, 8), 8), :])
        for j in range(8):
            at = pl.ds(pl.multiple_of(g * 8 * LANES + j * LANES, LANES), LANES)
            wide[at, :] = jnp.broadcast_to(cols[:, j:j + 1], (LANES, LANES))
        return carry

    lax.fori_loop(first // 8, (last + 7) // 8, body, 0)


def clear_rows(bufs):
    def body(i, carry):
        for buf in bufs:
            buf[pl.ds(pl.multiple_of(i * 64, 64), 64), :] = jnp.zeros((64, LANES), F32)
        return carry

    lax.fori_loop(0, bufs[0].shape[0] // 64, body, 0)


def chunk_copies(lists, fast, sems, c):
    at = pl.ds(pl.multiple_of(c * 8, 8), CHUNK // LANES)
    return [pltpu.make_async_copy(a.at[at, :], b.at[at, :], sems.at[k, c]) for k, (a, b) in enumerate(zip(lists, fast))]


def chunks_of(first, last):
    per = CHUNK // BLOCK
    return first // per, (last + per - 1) // per


def start_lists(lists, fast, sems, first, last):
    def body(c, carry):
        for copy in chunk_copies(lists, fast, sems, c):
            copy.start()
        return carry

    lax.fori_loop(*chunks_of(first, last), body, 0)


def row_loop(lists, fast, sems, wide, table, bufs, first, last, rename=None):
    num = len(bufs)
    take_ref, put_ref = fast
    per = CHUNK // BLOCK

    def step(i, carry):
        base = i * BLOCK
        for lead in range(0, BLOCK, num):
            take = [pl.multiple_of(take_ref[i, lead + j], 2) for j in range(num)]
            put = [put_ref[i, lead + j] for j in range(num)]
            if rename is not None:
                put = [rename[p] for p in put]
            put = [pl.multiple_of(p, 2) for p in put]
            vals = [wide[pl.ds(base + lead + j, 1), :] * table[pl.ds(take[j], 2), :] for j in range(num)]
            old = [bufs[j][pl.ds(put[j], 2), :] for j in range(num)]
            for j in range(num):
                bufs[j][pl.ds(put[j], 2), :] = old[j] + vals[j]
        return carry

    def chunk(c, carry):
        for copy in chunk_copies(lists, fast, sems, c):
            copy.wait()
        return lax.fori_loop(jnp.maximum(first, c * per), jnp.minimum(last, c * per + per), step, carry)

    lax.fori_loop(*chunks_of(first, last), chunk, 0)


def slot_copies(lists, slots, sems, c):
    at = pl.ds(pl.multiple_of(c * 8, 8), 8)
    return lambda slot: [pltpu.make_async_copy(a.at[at, :], b, sems.at[slot, k]) for k, (a, b) in enumerate(zip(lists, slots[slot]))]


def start_slots(lists, slots, sems):
    for slot in range(2):
        for copy in slot_copies(lists, slots, sems, slot)(slot):
            copy.start()


def slot_loop(lists, slots, sems, wide, table, bufs, last):
    num = len(bufs)
    pairs = jnp.maximum((last + 15) // 16, 1)

    def group(k, carry):
        for slot in range(2):
            take_ref, put_ref = slots[slot]
            for copy in slot_copies(lists, slots, sems, 2 * k + slot)(slot):
                copy.wait()
            for r in range(8):
                row = 16 * k + 8 * slot + r

                @pl.when(row < last)
                def _():
                    base = pl.multiple_of(row * LANES, LANES)
                    for lead in range(0, LANES, num):
                        here = range(min(num, LANES - lead))
                        take = [pl.multiple_of(take_ref[r, lead + j], 2) for j in here]
                        put = [pl.multiple_of(put_ref[r, lead + j], 2) for j in here]
                        vals = [wide[pl.ds(base + lead + j, 1), :] * table[pl.ds(take[j], 2), :] for j in here]
                        old = [bufs[j][pl.ds(put[j], 2), :] for j in here]
                        for j in here:
                            bufs[j][pl.ds(put[j], 2), :] = old[j] + vals[j]

            @pl.when(k + 1 < pairs)
            def _():
                for copy in slot_copies(lists, slots, sems, 2 * k + 2 + slot)(slot):
                    copy.start()
        return carry

    lax.fori_loop(0, pairs, group, 0)


def list_rows(first, last):
    return first * BLOCK // LANES, (last * BLOCK + LANES - 1) // LANES


def to_rows(blk, table, first_row):
    for h in range(2):
        table[pl.ds(2 * first_row + h, blk.shape[0], stride=2), :] = blk[:, h * LANES:(h + 1) * LANES]


def sum_rows(bufs, blk):
    halves = []
    for h in range(2):
        parts = [buf[pl.ds(2 * blk * LANES + h, LANES, stride=2), :] for buf in bufs]
        while len(parts) > 1:
            parts = [a + b for a, b in zip(parts[::2], parts[1::2])] + parts[len(parts) // 2 * 2:]
        halves.append(parts[0])
    return jnp.concatenate(halves, axis=1)


def k2a_body(own_t_ref, src_ref, dst_ref, ew_ref, part_ref, lsrc_ref, ldst_ref, lpair_ref, lw_ref, num_ref,
             pos, acc, table, wide, num_fast, src_a, dst_a, src_b, dst_b, sems, slot_sems, *bufs):
    rows = part_ref.shape[0]
    sort_edges(src_ref, dst_ref, ew_ref, rows, rows // 2, pos, acc, lsrc_ref, ldst_ref, lpair_ref, lw_ref, num_ref)

    def widen(i, carry):
        at = pl.ds(pl.multiple_of(i * LANES, LANES), LANES)
        to_rows(jnp.transpose(own_t_ref[:, at].astype(F32)), table, i * LANES)
        return carry

    lax.fori_loop(0, rows // LANES, widen, 0)
    copy = pltpu.make_async_copy(num_ref, num_fast, sems.at[0])
    copy.start()
    lists, slots = (lsrc_ref, ldst_ref), ((src_a, dst_a), (src_b, dst_b))
    start_slots(lists, slots, slot_sems)
    clear_rows(bufs)
    copy.wait()
    end = num_fast[0, 0]
    spread_weights(lw_ref, wide, *list_rows(0, end))
    slot_loop(lists, slots, slot_sems, wide, table, bufs, end)

    def finish(i, carry):
        part_ref[pl.ds(pl.multiple_of(i * LANES, LANES), LANES), :] = sum_rows(bufs, i)
        return carry

    lax.fori_loop(0, rows // LANES, finish, 0)


def k2b_body(part_ref, prev_ref, next_ref, lsrc_ref, ldst_ref, num_ref, lw_ref, w2_ref,
             hid_ref, pos_a_ref, pos_b_ref, tab_ref, table, wide, src_fast, dst_fast, sems, *bufs):
    first = num_ref[0, 0]
    end = first + num_ref[0, 1] + num_ref[0, 2]
    lists, fast = (lsrc_ref, ldst_ref), (src_fast, dst_fast)
    start_lists(lists, fast, sems, first, end)
    spread_weights(lw_ref, wide, *list_rows(first, end))
    halo = prev_ref.shape[0]

    def widen(i, carry):
        at = pl.ds(pl.multiple_of(i * LANES, LANES), LANES)
        to_rows(prev_ref[at, :].astype(F32), table, i * LANES)
        to_rows(next_ref[at, :].astype(F32), table, halo + i * LANES)
        return carry

    lax.fori_loop(0, halo // LANES, widen, 0)
    clear_rows(bufs)
    row_loop(lists, fast, sems, wide, table, bufs, first, end)
    w2t = class_weights(w2_ref)

    for pos_ref, lead in ((pos_a_ref, 0), (pos_b_ref, pos_a_ref.shape[0] // LANES)):
        def finish(j, carry):
            i = lead + j
            at = pl.ds(pl.multiple_of(i * LANES, LANES), LANES)
            pre = part_ref[at, :] + sum_rows(bufs, i)
            hid = jnp.maximum(pre, 0.0).astype(BF16)
            hid_ref[at, :] = hid
            pos_ref[pl.ds(pl.multiple_of(j * LANES, LANES), LANES), :] = (pre > 0.0).astype(F32).astype(BF16)
            t2 = lax.dot_general(w2t, hid, NT, preferred_element_type=F32)
            tab_ref[pl.ds(pl.multiple_of(i * CLASS_ROWS, CLASS_ROWS), CLASS_ROWS), :] = t2.astype(BF16).astype(F32)
            return carry

        lax.fori_loop(0, pos_ref.shape[0] // LANES, finish, 0)


def stack_classes(w2_ref, blocks):
    w2_all = jnp.concatenate([class_weights(w2_ref).astype(F32)] * blocks, axis=0)
    return w2_all, lax.shift_right_logical(lax.broadcasted_iota(jnp.int32, w2_all.shape, 0), 3)


def fill_table(dt_ref, pos_refs, w2_all, group, table):
    dt_cols = jnp.transpose(dt_ref[...].astype(F32)).astype(BF16)
    for pos_ref, lead in zip(pos_refs, (0, pos_refs[0].shape[0] // LANES)):
        def widen(j, carry):
            i = lead + j
            d_hid = jnp.dot(dt_cols, jnp.where(group == i, w2_all, 0.0).astype(BF16), preferred_element_type=F32)
            at = pl.ds(pl.multiple_of(j * LANES, LANES), LANES)
            to_rows(jnp.where(pos_ref[at, :].astype(F32) > 0.0, d_hid, 0.0), table, i * LANES)
            return carry

        lax.fori_loop(0, pos_ref.shape[0] // LANES, widen, 0)


def k4a_body(ldst_ref, lsrc_ref, num_ref, lw_ref, pos_a_ref, pos_b_ref, dt_ref, w2_ref, part_ref,
             table, wide, take_a, put_a, take_b, put_b, slot_sems, *bufs):
    rows = part_ref.shape[0]
    lists, slots, end = (ldst_ref, lsrc_ref), ((take_a, put_a), (take_b, put_b)), num_ref[0, 0]
    start_slots(lists, slots, slot_sems)
    w2_all, group = stack_classes(w2_ref, rows // LANES)
    clear_rows(bufs)
    fill_table(dt_ref, (pos_a_ref, pos_b_ref), w2_all, group, table)
    spread_weights(lw_ref, wide, *list_rows(0, end))
    slot_loop(lists, slots, slot_sems, wide, table, bufs, end)

    def finish(i, carry):
        part_ref[pl.ds(pl.multiple_of(i * LANES, LANES), LANES), :] = sum_rows(bufs, i)
        return carry

    lax.fori_loop(0, rows // LANES, finish, 0)


def k4b_body(part_ref, num_ref, names_ref, prev_dst, prev_src, prev_w, next_dst, next_src, next_w,
             prev_dt, prev_a, prev_b, next_dt, next_a, next_b, w2_ref, xt_ref, misc_ref, out_ref,
             table, wide, d_tab, *rest):
    fasts, pools, bufs = (rest[0:2], rest[2:4]), rest[4:6], rest[6:]
    rows = part_ref.shape[0]
    sides = (((prev_dst, prev_src), prev_w, prev_dt, (prev_a, prev_b), 1, 2),
             ((next_dst, next_src), next_w, next_dt, (next_a, next_b), 2, 1))
    spans = []
    for (lists, _, _, _, row, kind), fast, pool in zip(sides, fasts, pools):
        first = num_ref[row, 0]
        if kind == 2:
            first = first + num_ref[row, 1]
        spans.append((first, first + num_ref[row, kind]))
        start_lists(lists, fast, pool, *spans[-1])
    w2_all, group = stack_classes(w2_ref, rows // LANES)
    clear_rows(bufs)
    for (lists, w_ref, dt_ref, pos_refs, _, _), fast, pool, span in zip(sides, fasts, pools, spans):
        fill_table(dt_ref, pos_refs, w2_all, group, table)
        spread_weights(w_ref, wide, *list_rows(*span))
        row_loop(lists, fast, pool, wide, table, bufs, *span, rename=names_ref)

    def finish(i, carry):
        at = pl.ds(pl.multiple_of(i * LANES, LANES), LANES)
        d_tab[at, :] = (part_ref[at, :] + sum_rows(bufs, i)).astype(BF16)
        return carry

    lax.fori_loop(0, rows // LANES, finish, 0)
    feats = xt_ref.shape[0]
    out_ref[0:feats, :] = jnp.dot(xt_ref[...], d_tab[...], preferred_element_type=F32)
    out_ref[feats:feats + 12, :] = misc_ref[0:12, :]


def hi_of(idx):
    return jnp.broadcast_to(lax.shift_right_logical(idx, 7), (CLASS_ROWS, idx.shape[1]))


def pick_cols(table_b, pieces, idx, hot):
    cols = jnp.dot(table_b, hot, preferred_element_type=F32)
    rows = table_b.shape[0] // pieces
    hi = hi_of(idx)
    out = jnp.zeros(hi.shape, F32)
    for h in range(rows // CLASS_ROWS):
        part = cols[h * CLASS_ROWS:(h + 1) * CLASS_ROWS]
        for p in range(1, pieces):
            part = part + cols[p * rows + h * CLASS_ROWS:p * rows + (h + 1) * CLASS_ROWS]
        out = out + jnp.where(hi == h, part, 0.0)
    return out


def add_cols(val, idx, hot, num_hi):
    hi = packed(lax.shift_right_logical(idx, 7))
    low_half = lax.broadcasted_iota(jnp.int32, hi.shape, 0) >= CLASS_ROWS
    mixed = hi - low_half.astype(jnp.int32).astype(jnp.int16)
    top, mid, low = three_pieces(val)
    pieces = [jnp.concatenate(two, axis=0).astype(BF16) for two in ((top, mid), (low, top), (mid, low))]
    rows = []
    for h in range(0, num_hi, 2):
        masks = (hi == jnp.int16(h), mixed == jnp.int16(h), hi == jnp.int16(h + 1))
        rows += [jnp.where(m, p, jnp.zeros((), BF16)) for m, p in zip(masks, pieces)]
    return lax.dot_general(jnp.concatenate(rows, axis=0), hot, NT, preferred_element_type=F32)


def join_pieces(acc, num_hi):
    out = []
    for h in range(num_hi):
        a = acc[h * 24:h * 24 + 24, :]
        out.append(a[0:8] + a[8:16] + a[16:24])
    return out


def stack_pieces(val):
    return jnp.concatenate(three_pieces(val), axis=0).astype(BF16)


def k3_body(num_dev, tab_ref, send_ref, src_ref, dst_ref, w_ref, lab_ref, mask_ref, hid_ref, pos_ref,
            lpair_ref, lw_ref, num_ref,
            dt_ref, misc_ref, dt_prev_ref, dt_next_ref, pos_prev_ref, pos_next_ref, dst_prev_ref, dst_next_ref,
            put_prev_ref, put_next_ref, w_prev_ref, w_next_ref, nums_ref, names_ref, pairs, nums,
            ext_b, fwd_send, fwd_recv, bwd_send, bwd_recv, acc_z, acc_s, acc_r, dz_b, cnt_send, cnt_recv,
            sems, cnt_sems, list_sems, pos_sems):
    me, nxt, prv = ring_peers(num_dev)
    layers = layer_peers(me, num_dev)
    layer = [me - me % PLANE + (me % PLANE + k) % PLANE for k in range(1, PLANE)]
    meet([nxt, prv] + layer + layers)
    total = jnp.sum(jnp.sum(mask_ref[...].astype(F32), axis=1, keepdims=True), axis=0, keepdims=True)
    cnt_send[0] = jnp.broadcast_to(total, cnt_send.shape[1:])
    counts = [remote(cnt_send.at[0], cnt_recv.at[k], cnt_sems, k, dev) for k, dev in enumerate(layer)]
    for copy in counts:
        copy.start()
    late = []

    def send_late(pairs, pool, first):
        for k, (src, dst) in enumerate(pairs):
            for s, dev in enumerate((nxt, prv)):
                copy = remote(src, dst[s], pool, 2 * (first + k) + s, dev)
                copy.start()
                late.append(copy)

    chunk = pos_ref.shape[0] // 3

    def send_pos(q):
        at = pl.ds(q * chunk, chunk)
        send_late([(pos_ref.at[at, :], [pos_prev_ref.at[at, :], pos_next_ref.at[at, :]])], pos_sems, q)

    own_hi = tab_ref.shape[0] // CLASS_ROWS
    halo = send_ref.shape[1]
    halo_hi = halo // LANES
    all_hi = own_hi + 2 * halo_hi
    own_b = tab_ref[...].astype(BF16)
    ext_b[pl.ds(0, own_hi * CLASS_ROWS), :] = own_b
    hot_send = [lo_hot(send_ref[r:r + 1, :]) for r in range(2)]
    copies = []
    for r in (1, 0):
        val = pick_cols(own_b, 1, send_ref[r:r + 1, :], hot_send[r])
        fwd_send[r] = jnp.concatenate([val, jnp.zeros_like(val)], axis=0).astype(BF16)
        copy = remote(fwd_send.at[r], fwd_recv.at[1 - r], sems, r, nxt if r == 1 else prv)
        copy.start()
        copies.append(copy)
    send_late([(lpair_ref, [pairs.at[0], pairs.at[1]]), (lw_ref, [w_prev_ref, w_next_ref]),
               (num_ref, [nums.at[0], nums.at[1]])], list_sems, 0)
    send_pos(0)
    for copy in counts:
        copy.wait()
    for k in range(len(layer)):
        total = total + cnt_recv[k][0:1, 0:1]
    cnt_send[1] = jnp.broadcast_to(total, cnt_send.shape[1:])
    counts = [remote(cnt_send.at[1], cnt_recv.at[len(layer) + k], cnt_sems, len(layer) + k, dev)
              for k, dev in enumerate(layers)]
    for copy in counts:
        copy.start()
    send_pos(1)
    send_pos(2)
    acc_z[...] = jnp.zeros_like(acc_z)
    acc_s[...] = jnp.zeros_like(acc_s)
    for copy in copies:
        copy.wait()
    for r in range(2):
        got = fwd_recv[r].astype(F32)
        for j in range(0, halo_hi, 2):
            two = jnp.concatenate([got[0:8, (j + k) * LANES:(j + k + 1) * LANES] for k in range(2)], axis=0)
            ext_b[pl.ds((own_hi + r * halo_hi + j) * CLASS_ROWS, 16), :] = two.astype(BF16)

    steps = src_ref.shape[0] // 8

    def forward(i, carry):
        first = pl.multiple_of(i * 8, 8)
        src, dst = wide_row(src_ref, first), wide_row(dst_ref, first)
        val = pick_cols(ext_b[...], 1, src, lo_hot(src)) * wide_row(w_ref, first)
        acc_z[...] += add_cols(val, dst, lo_hot(dst), own_hi)
        return carry

    lax.fori_loop(0, steps, forward, 0)

    logits = join_pieces(acc_z[...], own_hi)
    cls = lax.broadcasted_iota(jnp.int32, (CLASS_ROWS, LANES), 0)
    count = jnp.broadcast_to(total, (1, LANES))
    for k, copy in enumerate(counts):
        copy.wait()
        count = count + cnt_recv[len(layer) + k][0:1, :]
    count = jnp.maximum(count, 1.0)
    loss = jnp.zeros((1, LANES), F32)
    d_log = []
    for h in range(own_hi):
        z = jnp.where(cls < 7, logits[h], -jnp.inf)
        top = jnp.max(z, axis=0, keepdims=True)
        norm = jnp.log(jnp.sum(jnp.exp(z - top), axis=0, keepdims=True)) + top
        hot = cls == lab_ref[h:h + 1, :]
        mask = mask_ref[h:h + 1, :].astype(F32)
        picked = jnp.sum(jnp.where(hot, logits[h], 0.0), axis=0, keepdims=True)
        loss = loss + mask * (norm - picked)
        d_log.append((jnp.exp(z - norm) - hot.astype(F32)) * (mask / count))
    dz_b[...] = stack_pieces(jnp.concatenate(d_log, axis=0))

    def backward(i, carry):
        first = pl.multiple_of(i * 8, 8)
        src, dst = wide_row(src_ref, first), wide_row(dst_ref, first)
        val = pick_cols(dz_b[...], 3, dst, lo_hot(dst)) * wide_row(w_ref, first)
        acc_s[...] += add_cols(val, src, lo_hot(src), all_hi)
        return carry

    lax.fori_loop(0, steps, backward, 0)

    d_ext = join_pieces(acc_s[...], all_hi)
    copies = []
    for r in range(2):
        for j in range(halo_hi):
            bwd_send[r, :, j * LANES:(j + 1) * LANES] = d_ext[own_hi + r * halo_hi + j]
        copy = remote(bwd_send.at[r], bwd_recv.at[1 - r], sems, 2 + r, prv if r == 0 else nxt)
        copy.start()
        copies.append(copy)
    for copy in copies:
        copy.wait()
    for r in range(2):
        part = add_cols(bwd_recv[r], send_ref[r:r + 1, :], hot_send[r], own_hi)
        acc_r[...] = part if r == 0 else acc_r[...] + part
    back = join_pieces(acc_r[...], own_hi)
    d_tab = [d_ext[h] + back[h] for h in range(own_hi)]
    dt_ref[...] = jnp.concatenate(d_tab, axis=0).astype(BF16)
    send_late([(dt_ref, [dt_prev_ref, dt_next_ref])], list_sems, 3)
    grad = jnp.zeros((CLASS_ROWS, hid_ref.shape[1]), F32)
    for h in range(own_hi):
        grad = grad + jnp.dot(d_tab[h].astype(BF16), hid_ref[pl.ds(h * LANES, LANES), :], preferred_element_type=F32)
    misc_ref[0:8, :] = grad
    total = jnp.sum(loss, axis=1, keepdims=True) / count[:, 0:1]
    misc_ref[8:16, :] = jnp.broadcast_to(total, (8, misc_ref.shape[1]))
    for copy in late:
        copy.wait()
    for s, (to_dst, to_put) in enumerate(((dst_prev_ref, put_prev_ref), (dst_next_ref, put_next_ref))):
        to_dst[...] = pairs[s] & 0xFFFF
        to_put[...] = lax.shift_right_logical(pairs[s], 16)
    row = lax.broadcasted_iota(jnp.int32, nums_ref.shape, 0)
    nums_ref[...] = jnp.where(row == 0, num_ref[0:1, :], jnp.where(row == 1, nums[0, 0:1, :], nums[1, 0:1, :]))
    names_ref[...] = 2 * jnp.concatenate(
        [send_ref[r:r + 1, j * LANES:(j + 1) * LANES] for r in (1, 0) for j in range(halo_hi)], axis=0)


def k5_body(num_dev, part_ref, full_ref, land_core, land_chip, land_z, by_core, by_chip, sems):
    me = lax.axis_index(GRAPH_AXIS)
    core, chip, z = me % 2, (me // 2) % 4, me // PLANE
    other = me + 1 - 2 * core
    chips = [me + 2 * ((chip + k) % 4 - chip) for k in range(1, 4)]
    layers = layer_peers(me, num_dev)
    num_z = num_dev // PLANE
    meet([other] + chips + layers)
    rows, width = part_ref.shape
    n1, n2, n3 = rows // 2, rows // 8, rows // 8 // num_z
    parts = [pl.ds(c * LANES, LANES) for c in range(width // LANES)]
    used = [0]

    def send(pairs):
        out = []
        for src, dst, dev in pairs:
            out.append(remote(src, dst, sems, used[0], dev))
            used[0] += 1
        for copy in out:
            copy.start()
        return out

    def wait(copies):
        for copy in copies:
            copy.wait()

    def at(first, size):
        return pl.ds(pl.multiple_of(first, size), size)

    flying = [send([(part_ref.at[at((1 - core) * n1, n1), c], land_core.at[:, c], other)]) for c in parts]
    for i, c in enumerate(parts):
        wait(flying[i])
        by_core[:, c] = part_ref[at(core * n1, n1), c] + land_core[:, c]
        flying[i] = send([(by_core.at[at((chip + k + 1) % 4 * n2, n2), c], land_chip.at[k, :, c], dev)
                          for k, dev in enumerate(chips)])
    for i, c in enumerate(parts):
        wait(flying[i])
        total = by_core[at(chip * n2, n2), c]
        for k in range(len(chips)):
            total = total + land_chip[k, :, c]
        by_chip[:, c] = total
        flying[i] = send([(by_chip.at[at((z + k + 1) % num_z * n3, n3), c], land_z.at[k, :, c], dev)
                          for k, dev in enumerate(layers)])
    first = core * n1 + chip * n2 + z * n3
    gathers = ((first, n3, layers), (core * n1 + chip * n2, n2, chips), (core * n1, n1, [other]))

    def gather(level, c):
        first, size, devs = gathers[level]
        own = full_ref.at[at(first, size), c]
        return send([(own, own, dev) for dev in devs])

    for i, c in enumerate(parts):
        wait(flying[i])
        total = by_chip[at(z * n3, n3), c]
        for k in range(len(layers)):
            total = total + land_z[k, :, c]
        full_ref[at(first, n3), c] = total
        flying[i] = gather(0, c)
    for level in (1, 2):
        for i, c in enumerate(parts):
            wait(flying[i])
            flying[i] = gather(level, c)
    for copies in flying:
        wait(copies)


def k6_body(full_ref, loss_ref, one_ref, two_ref):
    feats, classes = one_ref.shape[0], two_ref.shape[0]
    one_ref[...] = full_ref[0:feats, :]
    two_ref[...] = full_ref[feats:feats + classes, :]
    loss_ref[...] = full_ref[feats + 8:feats + 9, 0:1]


def solution(mesh):
    num_dev = mesh.shape[GRAPH_AXIS]

    def params(cid=None):
        if cid is None:
            return pltpu.CompilerParams(vmem_limit_bytes=VMEM_BYTES)
        return pltpu.CompilerParams(vmem_limit_bytes=VMEM_BYTES, collective_id=cid, has_side_effects=True)

    def arr(dtype, *shape):
        return jax.ShapeDtypeStruct(shape, dtype)

    def scr(dtype, *shape):
        return pltpu.VMEM(shape, dtype)

    def dma(count):
        return pltpu.SemaphoreType.DMA((2, count))

    I32 = jnp.int32

    def device_step(node_feats, w_one, w_two, send_rows, edge_src, edge_dst, edge_w, labels, label_mask):
        rows, feats = node_feats.shape
        width = w_one.shape[1]
        halo = send_rows.shape[1]
        edges = edge_src.shape[0]
        own_hi, all_hi = rows // LANES, (rows + 2 * halo) // LANES
        feats_t, w2 = node_feats.T, w_two.T
        src2, dst2, ew2 = (a.reshape(edges // LANES, LANES) for a in (edge_src, edge_dst, edge_w))
        lab2, mask2 = labels.reshape(own_hi, LANES), label_mask.reshape(own_hi, LANES)
        listed = (LIST_ROWS, LANES)
        entries = LIST_ROWS * LANES
        fast_list = pltpu.SMEM(listed, I32)
        list_dma = dma(entries // CHUNK)

        late_rows = rows - EARLY_ROWS
        busy = pl.CostEstimate(flops=8 * 10**9, bytes_accessed=10**7, transcendentals=0)
        own_t, to_next, to_prev = pl.pallas_call(
            k1_body,
            out_shape=(arr(BF16, width, rows), arr(BF16, halo, width), arr(BF16, halo, width)),
            in_specs=[pl.BlockSpec(memory_space=pltpu.HBM)] * 3, out_specs=(vmem(),) * 3,
            scratch_shapes=[scr(BF16, feats, rows), scr(F32, feats, width), pltpu.VMEM((2, halo), I32),
                            scr(BF16, 2 * halo, rows), pltpu.SemaphoreType.DMA((3,))],
            compiler_params=pltpu.CompilerParams(vmem_limit_bytes=K1_VMEM), name="transform",
        )(feats_t, w_one, send_rows)
        from_prev = lax.ppermute(to_next, GRAPH_AXIS, [(g, (g + 1) % num_dev) for g in range(num_dev)])
        from_next = lax.ppermute(to_prev, GRAPH_AXIS, [(g, (g - 1) % num_dev) for g in range(num_dev)])

        bufs, own_bufs = ([scr(F32, 2 * rows, LANES)] * n for n in (NUM_BUFS, OWN_BUFS))
        fast_row = pltpu.SMEM((8, LANES), I32)
        lists_in = (arr(I32, *listed), arr(I32, *listed), arr(I32, *listed), arr(F32, *listed), arr(I32, 8, LANES))
        part_own, lsrc, ldst, lpair, lw, num = pl.pallas_call(
            k2a_body,
            out_shape=(arr(F32, rows, width),) + lists_in,
            in_specs=[vmem()] * 4, out_specs=(vmem(),) * 6,
            scratch_shapes=[scr(I32, edges // LANES, LANES), scr(F32, 6 * LIST_ROWS, LANES), scr(F32, 2 * rows, LANES),
                            scr(F32, entries, LANES), fast_row, fast_row, fast_row, fast_row, fast_row,
                            pltpu.SemaphoreType.DMA((1,)), dma(2)] + own_bufs,
            compiler_params=pltpu.CompilerParams(vmem_limit_bytes=OWN_VMEM), cost_estimate=busy, name="aggregate_own",
        )(own_t, src2, dst2, ew2)

        hid, pos_a, pos_b, tab = pl.pallas_call(
            k2b_body,
            out_shape=(arr(BF16, rows, width), arr(BF16, EARLY_ROWS, width), arr(BF16, late_rows, width),
                       arr(F32, own_hi * CLASS_ROWS, LANES)),
            in_specs=[vmem(), vmem(), vmem(), hbm(), hbm(), smem(), vmem(), vmem()], out_specs=(vmem(),) * 4,
            scratch_shapes=[scr(F32, 4 * halo, LANES), scr(F32, entries, LANES), fast_list, fast_list, list_dma] + bufs,
            compiler_params=params(), name="aggregate_halo",
        )(part_own, from_prev, from_next, lsrc, ldst, num, lw, w2)

        num_z = num_dev // PLANE
        tab_b = arr(BF16, own_hi * CLASS_ROWS, LANES)
        pos_early = arr(BF16, EARLY_ROWS, width)
        list_i = arr(I32, *listed)
        (d_tab, misc, d_prev, d_next, prev_a, next_a, dst_prev, dst_next, put_prev, put_next, w_prev, w_next,
         nums, names) = pl.pallas_call(
            functools.partial(k3_body, num_dev),
            out_shape=(tab_b, arr(F32, 16, width), tab_b, tab_b, pos_early, pos_early, list_i, list_i, list_i, list_i,
                       arr(F32, *listed), arr(F32, *listed), arr(I32, 8, LANES), arr(I32, 2 * halo // LANES, LANES)),
            in_specs=[vmem()] * 12, out_specs=(vmem(),) * 14,
            scratch_shapes=[scr(I32, 2, *listed), scr(I32, 2, 8, LANES), scr(BF16, all_hi * CLASS_ROWS, LANES),
                            scr(BF16, 2, 16, halo), scr(BF16, 2, 16, halo), scr(F32, 2, CLASS_ROWS, halo),
                            scr(F32, 2, CLASS_ROWS, halo), scr(F32, own_hi * 24, LANES), scr(F32, all_hi * 24, LANES),
                            scr(F32, own_hi * 24, LANES), scr(BF16, 3 * own_hi * CLASS_ROWS, LANES),
                            scr(F32, 2, 8, LANES), scr(F32, PLANE + num_z - 2, 8, LANES),
                            dma(4), dma(PLANE + num_z - 2), dma(8), dma(6)],
            compiler_params=params(1), name="layer_two",
        )(tab, send_rows, src2, dst2, ew2, lab2, mask2, hid, pos_a, lpair, lw, num)

        pos_b_late, d_tab = lax.optimization_barrier((pos_b, d_tab))
        prev_b = lax.ppermute(pos_b_late, GRAPH_AXIS, [(g, (g + 1) % num_dev) for g in range(num_dev)])
        next_b = lax.ppermute(pos_b_late, GRAPH_AXIS, [(g, (g - 1) % num_dev) for g in range(num_dev)])
        part_own = pl.pallas_call(
            k4a_body,
            out_shape=arr(F32, rows, width),
            in_specs=[hbm(), hbm(), smem()] + [vmem()] * 5, out_specs=vmem(),
            scratch_shapes=[scr(F32, 2 * rows, LANES), scr(F32, entries, LANES), fast_row, fast_row, fast_row, fast_row,
                            dma(2)] + own_bufs,
            compiler_params=pltpu.CompilerParams(vmem_limit_bytes=OWN_VMEM), cost_estimate=busy, name="scatter_own",
        )(ldst, lsrc, num, lw, pos_a, pos_b, d_tab, w2)

        sum_rows_pad = 512
        part = pl.pallas_call(
            k4b_body,
            out_shape=arr(F32, sum_rows_pad, width),
            in_specs=[vmem(), smem(), smem()] + [hbm(), hbm(), vmem()] * 2 + [vmem()] * 9, out_specs=vmem(),
            scratch_shapes=[scr(F32, 2 * rows, LANES), scr(F32, entries, LANES), scr(BF16, rows, width)]
            + [fast_list] * 4 + [list_dma] * 2 + bufs,
            compiler_params=params(), name="scatter_peers",
        )(part_own, nums, names.reshape(2 * halo), dst_prev, put_prev, w_prev,
          dst_next, put_next, w_next,
          d_prev, prev_a, prev_b, d_next, next_a, next_b, w2, feats_t, misc)

        n1, n2 = sum_rows_pad // 2, sum_rows_pad // 8
        n3 = n2 // num_z
        full = pl.pallas_call(
            functools.partial(k5_body, num_dev),
            out_shape=arr(F32, sum_rows_pad, width),
            in_specs=[vmem()], out_specs=vmem(),
            scratch_shapes=[scr(F32, n1, width), scr(F32, 3, n2, width), scr(F32, num_z - 1, n3, width),
                            scr(F32, n1, width), scr(F32, n2, width), dma(4 * (1 + 3 + num_z - 1))],
            compiler_params=params(2), name="sum_gradients",
        )(part)
        loss, grad_one, grad_two = pl.pallas_call(
            k6_body,
            out_shape=(arr(F32, 1, 1), arr(F32, feats, width), arr(F32, w2.shape[0], width)),
            in_specs=[vmem()], out_specs=(vmem(),) * 3, compiler_params=params(), name="outputs",
        )(full)
        return loss.reshape(()), grad_one, grad_two.T

    row_spec = P(GRAPH_AXIS)
    return jax.shard_map(device_step, mesh=mesh,
                         in_specs=(row_spec, P(), P(), row_spec, row_spec, row_spec, row_spec, row_spec, row_spec),
                         out_specs=(P(), P(), P()), check_vma=False)
```

```python
import functools

import jax
import jax.numpy as jnp
from jax import lax
from jax.experimental import pallas as pl
from jax.experimental.pallas import tpu as pltpu
from jax.sharding import PartitionSpec as P

GRAPH_AXIS = "graph"
MESH = pl.DeviceIdType.MESH
LANES = 128
CLASS_ROWS = 8
VMEM_BYTES = 28 * 2**20
K1_VMEM = 50 * 2**20
OWN_VMEM = 34 * 2**20
F32 = jnp.float32
BF16 = jnp.bfloat16
NT = (((1,), (1,)), ((), ()))
TN = (((0,), (0,)), ((), ()))


def vmem():
    return pl.BlockSpec(memory_space=pltpu.VMEM)


def hbm():
    return pl.BlockSpec(memory_space=pl.ANY)


def smem():
    return pl.BlockSpec(memory_space=pltpu.SMEM)


PLANE = 8
LIST_ROWS = 80
BLOCK = 128
NUM_BUFS = 4
OWN_BUFS = 6
EARLY_ROWS = 768
CHUNK = 1024


def ring_peers(num_dev):
    me = lax.axis_index(GRAPH_AXIS)
    return me, (me + 1) % num_dev, (me + num_dev - 1) % num_dev


def layer_peers(me, num_dev):
    return [(me + PLANE * k) % num_dev for k in range(1, num_dev // PLANE)]


def class_weights(w_ref):
    w = w_ref[...]
    return jnp.concatenate([w, jnp.zeros((CLASS_ROWS - w.shape[0], w.shape[1]), F32)], axis=0).astype(BF16)


def meet(partners):
    barrier = pltpu.get_barrier_semaphore()
    for dev in partners:
        pl.semaphore_signal(barrier, inc=1, device_id=(dev,), device_id_type=MESH)
    pl.semaphore_wait(barrier, len(partners))


def remote(src, dst, sems, slot, dev):
    return pltpu.make_async_remote_copy(
        src_ref=src, dst_ref=dst, send_sem=sems.at[0, slot], recv_sem=sems.at[1, slot],
        device_id=(dev,), device_id_type=MESH)


def three_pieces(val):
    top = val.astype(BF16).astype(F32)
    rest = val - top
    mid = rest.astype(BF16).astype(F32)
    return top, mid, rest - mid


def wide_row(ref, first):
    blk = ref[pl.ds(first, 8), :]
    return jnp.concatenate([blk[j:j + 1, :] for j in range(8)], axis=1)


def packed(row):
    return jnp.broadcast_to(row, (16, row.shape[1])).astype(jnp.int16)


def hot_rows(row, count):
    n = row.shape[1]
    ids = lax.broadcasted_iota(jnp.int32, (count, LANES), 0).astype(jnp.int16)
    return jnp.concatenate([ids] * (n // LANES), axis=1) == jnp.concatenate([packed(row)] * (count // 16), axis=0)


def ones_at(mask):
    return jnp.where(mask, jnp.ones((), BF16), jnp.zeros((), BF16))


def lo_hot(idx):
    return ones_at(hot_rows(idx & (LANES - 1), LANES))


def list_places(src_ref, w_ref, rows, halo, pos, num_ref):
    src, live = src_ref[...], w_ref[...] != 0.0
    n_rows = src.shape[0]
    tri = (lax.broadcasted_iota(jnp.int32, (LANES, LANES), 0) <= lax.broadcasted_iota(jnp.int32, (LANES, LANES), 1))
    tri = tri.astype(F32).astype(BF16)
    low = (lax.broadcasted_iota(jnp.int32, (n_rows, n_rows), 1) < lax.broadcasted_iota(jnp.int32, (n_rows, n_rows), 0))
    low = low.astype(F32).astype(BF16)
    place = jnp.full(src.shape, LIST_ROWS * LANES, jnp.int32)
    start = jnp.zeros((1, 1), jnp.int32)
    lane = lax.broadcasted_iota(jnp.int32, num_ref.shape, 1)
    num = jnp.zeros(num_ref.shape, jnp.int32)
    kinds = (src < rows, (src >= rows) & (src < rows + halo), src >= rows + halo)
    for k, kind in enumerate(kinds):
        kind = kind & live
        flag = kind.astype(F32)
        inner = jnp.dot(flag.astype(BF16), tri, preferred_element_type=F32)
        row_sum = jnp.broadcast_to(jnp.sum(flag, axis=1, keepdims=True), flag.shape)
        before = jnp.dot(low, row_sum.astype(BF16), preferred_element_type=F32)
        rank = (inner + before).astype(jnp.int32) - 1
        place = jnp.where(kind, start + rank, place)
        total = jnp.sum(jnp.sum(flag, axis=1, keepdims=True), axis=0, keepdims=True).astype(jnp.int32)
        blocks = lax.shift_right_logical(total + (BLOCK - 1), BLOCK.bit_length() - 1)
        start = start + blocks * BLOCK
        num = jnp.where(lane == k, blocks, num)
    pos[...] = place
    num_ref[...] = num


def k1_body(xt_hbm, w_hbm, send_hbm, own_t_ref, to_next_ref, to_prev_ref, xt_ref, w_ref, send_ref, hot, sems):
    copies = [pltpu.make_async_copy(a, b, sems.at[k])
              for k, (a, b) in enumerate(((send_hbm, send_ref), (w_hbm, w_ref), (xt_hbm, xt_ref)))]
    for copy in copies:
        copy.start()
    copies[0].wait()
    halo = send_ref.shape[1]
    rows = xt_ref.shape[1]
    blocks = halo // LANES
    ids = jnp.concatenate([send_ref[r:r + 1, b * LANES:(b + 1) * LANES] for r in range(2) for b in range(blocks)], axis=0)
    ids_col = jnp.transpose(ids)
    node = lax.broadcasted_iota(jnp.int32, (LANES, rows), 1).astype(jnp.int16)
    for b in range(2 * blocks):
        col = jnp.broadcast_to(ids_col[:, b:b + 1], (LANES, LANES)).astype(jnp.int16)
        hot[b * LANES:(b + 1) * LANES, :] = ones_at(node == jnp.concatenate([col] * (rows // LANES), axis=1))
    copies[1].wait()
    w_b = w_ref[...].astype(BF16)
    copies[2].wait()
    own_t_ref[...] = lax.dot_general(w_b, xt_ref[...], TN, preferred_element_type=F32).astype(BF16)
    for r, out in ((1, to_next_ref), (0, to_prev_ref)):
        out[...] = lax.dot_general(hot[r * halo:(r + 1) * halo, :], own_t_ref[...], NT, preferred_element_type=F32).astype(BF16)


def sort_edges(src_ref, dst_ref, ew_ref, rows, halo, pos, acc, lsrc_ref, ldst_ref, lpair_ref, lw_ref, num_ref):
    list_places(src_ref, ew_ref, rows, halo, pos, num_ref)
    acc[...] = jnp.zeros_like(acc)

    def sort(i, carry):
        first = pl.multiple_of(i * 8, 8)
        src, dst, wgt, place = (wide_row(ref, first) for ref in (src_ref, dst_ref, ew_ref, pos))
        both = src + dst * 4096
        ints = [both & 255, lax.shift_right_logical(both, 8) & 255, lax.shift_right_logical(both, 16)]
        cargo = [v.astype(F32) for v in ints] + list(three_pieces(wgt))
        here = hot_rows(lax.shift_right_logical(place, 7), LIST_ROWS)
        cargo = [jnp.concatenate([jnp.broadcast_to(v, (16, v.shape[1])).astype(BF16)] * (LIST_ROWS // 16), axis=0) for v in cargo]
        lhs = jnp.concatenate([jnp.where(here, v, jnp.zeros((), BF16)) for v in cargo], axis=0)
        acc[...] += lax.dot_general(lhs, lo_hot(place), NT, preferred_element_type=F32)
        return carry

    lax.fori_loop(0, src_ref.shape[0] // 8, sort, 0)
    got = [acc[p * LIST_ROWS:(p + 1) * LIST_ROWS, :] for p in range(6)]
    ints = [g.astype(jnp.int32) for g in got[:3]]
    both = ints[0] + ints[1] * 256 + ints[2] * 65536
    src, dst = both & 4095, lax.shift_right_logical(both, 12) * 2
    src = jnp.where(src < rows, src, src - rows)
    lsrc_ref[...] = src * 2
    ldst_ref[...] = dst
    lpair_ref[...] = dst + src * 65536
    lw_ref[...] = got[3] + got[4] + got[5]


def spread_weights(w_ref, wide, first, last):
    def body(g, carry):
        cols = jnp.transpose(w_ref[pl.ds(pl.multiple_of(g * 8, 8), 8), :])
        for j in range(8):
            at = pl.ds(pl.multiple_of(g * 8 * LANES + j * LANES, LANES), LANES)
            wide[at, :] = jnp.broadcast_to(cols[:, j:j + 1], (LANES, LANES))
        return carry

    lax.fori_loop(first // 8, (last + 7) // 8, body, 0)


def clear_rows(bufs):
    def body(i, carry):
        for buf in bufs:
            buf[pl.ds(pl.multiple_of(i * 64, 64), 64), :] = jnp.zeros((64, LANES), F32)
        return carry

    lax.fori_loop(0, bufs[0].shape[0] // 64, body, 0)


def chunk_copies(lists, fast, sems, c):
    at = pl.ds(pl.multiple_of(c * 8, 8), CHUNK // LANES)
    return [pltpu.make_async_copy(a.at[at, :], b.at[at, :], sems.at[k, c]) for k, (a, b) in enumerate(zip(lists, fast))]


def chunks_of(first, last):
    per = CHUNK // BLOCK
    return first // per, (last + per - 1) // per


def start_lists(lists, fast, sems, first, last):
    def body(c, carry):
        for copy in chunk_copies(lists, fast, sems, c):
            copy.start()
        return carry

    lax.fori_loop(*chunks_of(first, last), body, 0)


def row_loop(lists, fast, sems, wide, table, bufs, first, last, rename=None):
    num = len(bufs)
    take_ref, put_ref = fast
    per = CHUNK // BLOCK

    def step(i, carry):
        base = i * BLOCK
        for lead in range(0, BLOCK, num):
            take = [pl.multiple_of(take_ref[i, lead + j], 2) for j in range(num)]
            put = [put_ref[i, lead + j] for j in range(num)]
            if rename is not None:
                put = [rename[p] for p in put]
            put = [pl.multiple_of(p, 2) for p in put]
            vals = [wide[pl.ds(base + lead + j, 1), :] * table[pl.ds(take[j], 2), :] for j in range(num)]
            old = [bufs[j][pl.ds(put[j], 2), :] for j in range(num)]
            for j in range(num):
                bufs[j][pl.ds(put[j], 2), :] = old[j] + vals[j]
        return carry

    def chunk(c, carry):
        for copy in chunk_copies(lists, fast, sems, c):
            copy.wait()
        return lax.fori_loop(jnp.maximum(first, c * per), jnp.minimum(last, c * per + per), step, carry)

    lax.fori_loop(*chunks_of(first, last), chunk, 0)


def slot_copies(lists, slots, sems, c):
    at = pl.ds(pl.multiple_of(c * 8, 8), 8)
    return lambda slot: [pltpu.make_async_copy(a.at[at, :], b, sems.at[slot, k]) for k, (a, b) in enumerate(zip(lists, slots[slot]))]


def start_slots(lists, slots, sems):
    for slot in range(2):
        for copy in slot_copies(lists, slots, sems, slot)(slot):
            copy.start()


def slot_loop(lists, slots, sems, wide, table, bufs, last):
    num = len(bufs)
    pairs = jnp.maximum((last + 15) // 16, 1)

    def group(k, carry):
        for slot in range(2):
            take_ref, put_ref = slots[slot]
            for copy in slot_copies(lists, slots, sems, 2 * k + slot)(slot):
                copy.wait()
            for r in range(8):
                row = 16 * k + 8 * slot + r

                @pl.when(row < last)
                def _():
                    base = pl.multiple_of(row * LANES, LANES)
                    for lead in range(0, LANES, num):
                        here = range(min(num, LANES - lead))
                        take = [pl.multiple_of(take_ref[r, lead + j], 2) for j in here]
                        put = [pl.multiple_of(put_ref[r, lead + j], 2) for j in here]
                        vals = [wide[pl.ds(base + lead + j, 1), :] * table[pl.ds(take[j], 2), :] for j in here]
                        old = [bufs[j][pl.ds(put[j], 2), :] for j in here]
                        for j in here:
                            bufs[j][pl.ds(put[j], 2), :] = old[j] + vals[j]

            @pl.when(k + 1 < pairs)
            def _():
                for copy in slot_copies(lists, slots, sems, 2 * k + 2 + slot)(slot):
                    copy.start()
        return carry

    lax.fori_loop(0, pairs, group, 0)


def list_rows(first, last):
    return first * BLOCK // LANES, (last * BLOCK + LANES - 1) // LANES


def to_rows(blk, table, first_row):
    for h in range(2):
        table[pl.ds(2 * first_row + h, blk.shape[0], stride=2), :] = blk[:, h * LANES:(h + 1) * LANES]


def sum_rows(bufs, blk):
    halves = []
    for h in range(2):
        parts = [buf[pl.ds(2 * blk * LANES + h, LANES, stride=2), :] for buf in bufs]
        while len(parts) > 1:
            parts = [a + b for a, b in zip(parts[::2], parts[1::2])] + parts[len(parts) // 2 * 2:]
        halves.append(parts[0])
    return jnp.concatenate(halves, axis=1)


def k2a_body(own_t_ref, src_ref, dst_ref, ew_ref, part_ref, lsrc_ref, ldst_ref, lpair_ref, lw_ref, num_ref,
             pos, acc, table, wide, num_fast, src_a, dst_a, src_b, dst_b, sems, slot_sems, *bufs):
    rows = part_ref.shape[0]
    sort_edges(src_ref, dst_ref, ew_ref, rows, rows // 2, pos, acc, lsrc_ref, ldst_ref, lpair_ref, lw_ref, num_ref)

    def widen(i, carry):
        at = pl.ds(pl.multiple_of(i * LANES, LANES), LANES)
        to_rows(jnp.transpose(own_t_ref[:, at].astype(F32)), table, i * LANES)
        return carry

    lax.fori_loop(0, rows // LANES, widen, 0)
    copy = pltpu.make_async_copy(num_ref, num_fast, sems.at[0])
    copy.start()
    lists, slots = (lsrc_ref, ldst_ref), ((src_a, dst_a), (src_b, dst_b))
    start_slots(lists, slots, slot_sems)
    clear_rows(bufs)
    copy.wait()
    end = num_fast[0, 0]
    spread_weights(lw_ref, wide, *list_rows(0, end))
    slot_loop(lists, slots, slot_sems, wide, table, bufs, end)

    def finish(i, carry):
        part_ref[pl.ds(pl.multiple_of(i * LANES, LANES), LANES), :] = sum_rows(bufs, i)
        return carry

    lax.fori_loop(0, rows // LANES, finish, 0)


def k2b_body(part_ref, prev_ref, next_ref, lsrc_ref, ldst_ref, num_ref, lw_ref, w2_ref,
             hid_ref, pos_a_ref, pos_b_ref, tab_ref, table, wide, src_fast, dst_fast, sems, *bufs):
    first = num_ref[0, 0]
    end = first + num_ref[0, 1] + num_ref[0, 2]
    lists, fast = (lsrc_ref, ldst_ref), (src_fast, dst_fast)
    start_lists(lists, fast, sems, first, end)
    spread_weights(lw_ref, wide, *list_rows(first, end))
    halo = prev_ref.shape[0]

    def widen(i, carry):
        at = pl.ds(pl.multiple_of(i * LANES, LANES), LANES)
        to_rows(prev_ref[at, :].astype(F32), table, i * LANES)
        to_rows(next_ref[at, :].astype(F32), table, halo + i * LANES)
        return carry

    lax.fori_loop(0, halo // LANES, widen, 0)
    clear_rows(bufs)
    row_loop(lists, fast, sems, wide, table, bufs, first, end)
    w2t = class_weights(w2_ref)

    for pos_ref, lead in ((pos_a_ref, 0), (pos_b_ref, pos_a_ref.shape[0] // LANES)):
        def finish(j, carry):
            i = lead + j
            at = pl.ds(pl.multiple_of(i * LANES, LANES), LANES)
            pre = part_ref[at, :] + sum_rows(bufs, i)
            hid = jnp.maximum(pre, 0.0).astype(BF16)
            hid_ref[at, :] = hid
            pos_ref[pl.ds(pl.multiple_of(j * LANES, LANES), LANES), :] = (pre > 0.0).astype(F32).astype(BF16)
            t2 = lax.dot_general(w2t, hid, NT, preferred_element_type=F32)
            tab_ref[pl.ds(pl.multiple_of(i * CLASS_ROWS, CLASS_ROWS), CLASS_ROWS), :] = t2.astype(BF16).astype(F32)
            return carry

        lax.fori_loop(0, pos_ref.shape[0] // LANES, finish, 0)


def stack_classes(w2_ref, blocks):
    w2_all = jnp.concatenate([class_weights(w2_ref).astype(F32)] * blocks, axis=0)
    return w2_all, lax.shift_right_logical(lax.broadcasted_iota(jnp.int32, w2_all.shape, 0), 3)


def fill_table(dt, pos_refs, w2_all, group, table):
    dt_cols = jnp.transpose(dt).astype(BF16)
    for pos_ref, lead in zip(pos_refs, (0, pos_refs[0].shape[0] // LANES)):
        def widen(j, carry):
            i = lead + j
            d_hid = jnp.dot(dt_cols, jnp.where(group == i, w2_all, 0.0).astype(BF16), preferred_element_type=F32)
            at = pl.ds(pl.multiple_of(j * LANES, LANES), LANES)
            to_rows(jnp.where(pos_ref[at, :].astype(F32) > 0.0, d_hid, 0.0), table, i * LANES)
            return carry

        lax.fori_loop(0, pos_ref.shape[0] // LANES, widen, 0)


def k4a_body(ldst_ref, lsrc_ref, num_ref, lw_ref, pos_a_ref, pos_b_ref, dt_ref, w2_ref, part_ref,
             table, wide, take_a, put_a, take_b, put_b, slot_sems, *bufs):
    rows = part_ref.shape[0]
    lists, slots, end = (ldst_ref, lsrc_ref), ((take_a, put_a), (take_b, put_b)), num_ref[0, 0]
    start_slots(lists, slots, slot_sems)
    w2_all, group = stack_classes(w2_ref, rows // LANES)
    clear_rows(bufs)
    fill_table(dt_ref[...].astype(F32), (pos_a_ref, pos_b_ref), w2_all, group, table)
    spread_weights(lw_ref, wide, *list_rows(0, end))
    slot_loop(lists, slots, slot_sems, wide, table, bufs, end)

    def finish(i, carry):
        part_ref[pl.ds(pl.multiple_of(i * LANES, LANES), LANES), :] = sum_rows(bufs, i)
        return carry

    lax.fori_loop(0, rows // LANES, finish, 0)


def k4b_body(part_ref, num_ref, names_ref, prev_dst, prev_src, prev_w, next_dst, next_src, next_w,
             prev_a, prev_late, next_a, next_late, w2_ref, xt_ref, misc_ref, out_ref,
             table, wide, d_tab, names, names_sem, *rest):
    fasts, pools, bufs = (rest[0:2], rest[2:4]), rest[4:6], rest[6:]
    rows = part_ref.shape[0]
    late_rows = rows - prev_a.shape[0]
    load = pltpu.make_async_copy(names_ref, names, names_sem)
    load.start()
    sides = (((prev_dst, prev_src), prev_w, prev_late, prev_a, 1, 2),
             ((next_dst, next_src), next_w, next_late, next_a, 2, 1))
    spans = []
    for (lists, _, _, _, row, kind), fast, pool in zip(sides, fasts, pools):
        first = num_ref[row, 0]
        if kind == 2:
            first = first + num_ref[row, 1]
        spans.append((first, first + num_ref[row, kind]))
        start_lists(lists, fast, pool, *spans[-1])
    w2_all, group = stack_classes(w2_ref, rows // LANES)
    clear_rows(bufs)
    for (lists, w_ref, late, early, _, _), fast, pool, span in zip(sides, fasts, pools, spans):
        dt = late[late_rows:, :].astype(F32)
        dt = jnp.concatenate([dt[:, 0:LANES], dt[:, LANES:]], axis=0)
        fill_table(dt, (early, late.at[0:late_rows, :]), w2_all, group, table)
        spread_weights(w_ref, wide, *list_rows(*span))
        if late is prev_late:
            load.wait()
        row_loop(lists, fast, pool, wide, table, bufs, *span, rename=names)

    def finish(i, carry):
        at = pl.ds(pl.multiple_of(i * LANES, LANES), LANES)
        d_tab[at, :] = (part_ref[at, :] + sum_rows(bufs, i)).astype(BF16)
        return carry

    lax.fori_loop(0, rows // LANES, finish, 0)
    feats = xt_ref.shape[0]
    out_ref[0:feats, :] = jnp.dot(xt_ref[...], d_tab[...], preferred_element_type=F32)
    out_ref[feats:feats + 12, :] = misc_ref[0:12, :]


def hi_of(idx):
    return jnp.broadcast_to(lax.shift_right_logical(idx, 7), (CLASS_ROWS, idx.shape[1]))


def pick_cols(table_b, pieces, idx, hot, first=0):
    cols = jnp.dot(table_b, hot, preferred_element_type=F32)
    rows = table_b.shape[0] // pieces
    hi = hi_of(idx) - first
    out = jnp.zeros(hi.shape, F32)
    for h in range(rows // CLASS_ROWS):
        part = cols[h * CLASS_ROWS:(h + 1) * CLASS_ROWS]
        for p in range(1, pieces):
            part = part + cols[p * rows + h * CLASS_ROWS:p * rows + (h + 1) * CLASS_ROWS]
        out = out + jnp.where(hi == h, part, 0.0)
    return out


def add_cols(val, idx, hot, num_hi, first=0):
    hi = packed(lax.shift_right_logical(idx, 7) - first)
    low_half = lax.broadcasted_iota(jnp.int32, hi.shape, 0) >= CLASS_ROWS
    mixed = hi - low_half.astype(jnp.int32).astype(jnp.int16)
    top, mid, low = three_pieces(val)
    pieces = [jnp.concatenate(two, axis=0).astype(BF16) for two in ((top, mid), (low, top), (mid, low))]
    rows = []
    for h in range(0, num_hi, 2):
        masks = (hi == jnp.int16(h), mixed == jnp.int16(h), hi == jnp.int16(h + 1))
        rows += [jnp.where(m, p, jnp.zeros((), BF16)) for m, p in zip(masks, pieces)]
    return lax.dot_general(jnp.concatenate(rows, axis=0), hot, NT, preferred_element_type=F32)


def join_pieces(acc, num_hi):
    out = []
    for h in range(num_hi):
        a = acc[h * 24:h * 24 + 24, :]
        out.append(a[0:8] + a[8:16] + a[16:24])
    return out


def stack_pieces(val):
    return jnp.concatenate(three_pieces(val), axis=0).astype(BF16)


def k3_body(num_dev, tab_ref, send_ref, src_ref, dst_ref, w_ref, lab_ref, mask_ref, hid_ref, pos_ref, pos_late_ref,
            lpair_ref, lw_ref, num_ref,
            dt_ref, misc_ref, late_ref, pos_prev_ref, pos_next_ref, dst_prev_ref, dst_next_ref,
            put_prev_ref, put_next_ref, w_prev_ref, w_next_ref, nums_ref, names_ref, pairs, nums,
            ext_b, fwd_send, fwd_recv, bwd_send, bwd_recv, vals, acc_z, acc_s, acc_o, acc_r, dz_b, cnt_send, cnt_recv,
            sems, cnt_sems, list_sems, pos_sems):
    me, nxt, prv = ring_peers(num_dev)
    layers = layer_peers(me, num_dev)
    layer = [me - me % PLANE + (me % PLANE + k) % PLANE for k in range(1, PLANE)]
    meet([nxt, prv] + layer + layers)
    total = jnp.sum(jnp.sum(mask_ref[...].astype(F32), axis=1, keepdims=True), axis=0, keepdims=True)
    cnt_send[0] = jnp.broadcast_to(total, cnt_send.shape[1:])
    counts = [remote(cnt_send.at[0], cnt_recv.at[k], cnt_sems, k, dev) for k, dev in enumerate(layer)]
    for copy in counts:
        copy.start()
    late = []

    def send_late(pairs, pool, first):
        for k, (src, dst) in enumerate(pairs):
            for s, dev in enumerate((nxt, prv)):
                copy = remote(src, dst[s], pool, 2 * (first + k) + s, dev)
                copy.start()
                late.append(copy)

    chunk = pos_ref.shape[0] // 3

    def send_pos(q):
        at = pl.ds(q * chunk, chunk)
        send_late([(pos_ref.at[at, :], [pos_prev_ref.at[at, :], pos_next_ref.at[at, :]])], pos_sems, q)

    own_hi = tab_ref.shape[0] // CLASS_ROWS
    halo = send_ref.shape[1]
    halo_hi = halo // LANES
    all_hi = own_hi + 2 * halo_hi
    own_b = tab_ref[...].astype(BF16)
    ext_b[pl.ds(0, own_hi * CLASS_ROWS), :] = own_b
    hot_send = [lo_hot(send_ref[r:r + 1, :]) for r in range(2)]
    copies = []
    for r in (1, 0):
        val = pick_cols(own_b, 1, send_ref[r:r + 1, :], hot_send[r])
        fwd_send[r] = jnp.concatenate([val, jnp.zeros_like(val)], axis=0).astype(BF16)
        copy = remote(fwd_send.at[r], fwd_recv.at[1 - r], sems, r, nxt if r == 1 else prv)
        copy.start()
        copies.append(copy)
    send_late([(lpair_ref, [pairs.at[0], pairs.at[1]]), (lw_ref, [w_prev_ref, w_next_ref]),
               (num_ref, [nums.at[0], nums.at[1]])], list_sems, 0)
    send_pos(0)
    for copy in counts:
        copy.wait()
    for k in range(len(layer)):
        total = total + cnt_recv[k][0:1, 0:1]
    cnt_send[1] = jnp.broadcast_to(total, cnt_send.shape[1:])
    counts = [remote(cnt_send.at[1], cnt_recv.at[len(layer) + k], cnt_sems, len(layer) + k, dev)
              for k, dev in enumerate(layers)]
    for copy in counts:
        copy.start()
    send_pos(1)
    send_pos(2)
    acc_z[...] = jnp.zeros_like(acc_z)
    acc_s[...] = jnp.zeros_like(acc_s)
    acc_o[...] = jnp.zeros_like(acc_o)
    late_rows = pos_late_ref.shape[0]
    late_ref[0:late_rows, :] = pos_late_ref[...]
    steps = src_ref.shape[0] // 8

    def own_forward(i, carry):
        src = wide_row(src_ref, pl.multiple_of(i * 8, 8))
        vals[i] = pick_cols(ext_b[0:own_hi * CLASS_ROWS, :], 1, src, lo_hot(src))
        return carry

    lax.fori_loop(0, steps, own_forward, 0)
    for copy in copies:
        copy.wait()
    for r in range(2):
        got = fwd_recv[r].astype(F32)
        for j in range(0, halo_hi, 2):
            two = jnp.concatenate([got[0:8, (j + k) * LANES:(j + k + 1) * LANES] for k in range(2)], axis=0)
            ext_b[pl.ds((own_hi + r * halo_hi + j) * CLASS_ROWS, 16), :] = two.astype(BF16)


    def forward(i, carry):
        first = pl.multiple_of(i * 8, 8)
        src, dst = wide_row(src_ref, first), wide_row(dst_ref, first)
        val = vals[i] + pick_cols(ext_b[own_hi * CLASS_ROWS:, :], 1, src, lo_hot(src), own_hi)
        val = val * wide_row(w_ref, first)
        acc_z[...] += add_cols(val, dst, lo_hot(dst), own_hi)
        return carry

    lax.fori_loop(0, steps, forward, 0)

    logits = join_pieces(acc_z[...], own_hi)
    cls = lax.broadcasted_iota(jnp.int32, (CLASS_ROWS, LANES), 0)
    count = jnp.broadcast_to(total, (1, LANES))
    for k, copy in enumerate(counts):
        copy.wait()
        count = count + cnt_recv[len(layer) + k][0:1, :]
    count = jnp.maximum(count, 1.0)
    loss = jnp.zeros((1, LANES), F32)
    d_log = []
    for h in range(own_hi):
        z = jnp.where(cls < 7, logits[h], -jnp.inf)
        top = jnp.max(z, axis=0, keepdims=True)
        norm = jnp.log(jnp.sum(jnp.exp(z - top), axis=0, keepdims=True)) + top
        hot = cls == lab_ref[h:h + 1, :]
        mask = mask_ref[h:h + 1, :].astype(F32)
        picked = jnp.sum(jnp.where(hot, logits[h], 0.0), axis=0, keepdims=True)
        loss = loss + mask * (norm - picked)
        d_log.append((jnp.exp(z - norm) - hot.astype(F32)) * (mask / count))
    dz_b[...] = stack_pieces(jnp.concatenate(d_log, axis=0))

    def backward(i, carry):
        first = pl.multiple_of(i * 8, 8)
        src, dst = wide_row(src_ref, first), wide_row(dst_ref, first)
        val = pick_cols(dz_b[...], 3, dst, lo_hot(dst)) * wide_row(w_ref, first)
        vals[i] = val
        acc_s[...] += add_cols(val, src, lo_hot(src), 2 * halo_hi, own_hi)
        return carry

    lax.fori_loop(0, steps, backward, 0)

    d_halo = join_pieces(acc_s[...], 2 * halo_hi)
    copies = []
    for r in range(2):
        for j in range(halo_hi):
            bwd_send[r, :, j * LANES:(j + 1) * LANES] = d_halo[r * halo_hi + j]
        copy = remote(bwd_send.at[r], bwd_recv.at[1 - r], sems, 2 + r, prv if r == 0 else nxt)
        copy.start()
        copies.append(copy)

    def own_backward(i, carry):
        src = wide_row(src_ref, pl.multiple_of(i * 8, 8))
        acc_o[...] += add_cols(vals[i], src, lo_hot(src), own_hi)
        return carry

    lax.fori_loop(0, steps, own_backward, 0)
    d_own = join_pieces(acc_o[...], own_hi)
    for copy in copies:
        copy.wait()
    for r in range(2):
        part = add_cols(bwd_recv[r], send_ref[r:r + 1, :], hot_send[r], own_hi)
        acc_r[...] = part if r == 0 else acc_r[...] + part
    back = join_pieces(acc_r[...], own_hi)
    d_tab = [d_own[h] + back[h] for h in range(own_hi)]
    half = own_hi // 2
    dt_ref[...] = jnp.concatenate(d_tab, axis=0).astype(BF16)
    late_ref[late_rows:, :] = jnp.concatenate(
        [jnp.concatenate(d_tab[:half], axis=0), jnp.concatenate(d_tab[half:], axis=0)], axis=1).astype(BF16)
    grad = jnp.zeros((CLASS_ROWS, hid_ref.shape[1]), F32)
    for h in range(own_hi):
        grad = grad + jnp.dot(d_tab[h].astype(BF16), hid_ref[pl.ds(h * LANES, LANES), :], preferred_element_type=F32)
    misc_ref[0:8, :] = grad
    total = jnp.sum(loss, axis=1, keepdims=True) / count[:, 0:1]
    misc_ref[8:16, :] = jnp.broadcast_to(total, (8, misc_ref.shape[1]))
    for copy in late:
        copy.wait()
    for s, (to_dst, to_put) in enumerate(((dst_prev_ref, put_prev_ref), (dst_next_ref, put_next_ref))):
        to_dst[...] = pairs[s] & 0xFFFF
        to_put[...] = lax.shift_right_logical(pairs[s], 16)
    row = lax.broadcasted_iota(jnp.int32, nums_ref.shape, 0)
    nums_ref[...] = jnp.where(row == 0, num_ref[0:1, :], jnp.where(row == 1, nums[0, 0:1, :], nums[1, 0:1, :]))
    names_ref[...] = 2 * jnp.concatenate(
        [send_ref[r:r + 1, j * LANES:(j + 1) * LANES] for r in (1, 0) for j in range(halo_hi)], axis=0)


def k5_body(num_dev, part_ref, full_ref, land_core, land_chip, land_z, by_core, by_chip, sems):
    me = lax.axis_index(GRAPH_AXIS)
    core, chip, z = me % 2, (me // 2) % 4, me // PLANE
    other = me + 1 - 2 * core
    chips = [me + 2 * ((chip + k) % 4 - chip) for k in range(1, 4)]
    layers = layer_peers(me, num_dev)
    num_z = num_dev // PLANE
    meet([other] + chips + layers)
    rows, width = part_ref.shape
    rows //= 2
    n1, n2, n3 = rows // 2, rows // 8, rows // 8 // num_z
    parts = [(p, pl.ds(c * LANES, LANES)) for p in range(2) for c in range(width // LANES)]
    used = [0]

    def send(pairs):
        out = []
        for src, dst, dev in pairs:
            out.append(remote(src, dst, sems, used[0], dev))
            used[0] += 1
        for copy in out:
            copy.start()
        return out

    def wait(copies):
        for copy in copies:
            copy.wait()

    def at(first, size):
        return pl.ds(pl.multiple_of(first, size), size)

    def run(p, size):
        return pl.ds(p * size, size)

    flying = [send([(part_ref.at[at(p * rows + (1 - core) * n1, n1), c], land_core.at[run(p, n1), c], other)]) for p, c in parts]
    for i, (p, c) in enumerate(parts):
        wait(flying[i])
        by_core[run(p, n1), c] = part_ref[at(p * rows + core * n1, n1), c] + land_core[run(p, n1), c]
        flying[i] = send([(by_core.at[at(p * n1 + (chip + k + 1) % 4 * n2, n2), c], land_chip.at[k, run(p, n2), c], dev)
                          for k, dev in enumerate(chips)])
    for i, (p, c) in enumerate(parts):
        wait(flying[i])
        total = by_core[at(p * n1 + chip * n2, n2), c]
        for k in range(len(chips)):
            total = total + land_chip[k, run(p, n2), c]
        by_chip[run(p, n2), c] = total
        flying[i] = send([(by_chip.at[at(p * n2 + (z + k + 1) % num_z * n3, n3), c], land_z.at[k, run(p, n3), c], dev)
                          for k, dev in enumerate(layers)])
    firsts = (core * n1 + chip * n2 + z * n3, core * n1 + chip * n2, core * n1)
    gathers = list(zip(firsts, (n3, n2, n1), (layers, chips, [other])))

    def gather(level, p, c):
        first, size, devs = gathers[level]
        own = full_ref.at[at(p * rows + first, size), c]
        return send([(own, own, dev) for dev in devs])

    for i, (p, c) in enumerate(parts):
        wait(flying[i])
        total = by_chip[at(p * n2 + z * n3, n3), c]
        for k in range(len(layers)):
            total = total + land_z[k, run(p, n3), c]
        full_ref[at(p * rows + firsts[0], n3), c] = total
        flying[i] = gather(0, p, c)
    for level in (1, 2):
        for i, (p, c) in enumerate(parts):
            wait(flying[i])
            flying[i] = gather(level, p, c)
    for copies in flying:
        wait(copies)


def k6_body(full_ref, loss_ref, one_ref, two_ref):
    feats, classes = one_ref.shape[0], two_ref.shape[0]
    one_ref[...] = full_ref[0:feats, :]
    two_ref[...] = full_ref[feats:feats + classes, :]
    loss_ref[...] = full_ref[feats + 8:feats + 9, 0:1]


def solution(mesh):
    num_dev = mesh.shape[GRAPH_AXIS]

    def params(cid=None):
        if cid is None:
            return pltpu.CompilerParams(vmem_limit_bytes=VMEM_BYTES)
        return pltpu.CompilerParams(vmem_limit_bytes=VMEM_BYTES, collective_id=cid, has_side_effects=True)

    def arr(dtype, *shape):
        return jax.ShapeDtypeStruct(shape, dtype)

    def scr(dtype, *shape):
        return pltpu.VMEM(shape, dtype)

    def dma(count):
        return pltpu.SemaphoreType.DMA((2, count))

    I32 = jnp.int32

    def device_step(node_feats, w_one, w_two, send_rows, edge_src, edge_dst, edge_w, labels, label_mask):
        rows, feats = node_feats.shape
        width = w_one.shape[1]
        halo = send_rows.shape[1]
        edges = edge_src.shape[0]
        own_hi, all_hi = rows // LANES, (rows + 2 * halo) // LANES
        feats_t, w2 = node_feats.T, w_two.T
        src2, dst2, ew2 = (a.reshape(edges // LANES, LANES) for a in (edge_src, edge_dst, edge_w))
        lab2, mask2 = labels.reshape(own_hi, LANES), label_mask.reshape(own_hi, LANES)
        listed = (LIST_ROWS, LANES)
        entries = LIST_ROWS * LANES
        fast_list = pltpu.SMEM(listed, I32)
        list_dma = dma(entries // CHUNK)

        late_rows = rows - EARLY_ROWS
        busy = pl.CostEstimate(flops=8 * 10**9, bytes_accessed=10**7, transcendentals=0)
        own_t, to_next, to_prev = pl.pallas_call(
            k1_body,
            out_shape=(arr(BF16, width, rows), arr(BF16, halo, width), arr(BF16, halo, width)),
            in_specs=[pl.BlockSpec(memory_space=pltpu.HBM)] * 3, out_specs=(vmem(),) * 3,
            scratch_shapes=[scr(BF16, feats, rows), scr(F32, feats, width), pltpu.VMEM((2, halo), I32),
                            scr(BF16, 2 * halo, rows), pltpu.SemaphoreType.DMA((3,))],
            compiler_params=pltpu.CompilerParams(vmem_limit_bytes=K1_VMEM), name="transform",
        )(feats_t, w_one, send_rows)
        from_prev = lax.ppermute(to_next, GRAPH_AXIS, [(g, (g + 1) % num_dev) for g in range(num_dev)])
        from_next = lax.ppermute(to_prev, GRAPH_AXIS, [(g, (g - 1) % num_dev) for g in range(num_dev)])

        bufs, own_bufs = ([scr(F32, 2 * rows, LANES)] * n for n in (NUM_BUFS, OWN_BUFS))
        fast_row = pltpu.SMEM((8, LANES), I32)
        lists_in = (arr(I32, *listed), arr(I32, *listed), arr(I32, *listed), arr(F32, *listed), arr(I32, 8, LANES))
        part_own, lsrc, ldst, lpair, lw, num = pl.pallas_call(
            k2a_body,
            out_shape=(arr(F32, rows, width),) + lists_in,
            in_specs=[vmem()] * 4, out_specs=(vmem(),) * 6,
            scratch_shapes=[scr(I32, edges // LANES, LANES), scr(F32, 6 * LIST_ROWS, LANES), scr(F32, 2 * rows, LANES),
                            scr(F32, entries, LANES), fast_row, fast_row, fast_row, fast_row, fast_row,
                            pltpu.SemaphoreType.DMA((1,)), dma(2)] + own_bufs,
            compiler_params=pltpu.CompilerParams(vmem_limit_bytes=OWN_VMEM), cost_estimate=busy, name="aggregate_own",
        )(own_t, src2, dst2, ew2)

        hid, pos_a, pos_b, tab = pl.pallas_call(
            k2b_body,
            out_shape=(arr(BF16, rows, width), arr(BF16, EARLY_ROWS, width), arr(BF16, late_rows, width),
                       arr(F32, own_hi * CLASS_ROWS, LANES)),
            in_specs=[vmem(), vmem(), vmem(), hbm(), hbm(), smem(), vmem(), vmem()], out_specs=(vmem(),) * 4,
            scratch_shapes=[scr(F32, 4 * halo, LANES), scr(F32, entries, LANES), fast_list, fast_list, list_dma] + bufs,
            compiler_params=params(), name="aggregate_halo",
        )(part_own, from_prev, from_next, lsrc, ldst, num, lw, w2)

        num_z = num_dev // PLANE
        tab_b = arr(BF16, own_hi * CLASS_ROWS, LANES)
        pos_early = arr(BF16, EARLY_ROWS, width)
        list_i = arr(I32, *listed)
        (d_tab, misc, late, prev_a, next_a, dst_prev, dst_next, put_prev, put_next, w_prev, w_next,
         nums, names) = pl.pallas_call(
            functools.partial(k3_body, num_dev),
            out_shape=(tab_b, arr(F32, 16, width), arr(BF16, late_rows + own_hi * CLASS_ROWS * LANES // width, width), pos_early, pos_early, list_i, list_i, list_i, list_i,
                       arr(F32, *listed), arr(F32, *listed), arr(I32, 8, LANES), arr(I32, 2 * halo // LANES, LANES)),
            in_specs=[vmem()] * 13, out_specs=(vmem(),) * 13,
            scratch_shapes=[scr(I32, 2, *listed), scr(I32, 2, 8, LANES), scr(BF16, all_hi * CLASS_ROWS, LANES),
                            scr(BF16, 2, 16, halo), scr(BF16, 2, 16, halo), scr(F32, 2, CLASS_ROWS, halo),
                            scr(F32, 2, CLASS_ROWS, halo), scr(F32, edges // 1024, CLASS_ROWS, 1024),
                            scr(F32, own_hi * 24, LANES), scr(F32, 2 * halo // LANES * 24, LANES),
                            scr(F32, own_hi * 24, LANES), scr(F32, own_hi * 24, LANES), scr(BF16, 3 * own_hi * CLASS_ROWS, LANES),
                            scr(F32, 2, 8, LANES), scr(F32, PLANE + num_z - 2, 8, LANES),
                            dma(4), dma(PLANE + num_z - 2), dma(6), dma(6)],
            compiler_params=params(1), name="layer_two",
        )(tab, send_rows, src2, dst2, ew2, lab2, mask2, hid, pos_a, pos_b, lpair, lw, num)

        prev_late = lax.ppermute(late, GRAPH_AXIS, [(g, (g + 1) % num_dev) for g in range(num_dev)])
        next_late = lax.ppermute(late, GRAPH_AXIS, [(g, (g - 1) % num_dev) for g in range(num_dev)])
        part_own = pl.pallas_call(
            k4a_body,
            out_shape=arr(F32, rows, width),
            in_specs=[hbm(), hbm(), smem()] + [vmem()] * 5, out_specs=vmem(),
            scratch_shapes=[scr(F32, 2 * rows, LANES), scr(F32, entries, LANES), fast_row, fast_row, fast_row, fast_row,
                            dma(2)] + own_bufs,
            compiler_params=pltpu.CompilerParams(vmem_limit_bytes=OWN_VMEM), cost_estimate=busy, name="scatter_own",
        )(ldst, lsrc, num, lw, pos_a, pos_b, d_tab, w2)

        sum_rows_pad = 512
        part = pl.pallas_call(
            k4b_body,
            out_shape=arr(F32, sum_rows_pad, width),
            in_specs=[vmem(), smem(), vmem()] + [hbm(), hbm(), vmem()] * 2 + [vmem()] * 7, out_specs=vmem(),
            scratch_shapes=[scr(F32, 2 * rows, LANES), scr(F32, entries, LANES), scr(BF16, rows, width),
                            pltpu.SMEM((2 * halo,), I32), pltpu.SemaphoreType.DMA]
            + [fast_list] * 4 + [list_dma] * 2 + bufs,
            compiler_params=params(), name="scatter_peers",
        )(part_own, nums, names.reshape(2 * halo), dst_prev, put_prev, w_prev,
          dst_next, put_next, w_next,
          prev_a, prev_late, next_a, next_late, w2, feats_t, misc)

        n1, n2 = sum_rows_pad // 2, sum_rows_pad // 8
        n3 = n2 // num_z
        full = pl.pallas_call(
            functools.partial(k5_body, num_dev),
            out_shape=arr(F32, sum_rows_pad, width),
            in_specs=[vmem()], out_specs=vmem(),
            scratch_shapes=[scr(F32, n1, width), scr(F32, 3, n2, width), scr(F32, num_z - 1, n3, width),
                            scr(F32, n1, width), scr(F32, n2, width), dma(8 * (1 + 3 + num_z - 1))],
            compiler_params=params(2), name="sum_gradients",
        )(part)
        loss, grad_one, grad_two = pl.pallas_call(
            k6_body,
            out_shape=(arr(F32, 1, 1), arr(F32, feats, width), arr(F32, w2.shape[0], width)),
            in_specs=[vmem()], out_specs=(vmem(),) * 3, compiler_params=params(), name="outputs",
        )(full)
        return loss.reshape(()), grad_one, grad_two.T

    row_spec = P(GRAPH_AXIS)
    return jax.shard_map(device_step, mesh=mesh,
                         in_specs=(row_spec, P(), P(), row_spec, row_spec, row_spec, row_spec, row_spec, row_spec),
                         out_specs=(P(), P(), P()), check_vma=False)
```

```python
import functools

import jax
import jax.numpy as jnp
from jax import lax
from jax.experimental import pallas as pl
from jax.experimental.pallas import tpu as pltpu
from jax.sharding import PartitionSpec as P

GRAPH_AXIS = "graph"
MESH = pl.DeviceIdType.MESH
LANES = 128
CLASS_ROWS = 8
VMEM_BYTES = 28 * 2**20
K1_VMEM = 50 * 2**20
OWN_VMEM = 34 * 2**20
F32 = jnp.float32
BF16 = jnp.bfloat16
NT = (((1,), (1,)), ((), ()))
TN = (((0,), (0,)), ((), ()))


def vmem():
    return pl.BlockSpec(memory_space=pltpu.VMEM)


def hbm():
    return pl.BlockSpec(memory_space=pl.ANY)


def smem():
    return pl.BlockSpec(memory_space=pltpu.SMEM)


PLANE = 8
LIST_ROWS = 80
BLOCK = 128
NUM_BUFS = 4
OWN_BUFS = 5
EARLY_ROWS = 768
STEP_ROWS = 32
CHUNK = 1024


def ring_peers(num_dev):
    me = lax.axis_index(GRAPH_AXIS)
    return me, (me + 1) % num_dev, (me + num_dev - 1) % num_dev


def layer_peers(me, num_dev):
    return [(me + PLANE * k) % num_dev for k in range(1, num_dev // PLANE)]


def class_weights(w_ref):
    w = w_ref[...]
    return jnp.concatenate([w, jnp.zeros((CLASS_ROWS - w.shape[0], w.shape[1]), F32)], axis=0).astype(BF16)


def meet(partners):
    barrier = pltpu.get_barrier_semaphore()
    for dev in partners:
        pl.semaphore_signal(barrier, inc=1, device_id=(dev,), device_id_type=MESH)
    pl.semaphore_wait(barrier, len(partners))


def remote(src, dst, sems, slot, dev):
    return pltpu.make_async_remote_copy(
        src_ref=src, dst_ref=dst, send_sem=sems.at[0, slot], recv_sem=sems.at[1, slot],
        device_id=(dev,), device_id_type=MESH)


def three_pieces(val):
    top = val.astype(BF16).astype(F32)
    rest = val - top
    mid = rest.astype(BF16).astype(F32)
    return top, mid, rest - mid


def wide_row(ref, first):
    blk = ref[pl.ds(first, STEP_ROWS), :]
    return jnp.concatenate([blk[j:j + 1, :] for j in range(STEP_ROWS)], axis=1)


def number(ref, row, lane):
    here = lax.broadcasted_iota(jnp.int32, ref.shape, 0) == row
    here = here & (lax.broadcasted_iota(jnp.int32, ref.shape, 1) == lane)
    return jnp.sum(jnp.where(here, ref[...].astype(F32), 0.0)).astype(jnp.int32)


def packed(row):
    return jnp.broadcast_to(row, (16, row.shape[1])).astype(jnp.int16)


def hot_rows(row, count):
    n = row.shape[1]
    ids = lax.broadcasted_iota(jnp.int32, (count, LANES), 0).astype(jnp.int16)
    return jnp.concatenate([ids] * (n // LANES), axis=1) == jnp.concatenate([packed(row)] * (count // 16), axis=0)


def ones_at(mask):
    return jnp.where(mask, jnp.ones((), BF16), jnp.zeros((), BF16))


def lo_hot(idx):
    return ones_at(hot_rows(idx & (LANES - 1), LANES))


def list_places(src_ref, w_ref, rows, halo, pos, num_ref):
    src, live = src_ref[...], w_ref[...] != 0.0
    n_rows = src.shape[0]
    tri = (lax.broadcasted_iota(jnp.int32, (LANES, LANES), 0) <= lax.broadcasted_iota(jnp.int32, (LANES, LANES), 1))
    tri = tri.astype(F32).astype(BF16)
    low = (lax.broadcasted_iota(jnp.int32, (n_rows, n_rows), 1) < lax.broadcasted_iota(jnp.int32, (n_rows, n_rows), 0))
    low = low.astype(F32).astype(BF16)
    place = jnp.full(src.shape, LIST_ROWS * LANES, jnp.int32)
    start = jnp.zeros((1, 1), jnp.int32)
    lane = lax.broadcasted_iota(jnp.int32, num_ref.shape, 1)
    num = jnp.zeros(num_ref.shape, jnp.int32)
    kinds = (src < rows, (src >= rows) & (src < rows + halo), src >= rows + halo)
    for k, kind in enumerate(kinds):
        kind = kind & live
        flag = kind.astype(F32)
        inner = jnp.dot(flag.astype(BF16), tri, preferred_element_type=F32)
        row_sum = jnp.broadcast_to(jnp.sum(flag, axis=1, keepdims=True), flag.shape)
        before = jnp.dot(low, row_sum.astype(BF16), preferred_element_type=F32)
        rank = (inner + before).astype(jnp.int32) - 1
        place = jnp.where(kind, start + rank, place)
        total = jnp.sum(jnp.sum(flag, axis=1, keepdims=True), axis=0, keepdims=True).astype(jnp.int32)
        blocks = lax.shift_right_logical(total + (BLOCK - 1), BLOCK.bit_length() - 1)
        start = start + blocks * BLOCK
        num = jnp.where(lane == k, blocks, num)
    pos[...] = place
    num_ref[...] = num


def k1_body(xt_hbm, w_hbm, send_hbm, own_t_ref, to_next_ref, to_prev_ref, xt_ref, w_ref, send_ref, hot, sems):
    copies = [pltpu.make_async_copy(a, b, sems.at[k])
              for k, (a, b) in enumerate(((send_hbm, send_ref), (w_hbm, w_ref), (xt_hbm, xt_ref)))]
    for copy in copies:
        copy.start()
    copies[0].wait()
    halo = send_ref.shape[1]
    rows = xt_ref.shape[1]
    blocks = halo // LANES
    ids = jnp.concatenate([send_ref[r:r + 1, b * LANES:(b + 1) * LANES] for r in range(2) for b in range(blocks)], axis=0)
    ids_col = jnp.transpose(ids)
    node = lax.broadcasted_iota(jnp.int32, (LANES, rows), 1).astype(jnp.int16)
    for b in range(2 * blocks):
        col = jnp.broadcast_to(ids_col[:, b:b + 1], (LANES, LANES)).astype(jnp.int16)
        hot[b * LANES:(b + 1) * LANES, :] = ones_at(node == jnp.concatenate([col] * (rows // LANES), axis=1))
    copies[1].wait()
    w_b = w_ref[...].astype(BF16)
    copies[2].wait()
    own_t_ref[...] = lax.dot_general(w_b, xt_ref[...], TN, preferred_element_type=F32).astype(BF16)
    for r, out in ((1, to_next_ref), (0, to_prev_ref)):
        out[...] = lax.dot_general(hot[r * halo:(r + 1) * halo, :], own_t_ref[...], NT, preferred_element_type=F32).astype(BF16)


def sort_edges(src_ref, dst_ref, ew_ref, rows, halo, pos, acc, lsrc_ref, ldst_ref, lpair_ref, lw_ref, num_ref):
    list_places(src_ref, ew_ref, rows, halo, pos, num_ref)
    acc[...] = jnp.zeros_like(acc)

    def sort(i, carry):
        first = pl.multiple_of(i * STEP_ROWS, STEP_ROWS)
        src, dst, wgt, place = (wide_row(ref, first) for ref in (src_ref, dst_ref, ew_ref, pos))
        both = src + dst * 4096
        ints = [both & 255, lax.shift_right_logical(both, 8) & 255, lax.shift_right_logical(both, 16)]
        cargo = [v.astype(F32) for v in ints] + list(three_pieces(wgt))
        here = hot_rows(lax.shift_right_logical(place, 7), LIST_ROWS)
        cargo = [jnp.concatenate([jnp.broadcast_to(v, (16, v.shape[1])).astype(BF16)] * (LIST_ROWS // 16), axis=0) for v in cargo]
        lhs = jnp.concatenate([jnp.where(here, v, jnp.zeros((), BF16)) for v in cargo], axis=0)
        acc[...] += lax.dot_general(lhs, lo_hot(place), NT, preferred_element_type=F32)
        return carry

    lax.fori_loop(0, src_ref.shape[0] // STEP_ROWS, sort, 0)
    got = [acc[p * LIST_ROWS:(p + 1) * LIST_ROWS, :] for p in range(6)]
    ints = [g.astype(jnp.int32) for g in got[:3]]
    both = ints[0] + ints[1] * 256 + ints[2] * 65536
    src, dst = both & 4095, lax.shift_right_logical(both, 12) * 2
    src = jnp.where(src < rows, src, src - rows)
    lsrc_ref[...] = src * 2
    ldst_ref[...] = dst
    lpair_ref[...] = dst + src * 65536
    lw_ref[...] = got[3] + got[4] + got[5]


def spread_weights(w_ref, wide, first, last):
    def body(g, carry):
        cols = jnp.transpose(w_ref[pl.ds(pl.multiple_of(g * 8, 8), 8), :])
        for j in range(8):
            at = pl.ds(pl.multiple_of(g * 8 * LANES + j * LANES, LANES), LANES)
            wide[at, :] = jnp.broadcast_to(cols[:, j:j + 1], (LANES, LANES))
        return carry

    lax.fori_loop(first // 8, (last + 7) // 8, body, 0)


def clear_rows(bufs):
    def body(i, carry):
        for buf in bufs:
            buf[pl.ds(pl.multiple_of(i * 64, 64), 64), :] = jnp.zeros((64, LANES), F32)
        return carry

    lax.fori_loop(0, bufs[0].shape[0] // 64, body, 0)


def chunk_copies(lists, fast, sems, c):
    at = pl.ds(pl.multiple_of(c * 8, 8), CHUNK // LANES)
    return [pltpu.make_async_copy(a.at[at, :], b.at[at, :], sems.at[k, c]) for k, (a, b) in enumerate(zip(lists, fast))]


def chunks_of(first, last):
    per = CHUNK // BLOCK
    return first // per, (last + per - 1) // per


def start_lists(lists, fast, sems, first, last):
    def body(c, carry):
        for copy in chunk_copies(lists, fast, sems, c):
            copy.start()
        return carry

    lax.fori_loop(*chunks_of(first, last), body, 0)


def row_loop(lists, fast, sems, wide, table, bufs, first, last, rename=None):
    num = len(bufs)
    take_ref, put_ref = fast
    per = CHUNK // BLOCK

    def step(i, carry):
        base = i * BLOCK
        for lead in range(0, BLOCK, num):
            take = [pl.multiple_of(take_ref[i, lead + j], 2) for j in range(num)]
            put = [put_ref[i, lead + j] for j in range(num)]
            if rename is not None:
                put = [rename[p] for p in put]
            put = [pl.multiple_of(p, 2) for p in put]
            vals = [wide[pl.ds(base + lead + j, 1), :] * table[pl.ds(take[j], 2), :] for j in range(num)]
            old = [bufs[j][pl.ds(put[j], 2), :] for j in range(num)]
            for j in range(num):
                bufs[j][pl.ds(put[j], 2), :] = old[j] + vals[j]
        return carry

    def chunk(c, carry):
        for copy in chunk_copies(lists, fast, sems, c):
            copy.wait()
        return lax.fori_loop(jnp.maximum(first, c * per), jnp.minimum(last, c * per + per), step, carry)

    lax.fori_loop(*chunks_of(first, last), chunk, 0)


def slot_copies(lists, slots, sems, c):
    at = pl.ds(pl.multiple_of(c * 8, 8), 8)
    return lambda slot: [pltpu.make_async_copy(a.at[at, :], b, sems.at[slot, k]) for k, (a, b) in enumerate(zip(lists, slots[slot]))]


def start_slots(lists, slots, sems):
    for slot in range(2):
        for copy in slot_copies(lists, slots, sems, slot)(slot):
            copy.start()


def slot_loop(lists, slots, sems, wide, table, bufs, last):
    num = len(bufs)
    pairs = jnp.maximum((last + 15) // 16, 1)

    def group(k, carry):
        for slot in range(2):
            take_ref, put_ref = slots[slot]
            for copy in slot_copies(lists, slots, sems, 2 * k + slot)(slot):
                copy.wait()
            for r in range(8):
                row = 16 * k + 8 * slot + r

                @pl.when(row < last)
                def _():
                    base = pl.multiple_of(row * LANES, LANES)
                    for lead in range(0, LANES, num):
                        here = range(min(num, LANES - lead))
                        take = [pl.multiple_of(take_ref[r, lead + j], 2) for j in here]
                        put = [pl.multiple_of(put_ref[r, lead + j], 2) for j in here]
                        vals = [wide[pl.ds(base + lead + j, 1), :] * table[pl.ds(take[j], 2), :] for j in here]
                        old = [bufs[j][pl.ds(put[j], 2), :] for j in here]
                        for j in here:
                            bufs[j][pl.ds(put[j], 2), :] = old[j] + vals[j]

            @pl.when(k + 1 < pairs)
            def _():
                for copy in slot_copies(lists, slots, sems, 2 * k + 2 + slot)(slot):
                    copy.start()
        return carry

    lax.fori_loop(0, pairs, group, 0)


def list_rows(first, last):
    return first * BLOCK // LANES, (last * BLOCK + LANES - 1) // LANES


def to_rows(blk, table, first_row):
    for h in range(2):
        table[pl.ds(2 * first_row + h, blk.shape[0], stride=2), :] = blk[:, h * LANES:(h + 1) * LANES]


def sum_rows(bufs, blk):
    halves = []
    for h in range(2):
        parts = [buf[pl.ds(2 * blk * LANES + h, LANES, stride=2), :] for buf in bufs]
        while len(parts) > 1:
            parts = [a + b for a, b in zip(parts[::2], parts[1::2])] + parts[len(parts) // 2 * 2:]
        halves.append(parts[0])
    return jnp.concatenate(halves, axis=1)


def k2a_body(own_t_ref, src_ref, dst_ref, ew_ref, part_ref, lsrc_ref, ldst_ref, lpair_ref, lw_ref, num_ref,
             pos, acc, table, wide, src_a, dst_a, src_b, dst_b, slot_sems, *bufs):
    rows = part_ref.shape[0]
    sort_edges(src_ref, dst_ref, ew_ref, rows, rows // 2, pos, acc, lsrc_ref, ldst_ref, lpair_ref, lw_ref, num_ref)

    def widen(i, carry):
        at = pl.ds(pl.multiple_of(i * LANES, LANES), LANES)
        to_rows(jnp.transpose(own_t_ref[:, at].astype(F32)), table, i * LANES)
        return carry

    lax.fori_loop(0, rows // LANES, widen, 0)
    lists, slots = (lsrc_ref, ldst_ref), ((src_a, dst_a), (src_b, dst_b))
    start_slots(lists, slots, slot_sems)
    clear_rows(bufs)
    end = number(num_ref, 0, 0)
    spread_weights(lw_ref, wide, *list_rows(0, end))
    slot_loop(lists, slots, slot_sems, wide, table, bufs, end)

    def finish(i, carry):
        part_ref[pl.ds(pl.multiple_of(i * LANES, LANES), LANES), :] = sum_rows(bufs, i)
        return carry

    lax.fori_loop(0, rows // LANES, finish, 0)


def k2b_body(part_ref, prev_ref, next_ref, lsrc_ref, ldst_ref, num_ref, lw_ref, w2_ref,
             hid_ref, pos_a_ref, pos_b_ref, tab_ref, table, wide, src_fast, dst_fast, sems, *bufs):
    first = number(num_ref, 0, 0)
    end = first + number(num_ref, 0, 1) + number(num_ref, 0, 2)
    lists, fast = (lsrc_ref, ldst_ref), (src_fast, dst_fast)
    start_lists(lists, fast, sems, first, end)
    spread_weights(lw_ref, wide, *list_rows(first, end))
    halo = prev_ref.shape[0]

    def widen(i, carry):
        at = pl.ds(pl.multiple_of(i * LANES, LANES), LANES)
        to_rows(prev_ref[at, :].astype(F32), table, i * LANES)
        to_rows(next_ref[at, :].astype(F32), table, halo + i * LANES)
        return carry

    lax.fori_loop(0, halo // LANES, widen, 0)
    clear_rows(bufs)
    row_loop(lists, fast, sems, wide, table, bufs, first, end)
    w2t = class_weights(w2_ref)

    for pos_ref, lead in ((pos_a_ref, 0), (pos_b_ref, pos_a_ref.shape[0] // LANES)):
        def finish(j, carry):
            i = lead + j
            at = pl.ds(pl.multiple_of(i * LANES, LANES), LANES)
            pre = part_ref[at, :] + sum_rows(bufs, i)
            hid = jnp.maximum(pre, 0.0).astype(BF16)
            hid_ref[at, :] = hid
            pos_ref[pl.ds(pl.multiple_of(j * LANES, LANES), LANES), :] = (pre > 0.0).astype(F32).astype(BF16)
            t2 = lax.dot_general(w2t, hid, NT, preferred_element_type=F32)
            tab_ref[pl.ds(pl.multiple_of(i * CLASS_ROWS, CLASS_ROWS), CLASS_ROWS), :] = t2.astype(BF16).astype(F32)
            return carry

        lax.fori_loop(0, pos_ref.shape[0] // LANES, finish, 0)


def stack_classes(w2_ref, blocks):
    w2_all = jnp.concatenate([class_weights(w2_ref).astype(F32)] * blocks, axis=0)
    return w2_all, lax.shift_right_logical(lax.broadcasted_iota(jnp.int32, w2_all.shape, 0), 3)


def fill_table(dt, pos_refs, w2_all, group, table):
    dt_cols = jnp.transpose(dt).astype(BF16)
    for pos_ref, lead in zip(pos_refs, (0, pos_refs[0].shape[0] // LANES)):
        def widen(j, carry):
            i = lead + j
            d_hid = jnp.dot(dt_cols, jnp.where(group == i, w2_all, 0.0).astype(BF16), preferred_element_type=F32)
            at = pl.ds(pl.multiple_of(j * LANES, LANES), LANES)
            to_rows(jnp.where(pos_ref[at, :].astype(F32) > 0.0, d_hid, 0.0), table, i * LANES)
            return carry

        lax.fori_loop(0, pos_ref.shape[0] // LANES, widen, 0)


def k4a_body(ldst_ref, lsrc_ref, num_ref, lw_ref, pos_a_ref, pos_b_ref, dt_ref, w2_ref, part_ref,
             table, wide, take_a, put_a, take_b, put_b, slot_sems, *bufs):
    rows = part_ref.shape[0]
    lists, slots, end = (ldst_ref, lsrc_ref), ((take_a, put_a), (take_b, put_b)), number(num_ref, 0, 0)
    start_slots(lists, slots, slot_sems)
    w2_all, group = stack_classes(w2_ref, rows // LANES)
    clear_rows(bufs)
    fill_table(dt_ref[...].astype(F32), (pos_a_ref, pos_b_ref), w2_all, group, table)
    spread_weights(lw_ref, wide, *list_rows(0, end))
    slot_loop(lists, slots, slot_sems, wide, table, bufs, end)

    def finish(i, carry):
        part_ref[pl.ds(pl.multiple_of(i * LANES, LANES), LANES), :] = sum_rows(bufs, i)
        return carry

    lax.fori_loop(0, rows // LANES, finish, 0)


def k4b_body(part_ref, num_ref, names_ref, prev_dst, prev_src, prev_w, next_dst, next_src, next_w,
             prev_a, prev_late, next_a, next_late, w2_ref, xt_ref, misc_ref, out_ref,
             table, wide, d_tab, names, names_sem, *rest):
    fasts, pools, bufs = (rest[0:2], rest[2:4]), rest[4:6], rest[6:]
    rows = part_ref.shape[0]
    late_rows = rows - prev_a.shape[0]
    load = pltpu.make_async_copy(names_ref, names, names_sem)
    load.start()
    sides = (((prev_dst, prev_src), prev_w, prev_late, prev_a, 1, 2),
             ((next_dst, next_src), next_w, next_late, next_a, 2, 1))
    spans = []
    for (lists, _, _, _, row, kind), fast, pool in zip(sides, fasts, pools):
        first = number(num_ref, row, 0)
        if kind == 2:
            first = first + number(num_ref, row, 1)
        spans.append((first, first + number(num_ref, row, kind)))
        start_lists(lists, fast, pool, *spans[-1])
    w2_all, group = stack_classes(w2_ref, rows // LANES)
    clear_rows(bufs)
    for (lists, w_ref, late, early, _, _), fast, pool, span in zip(sides, fasts, pools, spans):
        dt = late[late_rows:, :].astype(F32)
        dt = jnp.concatenate([dt[:, 0:LANES], dt[:, LANES:]], axis=0)
        fill_table(dt, (early, late.at[0:late_rows, :]), w2_all, group, table)
        spread_weights(w_ref, wide, *list_rows(*span))
        if late is prev_late:
            load.wait()
        row_loop(lists, fast, pool, wide, table, bufs, *span, rename=names)

    def finish(i, carry):
        at = pl.ds(pl.multiple_of(i * LANES, LANES), LANES)
        d_tab[at, :] = (part_ref[at, :] + sum_rows(bufs, i)).astype(BF16)
        return carry

    lax.fori_loop(0, rows // LANES, finish, 0)
    feats = xt_ref.shape[0]
    out_ref[0:feats, :] = jnp.dot(xt_ref[...], d_tab[...], preferred_element_type=F32)
    out_ref[feats:feats + 12, :] = misc_ref[0:12, :]


def hi_of(idx):
    return jnp.broadcast_to(lax.shift_right_logical(idx, 7), (CLASS_ROWS, idx.shape[1]))


def pick_cols(table_b, pieces, idx, hot, first=0):
    cols = jnp.dot(table_b, hot, preferred_element_type=F32)
    rows = table_b.shape[0] // pieces
    hi = hi_of(idx) - first
    out = jnp.zeros(hi.shape, F32)
    for h in range(rows // CLASS_ROWS):
        part = cols[h * CLASS_ROWS:(h + 1) * CLASS_ROWS]
        for p in range(1, pieces):
            part = part + cols[p * rows + h * CLASS_ROWS:p * rows + (h + 1) * CLASS_ROWS]
        out = out + jnp.where(hi == h, part, 0.0)
    return out


def add_cols(val, idx, hot, num_hi, first=0):
    hi = packed(lax.shift_right_logical(idx, 7) - first)
    low_half = lax.broadcasted_iota(jnp.int32, hi.shape, 0) >= CLASS_ROWS
    mixed = hi - low_half.astype(jnp.int32).astype(jnp.int16)
    top, mid, low = three_pieces(val)
    pieces = [jnp.concatenate(two, axis=0).astype(BF16) for two in ((top, mid), (low, top), (mid, low))]
    rows = []
    for h in range(0, num_hi, 2):
        masks = (hi == jnp.int16(h), mixed == jnp.int16(h), hi == jnp.int16(h + 1))
        rows += [jnp.where(m, p, jnp.zeros((), BF16)) for m, p in zip(masks, pieces)]
    return lax.dot_general(jnp.concatenate(rows, axis=0), hot, NT, preferred_element_type=F32)


def join_pieces(acc, num_hi):
    out = []
    for h in range(num_hi):
        a = acc[h * 24:h * 24 + 24, :]
        out.append(a[0:8] + a[8:16] + a[16:24])
    return out


def stack_pieces(val):
    return jnp.concatenate(three_pieces(val), axis=0).astype(BF16)


def k3_body(num_dev, tab_ref, send_ref, src_ref, dst_ref, w_ref, lab_ref, mask_ref, hid_ref, pos_ref, pos_late_ref,
            lpair_ref, lw_ref, num_ref,
            dt_ref, misc_ref, late_ref, pos_prev_ref, pos_next_ref, dst_prev_ref, dst_next_ref,
            put_prev_ref, put_next_ref, w_prev_ref, w_next_ref, nums_ref, names_ref, pairs, nums,
            ext_b, fwd_send, fwd_recv, bwd_send, bwd_recv, vals, acc_z, acc_s, acc_o, acc_r, dz_b, cnt_send, cnt_recv,
            sems, cnt_sems, list_sems, pos_sems):
    me, nxt, prv = ring_peers(num_dev)
    layers = layer_peers(me, num_dev)
    layer = [me - me % PLANE + (me % PLANE + k) % PLANE for k in range(1, PLANE)]
    meet([nxt, prv] + layer + layers)
    total = jnp.sum(jnp.sum(mask_ref[...].astype(F32), axis=1, keepdims=True), axis=0, keepdims=True)
    cnt_send[0] = jnp.broadcast_to(total, cnt_send.shape[1:])
    counts = [remote(cnt_send.at[0], cnt_recv.at[k], cnt_sems, k, dev) for k, dev in enumerate(layer)]
    for copy in counts:
        copy.start()
    late = []

    def send_late(pairs, pool, first):
        for k, (src, dst) in enumerate(pairs):
            for s, dev in enumerate((nxt, prv)):
                copy = remote(src, dst[s], pool, 2 * (first + k) + s, dev)
                copy.start()
                late.append(copy)

    chunk = pos_ref.shape[0] // 3

    def send_pos(q):
        at = pl.ds(q * chunk, chunk)
        send_late([(pos_ref.at[at, :], [pos_prev_ref.at[at, :], pos_next_ref.at[at, :]])], pos_sems, q)

    own_hi = tab_ref.shape[0] // CLASS_ROWS
    halo = send_ref.shape[1]
    halo_hi = halo // LANES
    all_hi = own_hi + 2 * halo_hi
    own_b = tab_ref[...].astype(BF16)
    ext_b[pl.ds(0, own_hi * CLASS_ROWS), :] = own_b
    hot_send = [lo_hot(send_ref[r:r + 1, :]) for r in range(2)]
    copies = []
    for r in (1, 0):
        val = pick_cols(own_b, 1, send_ref[r:r + 1, :], hot_send[r])
        fwd_send[r] = jnp.concatenate([val, jnp.zeros_like(val)], axis=0).astype(BF16)
        copy = remote(fwd_send.at[r], fwd_recv.at[1 - r], sems, r, nxt if r == 1 else prv)
        copy.start()
        copies.append(copy)
    send_late([(lpair_ref, [pairs.at[0], pairs.at[1]]), (lw_ref, [w_prev_ref, w_next_ref]),
               (num_ref, [nums.at[0], nums.at[1]])], list_sems, 0)
    send_pos(0)
    for copy in counts:
        copy.wait()
    for k in range(len(layer)):
        total = total + cnt_recv[k][0:1, 0:1]
    cnt_send[1] = jnp.broadcast_to(total, cnt_send.shape[1:])
    counts = [remote(cnt_send.at[1], cnt_recv.at[len(layer) + k], cnt_sems, len(layer) + k, dev)
              for k, dev in enumerate(layers)]
    for copy in counts:
        copy.start()
    send_pos(1)
    send_pos(2)
    acc_z[...] = jnp.zeros_like(acc_z)
    acc_s[...] = jnp.zeros_like(acc_s)
    acc_o[...] = jnp.zeros_like(acc_o)
    late_rows = pos_late_ref.shape[0]
    late_ref[0:late_rows, :] = pos_late_ref[...]
    steps = src_ref.shape[0] // STEP_ROWS

    def own_forward(i, carry):
        src = wide_row(src_ref, pl.multiple_of(i * STEP_ROWS, STEP_ROWS))
        vals[i] = pick_cols(ext_b[0:own_hi * CLASS_ROWS, :], 1, src, lo_hot(src))
        return carry

    lax.fori_loop(0, steps, own_forward, 0)
    for copy in copies:
        copy.wait()
    for r in range(2):
        got = fwd_recv[r].astype(F32)
        for j in range(0, halo_hi, 2):
            two = jnp.concatenate([got[0:8, (j + k) * LANES:(j + k + 1) * LANES] for k in range(2)], axis=0)
            ext_b[pl.ds((own_hi + r * halo_hi + j) * CLASS_ROWS, 16), :] = two.astype(BF16)


    def forward(i, carry):
        first = pl.multiple_of(i * STEP_ROWS, STEP_ROWS)
        src, dst = wide_row(src_ref, first), wide_row(dst_ref, first)
        val = vals[i] + pick_cols(ext_b[own_hi * CLASS_ROWS:, :], 1, src, lo_hot(src), own_hi)
        val = val * wide_row(w_ref, first)
        acc_z[...] += add_cols(val, dst, lo_hot(dst), own_hi)
        return carry

    lax.fori_loop(0, steps, forward, 0)

    logits = join_pieces(acc_z[...], own_hi)
    cls = lax.broadcasted_iota(jnp.int32, (CLASS_ROWS, LANES), 0)
    count = jnp.broadcast_to(total, (1, LANES))
    for k, copy in enumerate(counts):
        copy.wait()
        count = count + cnt_recv[len(layer) + k][0:1, :]
    count = jnp.maximum(count, 1.0)
    loss = jnp.zeros((1, LANES), F32)
    d_log = []
    for h in range(own_hi):
        z = jnp.where(cls < 7, logits[h], -jnp.inf)
        top = jnp.max(z, axis=0, keepdims=True)
        norm = jnp.log(jnp.sum(jnp.exp(z - top), axis=0, keepdims=True)) + top
        hot = cls == lab_ref[h:h + 1, :]
        mask = mask_ref[h:h + 1, :].astype(F32)
        picked = jnp.sum(jnp.where(hot, logits[h], 0.0), axis=0, keepdims=True)
        loss = loss + mask * (norm - picked)
        d_log.append((jnp.exp(z - norm) - hot.astype(F32)) * (mask / count))
    dz_b[...] = stack_pieces(jnp.concatenate(d_log, axis=0))

    def backward(i, carry):
        first = pl.multiple_of(i * STEP_ROWS, STEP_ROWS)
        src, dst = wide_row(src_ref, first), wide_row(dst_ref, first)
        val = pick_cols(dz_b[...], 3, dst, lo_hot(dst)) * wide_row(w_ref, first)
        vals[i] = val
        acc_s[...] += add_cols(val, src, lo_hot(src), 2 * halo_hi, own_hi)
        return carry

    lax.fori_loop(0, steps, backward, 0)

    d_halo = join_pieces(acc_s[...], 2 * halo_hi)
    copies = []
    for r in range(2):
        for j in range(halo_hi):
            bwd_send[r, :, j * LANES:(j + 1) * LANES] = d_halo[r * halo_hi + j]
        copy = remote(bwd_send.at[r], bwd_recv.at[1 - r], sems, 2 + r, prv if r == 0 else nxt)
        copy.start()
        copies.append(copy)

    def own_backward(i, carry):
        src = wide_row(src_ref, pl.multiple_of(i * STEP_ROWS, STEP_ROWS))
        acc_o[...] += add_cols(vals[i], src, lo_hot(src), own_hi)
        return carry

    lax.fori_loop(0, steps, own_backward, 0)
    d_own = join_pieces(acc_o[...], own_hi)
    for copy in copies:
        copy.wait()
    for r in range(2):
        part = add_cols(bwd_recv[r], send_ref[r:r + 1, :], hot_send[r], own_hi)
        acc_r[...] = part if r == 0 else acc_r[...] + part
    back = join_pieces(acc_r[...], own_hi)
    d_tab = [d_own[h] + back[h] for h in range(own_hi)]
    half = own_hi // 2
    dt_ref[...] = jnp.concatenate(d_tab, axis=0).astype(BF16)
    late_ref[late_rows:, :] = jnp.concatenate(
        [jnp.concatenate(d_tab[:half], axis=0), jnp.concatenate(d_tab[half:], axis=0)], axis=1).astype(BF16)
    grad = jnp.zeros((CLASS_ROWS, hid_ref.shape[1]), F32)
    for h in range(own_hi):
        grad = grad + jnp.dot(d_tab[h].astype(BF16), hid_ref[pl.ds(h * LANES, LANES), :], preferred_element_type=F32)
    misc_ref[0:8, :] = grad
    total = jnp.sum(loss, axis=1, keepdims=True) / count[:, 0:1]
    misc_ref[8:16, :] = jnp.broadcast_to(total, (8, misc_ref.shape[1]))
    for copy in late:
        copy.wait()
    for s, (to_dst, to_put) in enumerate(((dst_prev_ref, put_prev_ref), (dst_next_ref, put_next_ref))):
        to_dst[...] = pairs[s] & 0xFFFF
        to_put[...] = lax.shift_right_logical(pairs[s], 16)
    row = lax.broadcasted_iota(jnp.int32, nums_ref.shape, 0)
    nums_ref[...] = jnp.where(row == 0, num_ref[0:1, :], jnp.where(row == 1, nums[0, 0:1, :], nums[1, 0:1, :]))
    names_ref[...] = 2 * jnp.concatenate(
        [send_ref[r:r + 1, j * LANES:(j + 1) * LANES] for r in (1, 0) for j in range(halo_hi)], axis=0)


def k5_body(num_dev, part_ref, full_ref, land_core, land_chip, land_z, by_core, by_chip, sems):
    me = lax.axis_index(GRAPH_AXIS)
    core, chip, z = me % 2, (me // 2) % 4, me // PLANE
    other = me + 1 - 2 * core
    chips = [me + 2 * ((chip + k) % 4 - chip) for k in range(1, 4)]
    layers = layer_peers(me, num_dev)
    num_z = num_dev // PLANE
    meet([other] + chips + layers)
    rows, width = part_ref.shape
    rows //= 2
    n1, n2, n3 = rows // 2, rows // 8, rows // 8 // num_z
    parts = [(p, pl.ds(c * LANES, LANES)) for p in range(2) for c in range(width // LANES)]
    used = [0]

    def send(pairs):
        out = []
        for src, dst, dev in pairs:
            out.append(remote(src, dst, sems, used[0], dev))
            used[0] += 1
        for copy in out:
            copy.start()
        return out

    def wait(copies):
        for copy in copies:
            copy.wait()

    def at(first, size):
        return pl.ds(pl.multiple_of(first, size), size)

    def run(p, size):
        return pl.ds(p * size, size)

    flying = [send([(part_ref.at[at(p * rows + (1 - core) * n1, n1), c], land_core.at[run(p, n1), c], other)]) for p, c in parts]
    for i, (p, c) in enumerate(parts):
        wait(flying[i])
        by_core[run(p, n1), c] = part_ref[at(p * rows + core * n1, n1), c] + land_core[run(p, n1), c]
        flying[i] = send([(by_core.at[at(p * n1 + (chip + k + 1) % 4 * n2, n2), c], land_chip.at[k, run(p, n2), c], dev)
                          for k, dev in enumerate(chips)])
    for i, (p, c) in enumerate(parts):
        wait(flying[i])
        total = by_core[at(p * n1 + chip * n2, n2), c]
        for k in range(len(chips)):
            total = total + land_chip[k, run(p, n2), c]
        by_chip[run(p, n2), c] = total
        flying[i] = send([(by_chip.at[at(p * n2 + (z + k + 1) % num_z * n3, n3), c], land_z.at[k, run(p, n3), c], dev)
                          for k, dev in enumerate(layers)])
    firsts = (core * n1 + chip * n2 + z * n3, core * n1 + chip * n2, core * n1)
    gathers = list(zip(firsts, (n3, n2, n1), (layers, chips, [other])))

    def gather(level, p, c):
        first, size, devs = gathers[level]
        own = full_ref.at[at(p * rows + first, size), c]
        return send([(own, own, dev) for dev in devs])

    for i, (p, c) in enumerate(parts):
        wait(flying[i])
        total = by_chip[at(p * n2 + z * n3, n3), c]
        for k in range(len(layers)):
            total = total + land_z[k, run(p, n3), c]
        full_ref[at(p * rows + firsts[0], n3), c] = total
        flying[i] = gather(0, p, c)
    for level in (1, 2):
        for i, (p, c) in enumerate(parts):
            wait(flying[i])
            flying[i] = gather(level, p, c)
    for copies in flying:
        wait(copies)


def k6_body(full_ref, loss_ref, one_ref, two_ref):
    feats, classes = one_ref.shape[0], two_ref.shape[0]
    one_ref[...] = full_ref[0:feats, :]
    two_ref[...] = full_ref[feats:feats + classes, :]
    loss_ref[...] = full_ref[feats + 8:feats + 9, 0:1]


def solution(mesh):
    num_dev = mesh.shape[GRAPH_AXIS]

    def params(cid=None):
        if cid is None:
            return pltpu.CompilerParams(vmem_limit_bytes=VMEM_BYTES)
        return pltpu.CompilerParams(vmem_limit_bytes=VMEM_BYTES, collective_id=cid, has_side_effects=True)

    def arr(dtype, *shape):
        return jax.ShapeDtypeStruct(shape, dtype)

    def scr(dtype, *shape):
        return pltpu.VMEM(shape, dtype)

    def dma(count):
        return pltpu.SemaphoreType.DMA((2, count))

    I32 = jnp.int32

    def device_step(node_feats, w_one, w_two, send_rows, edge_src, edge_dst, edge_w, labels, label_mask):
        rows, feats = node_feats.shape
        width = w_one.shape[1]
        halo = send_rows.shape[1]
        edges = edge_src.shape[0]
        own_hi, all_hi = rows // LANES, (rows + 2 * halo) // LANES
        feats_t, w2 = node_feats.T, w_two.T
        src2, dst2, ew2 = (a.reshape(edges // LANES, LANES) for a in (edge_src, edge_dst, edge_w))
        lab2, mask2 = labels.reshape(own_hi, LANES), label_mask.reshape(own_hi, LANES)
        listed = (LIST_ROWS, LANES)
        entries = LIST_ROWS * LANES
        fast_list = pltpu.SMEM(listed, I32)
        list_dma = dma(entries // CHUNK)

        late_rows = rows - EARLY_ROWS
        busy = pl.CostEstimate(flops=8 * 10**9, bytes_accessed=10**7, transcendentals=0)
        own_t, to_next, to_prev = pl.pallas_call(
            k1_body,
            out_shape=(arr(BF16, width, rows), arr(BF16, halo, width), arr(BF16, halo, width)),
            in_specs=[pl.BlockSpec(memory_space=pltpu.HBM)] * 3, out_specs=(vmem(),) * 3,
            scratch_shapes=[scr(BF16, feats, rows), scr(F32, feats, width), pltpu.VMEM((2, halo), I32),
                            scr(BF16, 2 * halo, rows), pltpu.SemaphoreType.DMA((3,))],
            compiler_params=pltpu.CompilerParams(vmem_limit_bytes=K1_VMEM), name="transform",
        )(feats_t, w_one, send_rows)
        from_prev = lax.ppermute(to_next, GRAPH_AXIS, [(g, (g + 1) % num_dev) for g in range(num_dev)])
        from_next = lax.ppermute(to_prev, GRAPH_AXIS, [(g, (g - 1) % num_dev) for g in range(num_dev)])

        bufs, own_bufs = ([scr(F32, 2 * rows, LANES)] * n for n in (NUM_BUFS, OWN_BUFS))
        fast_row = pltpu.SMEM((8, LANES), I32)
        lists_in = (arr(I32, *listed), arr(I32, *listed), arr(I32, *listed), arr(F32, *listed), arr(I32, 8, LANES))
        part_own, lsrc, ldst, lpair, lw, num = pl.pallas_call(
            k2a_body,
            out_shape=(arr(F32, rows, width),) + lists_in,
            in_specs=[vmem()] * 4, out_specs=(vmem(),) * 6,
            scratch_shapes=[scr(I32, edges // LANES, LANES), scr(F32, 6 * LIST_ROWS, LANES), scr(F32, 2 * rows, LANES),
                            scr(F32, entries, LANES), fast_row, fast_row, fast_row, fast_row,
                            dma(2)] + own_bufs,
            compiler_params=pltpu.CompilerParams(vmem_limit_bytes=OWN_VMEM), cost_estimate=busy, name="aggregate_own",
        )(own_t, src2, dst2, ew2)

        hid, pos_a, pos_b, tab = pl.pallas_call(
            k2b_body,
            out_shape=(arr(BF16, rows, width), arr(BF16, EARLY_ROWS, width), arr(BF16, late_rows, width),
                       arr(F32, own_hi * CLASS_ROWS, LANES)),
            in_specs=[vmem(), vmem(), vmem(), hbm(), hbm(), vmem(), vmem(), vmem()], out_specs=(vmem(),) * 4,
            scratch_shapes=[scr(F32, 4 * halo, LANES), scr(F32, entries, LANES), fast_list, fast_list, list_dma] + bufs,
            compiler_params=params(), name="aggregate_halo",
        )(part_own, from_prev, from_next, lsrc, ldst, num, lw, w2)

        num_z = num_dev // PLANE
        tab_b = arr(BF16, own_hi * CLASS_ROWS, LANES)
        pos_early = arr(BF16, EARLY_ROWS, width)
        list_i = arr(I32, *listed)
        (d_tab, misc, late, prev_a, next_a, dst_prev, dst_next, put_prev, put_next, w_prev, w_next,
         nums, names) = pl.pallas_call(
            functools.partial(k3_body, num_dev),
            out_shape=(tab_b, arr(F32, 16, width), arr(BF16, late_rows + own_hi * CLASS_ROWS * LANES // width, width), pos_early, pos_early, list_i, list_i, list_i, list_i,
                       arr(F32, *listed), arr(F32, *listed), arr(I32, 8, LANES), arr(I32, 2 * halo // LANES, LANES)),
            in_specs=[vmem()] * 13, out_specs=(vmem(),) * 13,
            scratch_shapes=[scr(I32, 2, *listed), scr(I32, 2, 8, LANES), scr(BF16, all_hi * CLASS_ROWS, LANES),
                            scr(BF16, 2, 16, halo), scr(BF16, 2, 16, halo), scr(F32, 2, CLASS_ROWS, halo),
                            scr(F32, 2, CLASS_ROWS, halo), scr(F32, edges // (STEP_ROWS * LANES), CLASS_ROWS, STEP_ROWS * LANES),
                            scr(F32, own_hi * 24, LANES), scr(F32, 2 * halo // LANES * 24, LANES),
                            scr(F32, own_hi * 24, LANES), scr(F32, own_hi * 24, LANES), scr(BF16, 3 * own_hi * CLASS_ROWS, LANES),
                            scr(F32, 2, 8, LANES), scr(F32, PLANE + num_z - 2, 8, LANES),
                            dma(4), dma(PLANE + num_z - 2), dma(6), dma(6)],
            compiler_params=params(1), name="layer_two",
        )(tab, send_rows, src2, dst2, ew2, lab2, mask2, hid, pos_a, pos_b, lpair, lw, num)

        prev_late = lax.ppermute(late, GRAPH_AXIS, [(g, (g + 1) % num_dev) for g in range(num_dev)])
        next_late = lax.ppermute(late, GRAPH_AXIS, [(g, (g - 1) % num_dev) for g in range(num_dev)])
        part_own = pl.pallas_call(
            k4a_body,
            out_shape=arr(F32, rows, width),
            in_specs=[hbm(), hbm()] + [vmem()] * 6, out_specs=vmem(),
            scratch_shapes=[scr(F32, 2 * rows, LANES), scr(F32, entries, LANES), fast_row, fast_row, fast_row, fast_row,
                            dma(2)] + own_bufs,
            compiler_params=pltpu.CompilerParams(vmem_limit_bytes=OWN_VMEM), cost_estimate=busy, name="scatter_own",
        )(ldst, lsrc, num, lw, pos_a, pos_b, d_tab, w2)

        sum_rows_pad = 512
        part = pl.pallas_call(
            k4b_body,
            out_shape=arr(F32, sum_rows_pad, width),
            in_specs=[vmem(), vmem(), vmem()] + [hbm(), hbm(), vmem()] * 2 + [vmem()] * 7, out_specs=vmem(),
            scratch_shapes=[scr(F32, 2 * rows, LANES), scr(F32, entries, LANES), scr(BF16, rows, width),
                            pltpu.SMEM((2 * halo,), I32), pltpu.SemaphoreType.DMA]
            + [fast_list] * 4 + [list_dma] * 2 + bufs,
            compiler_params=params(), name="scatter_peers",
        )(part_own, nums, names.reshape(2 * halo), dst_prev, put_prev, w_prev,
          dst_next, put_next, w_next,
          prev_a, prev_late, next_a, next_late, w2, feats_t, misc)

        n1, n2 = sum_rows_pad // 2, sum_rows_pad // 8
        n3 = n2 // num_z
        full = pl.pallas_call(
            functools.partial(k5_body, num_dev),
            out_shape=arr(F32, sum_rows_pad, width),
            in_specs=[vmem()], out_specs=vmem(),
            scratch_shapes=[scr(F32, n1, width), scr(F32, 3, n2, width), scr(F32, num_z - 1, n3, width),
                            scr(F32, n1, width), scr(F32, n2, width), dma(8 * (1 + 3 + num_z - 1))],
            compiler_params=params(2), name="sum_gradients",
        )(part)
        loss, grad_one, grad_two = pl.pallas_call(
            k6_body,
            out_shape=(arr(F32, 1, 1), arr(F32, feats, width), arr(F32, w2.shape[0], width)),
            in_specs=[vmem()], out_specs=(vmem(),) * 3, compiler_params=params(), name="outputs",
        )(full)
        return loss.reshape(()), grad_one, grad_two.T

    row_spec = P(GRAPH_AXIS)
    return jax.shard_map(device_step, mesh=mesh,
                         in_specs=(row_spec, P(), P(), row_spec, row_spec, row_spec, row_spec, row_spec, row_spec),
                         out_specs=(P(), P(), P()), check_vma=False)
```

```python
import functools

import jax
import jax.numpy as jnp
from jax import lax
from jax.experimental import pallas as pl
from jax.experimental.pallas import tpu as pltpu
from jax.sharding import PartitionSpec as P

GRAPH_AXIS = "graph"
MESH = pl.DeviceIdType.MESH
LANES = 128
CLASS_ROWS = 8
VMEM_BYTES = 28 * 2**20
K1_VMEM = 50 * 2**20
OWN_VMEM = 34 * 2**20
F32 = jnp.float32
BF16 = jnp.bfloat16
NT = (((1,), (1,)), ((), ()))
TN = (((0,), (0,)), ((), ()))


def vmem():
    return pl.BlockSpec(memory_space=pltpu.VMEM)


def hbm():
    return pl.BlockSpec(memory_space=pl.ANY)


def smem():
    return pl.BlockSpec(memory_space=pltpu.SMEM)


PLANE = 8
LIST_ROWS = 80
BLOCK = 128
NUM_BUFS = 4
OWN_BUFS = 5
EARLY_ROWS = 768
STEP_ROWS = 32
CHUNK = 1024


def ring_peers(num_dev):
    me = lax.axis_index(GRAPH_AXIS)
    return me, (me + 1) % num_dev, (me + num_dev - 1) % num_dev


def layer_peers(me, num_dev):
    return [(me + PLANE * k) % num_dev for k in range(1, num_dev // PLANE)]


def class_weights(w_ref):
    w = w_ref[...]
    return jnp.concatenate([w, jnp.zeros((CLASS_ROWS - w.shape[0], w.shape[1]), F32)], axis=0).astype(BF16)


def meet(partners):
    barrier = pltpu.get_barrier_semaphore()
    for dev in partners:
        pl.semaphore_signal(barrier, inc=1, device_id=(dev,), device_id_type=MESH)
    pl.semaphore_wait(barrier, len(partners))


def remote(src, dst, sems, slot, dev):
    return pltpu.make_async_remote_copy(
        src_ref=src, dst_ref=dst, send_sem=sems.at[0, slot], recv_sem=sems.at[1, slot],
        device_id=(dev,), device_id_type=MESH)


def three_pieces(val):
    top = val.astype(BF16).astype(F32)
    rest = val - top
    mid = rest.astype(BF16).astype(F32)
    return top, mid, rest - mid


def wide_row(ref, first):
    blk = ref[pl.ds(first, STEP_ROWS), :]
    return jnp.concatenate([blk[j:j + 1, :] for j in range(STEP_ROWS)], axis=1)


def number(ref, row, lane):
    here = lax.broadcasted_iota(jnp.int32, ref.shape, 0) == row
    here = here & (lax.broadcasted_iota(jnp.int32, ref.shape, 1) == lane)
    return jnp.sum(jnp.where(here, ref[...].astype(F32), 0.0)).astype(jnp.int32)


def packed(row):
    return jnp.broadcast_to(row, (16, row.shape[1])).astype(jnp.int16)


def hot_rows(row, count):
    n = row.shape[1]
    ids = lax.broadcasted_iota(jnp.int32, (count, LANES), 0).astype(jnp.int16)
    return jnp.concatenate([ids] * (n // LANES), axis=1) == jnp.concatenate([packed(row)] * (count // 16), axis=0)


def ones_at(mask):
    return jnp.where(mask, jnp.ones((), BF16), jnp.zeros((), BF16))


def lo_hot(idx):
    return ones_at(hot_rows(idx & (LANES - 1), LANES))


def list_places(src_ref, w_ref, rows, halo, pos, num_ref):
    src, live = src_ref[...], w_ref[...] != 0.0
    n_rows = src.shape[0]
    tri = (lax.broadcasted_iota(jnp.int32, (LANES, LANES), 0) <= lax.broadcasted_iota(jnp.int32, (LANES, LANES), 1))
    tri = tri.astype(F32).astype(BF16)
    low = (lax.broadcasted_iota(jnp.int32, (n_rows, n_rows), 1) < lax.broadcasted_iota(jnp.int32, (n_rows, n_rows), 0))
    low = low.astype(F32).astype(BF16)
    place = jnp.full(src.shape, LIST_ROWS * LANES, jnp.int32)
    start = jnp.zeros((1, 1), jnp.int32)
    lane = lax.broadcasted_iota(jnp.int32, num_ref.shape, 1)
    num = jnp.zeros(num_ref.shape, jnp.int32)
    kinds = (src < rows, (src >= rows) & (src < rows + halo), src >= rows + halo)
    for k, kind in enumerate(kinds):
        kind = kind & live
        flag = kind.astype(F32)
        inner = jnp.dot(flag.astype(BF16), tri, preferred_element_type=F32)
        row_sum = jnp.broadcast_to(jnp.sum(flag, axis=1, keepdims=True), flag.shape)
        before = jnp.dot(low, row_sum.astype(BF16), preferred_element_type=F32)
        rank = (inner + before).astype(jnp.int32) - 1
        place = jnp.where(kind, start + rank, place)
        total = jnp.sum(jnp.sum(flag, axis=1, keepdims=True), axis=0, keepdims=True).astype(jnp.int32)
        blocks = lax.shift_right_logical(total + (BLOCK - 1), BLOCK.bit_length() - 1)
        start = start + blocks * BLOCK
        num = jnp.where(lane == k, blocks, num)
    pos[...] = place
    num_ref[...] = num


def k1_body(xt_hbm, w_hbm, send_hbm, own_t_ref, to_next_ref, to_prev_ref, xt_ref, w_ref, send_ref, hot, sems):
    copies = [pltpu.make_async_copy(a, b, sems.at[k])
              for k, (a, b) in enumerate(((send_hbm, send_ref), (w_hbm, w_ref), (xt_hbm, xt_ref)))]
    for copy in copies:
        copy.start()
    copies[0].wait()
    halo = send_ref.shape[1]
    rows = xt_ref.shape[1]
    blocks = halo // LANES
    ids = jnp.concatenate([send_ref[r:r + 1, b * LANES:(b + 1) * LANES] for r in range(2) for b in range(blocks)], axis=0)
    ids_col = jnp.transpose(ids)
    node = lax.broadcasted_iota(jnp.int32, (LANES, rows), 1).astype(jnp.int16)
    for b in range(2 * blocks):
        col = jnp.broadcast_to(ids_col[:, b:b + 1], (LANES, LANES)).astype(jnp.int16)
        hot[b * LANES:(b + 1) * LANES, :] = ones_at(node == jnp.concatenate([col] * (rows // LANES), axis=1))
    copies[1].wait()
    w_b = w_ref[...].astype(BF16)
    copies[2].wait()
    own_t_ref[...] = lax.dot_general(w_b, xt_ref[...], TN, preferred_element_type=F32).astype(BF16)
    for r, out in ((1, to_next_ref), (0, to_prev_ref)):
        out[...] = lax.dot_general(hot[r * halo:(r + 1) * halo, :], own_t_ref[...], NT, preferred_element_type=F32).astype(BF16)


def sort_edges(src_ref, dst_ref, ew_ref, rows, halo, pos, acc, lsrc_ref, ldst_ref, lpair_ref, lw_ref, num_ref):
    list_places(src_ref, ew_ref, rows, halo, pos, num_ref)
    acc[...] = jnp.zeros_like(acc)

    def sort(i, carry):
        first = pl.multiple_of(i * STEP_ROWS, STEP_ROWS)
        src, dst, wgt, place = (wide_row(ref, first) for ref in (src_ref, dst_ref, ew_ref, pos))
        both = src + dst * 4096
        ints = [both & 255, lax.shift_right_logical(both, 8) & 255, lax.shift_right_logical(both, 16)]
        cargo = [v.astype(F32) for v in ints] + list(three_pieces(wgt))
        here = hot_rows(lax.shift_right_logical(place, 7), LIST_ROWS)
        cargo = [jnp.concatenate([jnp.broadcast_to(v, (16, v.shape[1])).astype(BF16)] * (LIST_ROWS // 16), axis=0) for v in cargo]
        lhs = jnp.concatenate([jnp.where(here, v, jnp.zeros((), BF16)) for v in cargo], axis=0)
        acc[...] += lax.dot_general(lhs, lo_hot(place), NT, preferred_element_type=F32)
        return carry

    lax.fori_loop(0, src_ref.shape[0] // STEP_ROWS, sort, 0)
    got = [acc[p * LIST_ROWS:(p + 1) * LIST_ROWS, :] for p in range(6)]
    ints = [g.astype(jnp.int32) for g in got[:3]]
    both = ints[0] + ints[1] * 256 + ints[2] * 65536
    src, dst = both & 4095, lax.shift_right_logical(both, 12) * 2
    src = jnp.where(src < rows, src, src - rows)
    lsrc_ref[...] = src * 2
    ldst_ref[...] = dst
    lpair_ref[...] = dst + src * 65536
    lw_ref[...] = got[3] + got[4] + got[5]


def spread_weights(w_ref, wide, first, last):
    def body(g, carry):
        cols = jnp.transpose(w_ref[pl.ds(pl.multiple_of(g * 8, 8), 8), :])
        for j in range(8):
            at = pl.ds(pl.multiple_of(g * 8 * LANES + j * LANES, LANES), LANES)
            wide[at, :] = jnp.broadcast_to(cols[:, j:j + 1], (LANES, LANES))
        return carry

    lax.fori_loop(first // 8, (last + 7) // 8, body, 0)


def clear_rows(bufs):
    def body(i, carry):
        for buf in bufs:
            buf[pl.ds(pl.multiple_of(i * 64, 64), 64), :] = jnp.zeros((64, LANES), F32)
        return carry

    lax.fori_loop(0, bufs[0].shape[0] // 64, body, 0)


def chunk_copies(lists, fast, sems, c):
    at = pl.ds(pl.multiple_of(c * 8, 8), CHUNK // LANES)
    return [pltpu.make_async_copy(a.at[at, :], b.at[at, :], sems.at[k, c]) for k, (a, b) in enumerate(zip(lists, fast))]


def chunks_of(first, last):
    per = CHUNK // BLOCK
    return first // per, (last + per - 1) // per


def start_lists(lists, fast, sems, first, last):
    def body(c, carry):
        for copy in chunk_copies(lists, fast, sems, c):
            copy.start()
        return carry

    lax.fori_loop(*chunks_of(first, last), body, 0)


def row_loop(lists, fast, sems, wide, table, bufs, first, last, rename=None):
    num = len(bufs)
    take_ref, put_ref = fast
    per = CHUNK // BLOCK

    def step(i, carry):
        base = i * BLOCK
        for lead in range(0, BLOCK, num):
            take = [pl.multiple_of(take_ref[i, lead + j], 2) for j in range(num)]
            put = [put_ref[i, lead + j] for j in range(num)]
            if rename is not None:
                put = [rename[p] for p in put]
            put = [pl.multiple_of(p, 2) for p in put]
            vals = [wide[pl.ds(base + lead + j, 1), :] * table[pl.ds(take[j], 2), :] for j in range(num)]
            old = [bufs[j][pl.ds(put[j], 2), :] for j in range(num)]
            for j in range(num):
                bufs[j][pl.ds(put[j], 2), :] = old[j] + vals[j]
        return carry

    def chunk(c, carry):
        for copy in chunk_copies(lists, fast, sems, c):
            copy.wait()
        return lax.fori_loop(jnp.maximum(first, c * per), jnp.minimum(last, c * per + per), step, carry)

    lax.fori_loop(*chunks_of(first, last), chunk, 0)


def slot_copies(lists, slots, sems, c):
    at = pl.ds(pl.multiple_of(c * 8, 8), 8)
    return lambda slot: [pltpu.make_async_copy(a.at[at, :], b, sems.at[slot, k]) for k, (a, b) in enumerate(zip(lists, slots[slot]))]


def start_slots(lists, slots, sems):
    for slot in range(2):
        for copy in slot_copies(lists, slots, sems, slot)(slot):
            copy.start()


def slot_loop(lists, slots, sems, wide, table, bufs, last):
    num = len(bufs)
    pairs = jnp.maximum((last + 15) // 16, 1)

    def group(k, carry):
        for slot in range(2):
            take_ref, put_ref = slots[slot]
            for copy in slot_copies(lists, slots, sems, 2 * k + slot)(slot):
                copy.wait()
            for r in range(8):
                row = 16 * k + 8 * slot + r

                @pl.when(row < last)
                def _():
                    base = pl.multiple_of(row * LANES, LANES)
                    for lead in range(0, LANES, num):
                        here = range(min(num, LANES - lead))
                        take = [pl.multiple_of(take_ref[r, lead + j], 2) for j in here]
                        put = [pl.multiple_of(put_ref[r, lead + j], 2) for j in here]
                        vals = [wide[pl.ds(base + lead + j, 1), :] * table[pl.ds(take[j], 2), :] for j in here]
                        old = [bufs[j][pl.ds(put[j], 2), :] for j in here]
                        for j in here:
                            bufs[j][pl.ds(put[j], 2), :] = old[j] + vals[j]

            @pl.when(k + 1 < pairs)
            def _():
                for copy in slot_copies(lists, slots, sems, 2 * k + 2 + slot)(slot):
                    copy.start()
        return carry

    lax.fori_loop(0, pairs, group, 0)


def list_rows(first, last):
    return first * BLOCK // LANES, (last * BLOCK + LANES - 1) // LANES


def to_rows(blk, table, first_row):
    for h in range(2):
        table[pl.ds(2 * first_row + h, blk.shape[0], stride=2), :] = blk[:, h * LANES:(h + 1) * LANES]


def sum_rows(bufs, blk):
    halves = []
    for h in range(2):
        parts = [buf[pl.ds(2 * blk * LANES + h, LANES, stride=2), :] for buf in bufs]
        while len(parts) > 1:
            parts = [a + b for a, b in zip(parts[::2], parts[1::2])] + parts[len(parts) // 2 * 2:]
        halves.append(parts[0])
    return jnp.concatenate(halves, axis=1)


def k2a_body(own_t_ref, src_ref, dst_ref, ew_ref, part_ref, lsrc_ref, ldst_ref, lpair_ref, lw_ref, num_ref,
             pos, acc, table, wide, src_a, dst_a, src_b, dst_b, slot_sems, *bufs):
    rows = part_ref.shape[0]
    sort_edges(src_ref, dst_ref, ew_ref, rows, rows // 2, pos, acc, lsrc_ref, ldst_ref, lpair_ref, lw_ref, num_ref)

    def widen(i, carry):
        at = pl.ds(pl.multiple_of(i * LANES, LANES), LANES)
        to_rows(jnp.transpose(own_t_ref[:, at].astype(F32)), table, i * LANES)
        return carry

    lax.fori_loop(0, rows // LANES, widen, 0)
    lists, slots = (lsrc_ref, ldst_ref), ((src_a, dst_a), (src_b, dst_b))
    start_slots(lists, slots, slot_sems)
    clear_rows(bufs)
    end = number(num_ref, 0, 0)
    spread_weights(lw_ref, wide, *list_rows(0, end))
    slot_loop(lists, slots, slot_sems, wide, table, bufs, end)

    def finish(i, carry):
        part_ref[pl.ds(pl.multiple_of(i * LANES, LANES), LANES), :] = sum_rows(bufs, i)
        return carry

    lax.fori_loop(0, rows // LANES, finish, 0)


def k2b_body(part_ref, prev_ref, next_ref, lsrc_ref, ldst_ref, num_ref, lw_ref, w2_ref,
             hid_ref, pos_a_ref, pos_b_ref, tab_ref, table, wide, src_fast, dst_fast, sems, *bufs):
    first = number(num_ref, 0, 0)
    end = first + number(num_ref, 0, 1) + number(num_ref, 0, 2)
    lists, fast = (lsrc_ref, ldst_ref), (src_fast, dst_fast)
    start_lists(lists, fast, sems, first, end)
    spread_weights(lw_ref, wide, *list_rows(first, end))
    halo = prev_ref.shape[0]

    def widen(i, carry):
        at = pl.ds(pl.multiple_of(i * LANES, LANES), LANES)
        to_rows(prev_ref[at, :].astype(F32), table, i * LANES)
        to_rows(next_ref[at, :].astype(F32), table, halo + i * LANES)
        return carry

    lax.fori_loop(0, halo // LANES, widen, 0)
    clear_rows(bufs)
    row_loop(lists, fast, sems, wide, table, bufs, first, end)
    w2t = class_weights(w2_ref)

    for pos_ref, lead in ((pos_a_ref, 0), (pos_b_ref, pos_a_ref.shape[0] // LANES)):
        def finish(j, carry):
            i = lead + j
            at = pl.ds(pl.multiple_of(i * LANES, LANES), LANES)
            pre = part_ref[at, :] + sum_rows(bufs, i)
            hid = jnp.maximum(pre, 0.0).astype(BF16)
            hid_ref[at, :] = hid
            pos_ref[pl.ds(pl.multiple_of(j * LANES, LANES), LANES), :] = (pre > 0.0).astype(F32).astype(BF16)
            t2 = lax.dot_general(w2t, hid, NT, preferred_element_type=F32)
            tab_ref[pl.ds(pl.multiple_of(i * CLASS_ROWS, CLASS_ROWS), CLASS_ROWS), :] = t2.astype(BF16).astype(F32)
            return carry

        lax.fori_loop(0, pos_ref.shape[0] // LANES, finish, 0)


def stack_classes(w2_ref, blocks):
    w2_all = jnp.concatenate([class_weights(w2_ref).astype(F32)] * blocks, axis=0)
    return w2_all, lax.shift_right_logical(lax.broadcasted_iota(jnp.int32, w2_all.shape, 0), 3)


def fill_table(dt, pos_refs, w2_all, group, table):
    dt_cols = jnp.transpose(dt).astype(BF16)
    for pos_ref, lead in zip(pos_refs, (0, pos_refs[0].shape[0] // LANES)):
        def widen(j, carry):
            i = lead + j
            d_hid = jnp.dot(dt_cols, jnp.where(group == i, w2_all, 0.0).astype(BF16), preferred_element_type=F32)
            at = pl.ds(pl.multiple_of(j * LANES, LANES), LANES)
            to_rows(jnp.where(pos_ref[at, :].astype(F32) > 0.0, d_hid, 0.0), table, i * LANES)
            return carry

        lax.fori_loop(0, pos_ref.shape[0] // LANES, widen, 0)


def k4a_body(ldst_ref, lsrc_ref, num_ref, lw_ref, pos_a_ref, pos_b_ref, dt_ref, w2_ref, part_ref,
             table, wide, take_a, put_a, take_b, put_b, slot_sems, *bufs):
    rows = part_ref.shape[0]
    lists, slots, end = (ldst_ref, lsrc_ref), ((take_a, put_a), (take_b, put_b)), number(num_ref, 0, 0)
    start_slots(lists, slots, slot_sems)
    w2_all, group = stack_classes(w2_ref, rows // LANES)
    clear_rows(bufs)
    fill_table(dt_ref[...].astype(F32), (pos_a_ref, pos_b_ref), w2_all, group, table)
    spread_weights(lw_ref, wide, *list_rows(0, end))
    slot_loop(lists, slots, slot_sems, wide, table, bufs, end)

    def finish(i, carry):
        part_ref[pl.ds(pl.multiple_of(i * LANES, LANES), LANES), :] = sum_rows(bufs, i)
        return carry

    lax.fori_loop(0, rows // LANES, finish, 0)


def k4b_body(part_ref, num_ref, names_ref, prev_dst, prev_src, prev_w, next_dst, next_src, next_w,
             prev_a, prev_late, next_a, next_late, w2_ref, xt_ref, misc_ref, out_ref,
             table, wide, d_tab, names, names_sem, *rest):
    fasts, pools, bufs = (rest[0:2], rest[2:4]), rest[4:6], rest[6:]
    rows = part_ref.shape[0]
    late_rows = rows - prev_a.shape[0]
    load = pltpu.make_async_copy(names_ref, names, names_sem)
    load.start()
    sides = (((prev_dst, prev_src), prev_w, prev_late, prev_a, 1, 2),
             ((next_dst, next_src), next_w, next_late, next_a, 2, 1))
    spans = []
    for (lists, _, _, _, row, kind), fast, pool in zip(sides, fasts, pools):
        first = number(num_ref, row, 0)
        if kind == 2:
            first = first + number(num_ref, row, 1)
        spans.append((first, first + number(num_ref, row, kind)))
        start_lists(lists, fast, pool, *spans[-1])
    w2_all, group = stack_classes(w2_ref, rows // LANES)
    clear_rows(bufs)
    for (lists, w_ref, late, early, _, _), fast, pool, span in zip(sides, fasts, pools, spans):
        dt = late[late_rows:, :].astype(F32)
        dt = jnp.concatenate([dt[:, 0:LANES], dt[:, LANES:]], axis=0)
        fill_table(dt, (early, late.at[0:late_rows, :]), w2_all, group, table)
        spread_weights(w_ref, wide, *list_rows(*span))
        if late is prev_late:
            load.wait()
        row_loop(lists, fast, pool, wide, table, bufs, *span, rename=names)

    def finish(i, carry):
        at = pl.ds(pl.multiple_of(i * LANES, LANES), LANES)
        d_tab[at, :] = (part_ref[at, :] + sum_rows(bufs, i)).astype(BF16)
        return carry

    lax.fori_loop(0, rows // LANES, finish, 0)
    feats = xt_ref.shape[0]
    out_ref[0:feats, :] = jnp.dot(xt_ref[...], d_tab[...], preferred_element_type=F32)
    out_ref[feats:feats + 12, :] = misc_ref[0:12, :]


def hi_of(idx):
    return jnp.broadcast_to(lax.shift_right_logical(idx, 7), (CLASS_ROWS, idx.shape[1]))


def pick_cols(table_b, idx, hot, first=0):
    pieces = table_b.shape[1] // LANES
    cols = jnp.dot(table_b, jnp.concatenate([hot] * pieces, axis=0), preferred_element_type=F32)
    hi = hi_of(idx) - first
    out = jnp.zeros(hi.shape, F32)
    for h in range(table_b.shape[0] // CLASS_ROWS):
        out = out + jnp.where(hi == h, cols[h * CLASS_ROWS:(h + 1) * CLASS_ROWS], 0.0)
    return out


def add_cols(val, idx, hot, num_hi, first=0):
    hi = packed(lax.shift_right_logical(idx, 7) - first)
    low_half = lax.broadcasted_iota(jnp.int32, hi.shape, 0) >= CLASS_ROWS
    mixed = hi - low_half.astype(jnp.int32).astype(jnp.int16)
    top, mid, low = three_pieces(val)
    pieces = [jnp.concatenate(two, axis=0).astype(BF16) for two in ((top, mid), (low, top), (mid, low))]
    rows = []
    for h in range(0, num_hi, 2):
        masks = (hi == jnp.int16(h), mixed == jnp.int16(h), hi == jnp.int16(h + 1))
        rows += [jnp.where(m, p, jnp.zeros((), BF16)) for m, p in zip(masks, pieces)]
    return lax.dot_general(jnp.concatenate(rows, axis=0), hot, NT, preferred_element_type=F32)


def join_pieces(acc, num_hi):
    out = []
    for h in range(num_hi):
        a = acc[h * 24:h * 24 + 24, :]
        out.append(a[0:8] + a[8:16] + a[16:24])
    return out


def stack_pieces(val):
    return jnp.concatenate(three_pieces(val), axis=1).astype(BF16)


def k3_body(num_dev, tab_ref, send_ref, src_ref, dst_ref, w_ref, lab_ref, mask_ref, hid_ref, pos_ref, pos_late_ref,
            lpair_ref, lw_ref, num_ref,
            dt_ref, misc_ref, late_ref, pos_prev_ref, pos_next_ref, dst_prev_ref, dst_next_ref,
            put_prev_ref, put_next_ref, w_prev_ref, w_next_ref, nums_ref, names_ref, pairs, nums,
            ext_b, fwd_send, fwd_recv, bwd_send, bwd_recv, vals, acc_z, acc_s, acc_o, acc_r, dz_b, cnt_send, cnt_recv,
            sems, cnt_sems, list_sems, pos_sems):
    me, nxt, prv = ring_peers(num_dev)
    layers = layer_peers(me, num_dev)
    layer = [me - me % PLANE + (me % PLANE + k) % PLANE for k in range(1, PLANE)]
    meet([nxt, prv] + layer + layers)
    total = jnp.sum(jnp.sum(mask_ref[...].astype(F32), axis=1, keepdims=True), axis=0, keepdims=True)
    cnt_send[0] = jnp.broadcast_to(total, cnt_send.shape[1:])
    counts = [remote(cnt_send.at[0], cnt_recv.at[k], cnt_sems, k, dev) for k, dev in enumerate(layer)]
    for copy in counts:
        copy.start()
    late = []

    def send_late(pairs, pool, first):
        for k, (src, dst) in enumerate(pairs):
            for s, dev in enumerate((nxt, prv)):
                copy = remote(src, dst[s], pool, 2 * (first + k) + s, dev)
                copy.start()
                late.append(copy)

    chunk = pos_ref.shape[0] // 3

    def send_pos(q):
        at = pl.ds(q * chunk, chunk)
        send_late([(pos_ref.at[at, :], [pos_prev_ref.at[at, :], pos_next_ref.at[at, :]])], pos_sems, q)

    own_hi = tab_ref.shape[0] // CLASS_ROWS
    halo = send_ref.shape[1]
    halo_hi = halo // LANES
    all_hi = own_hi + 2 * halo_hi
    own_b = tab_ref[...].astype(BF16)
    ext_b[pl.ds(0, own_hi * CLASS_ROWS), :] = own_b
    hot_send = [lo_hot(send_ref[r:r + 1, :]) for r in range(2)]
    copies = []
    for r in (1, 0):
        val = pick_cols(own_b, send_ref[r:r + 1, :], hot_send[r])
        fwd_send[r] = jnp.concatenate([val, jnp.zeros_like(val)], axis=0).astype(BF16)
        copy = remote(fwd_send.at[r], fwd_recv.at[1 - r], sems, r, nxt if r == 1 else prv)
        copy.start()
        copies.append(copy)
    send_late([(lpair_ref, [pairs.at[0], pairs.at[1]]), (lw_ref, [w_prev_ref, w_next_ref]),
               (num_ref, [nums.at[0], nums.at[1]])], list_sems, 0)
    send_pos(0)
    for copy in counts:
        copy.wait()
    for k in range(len(layer)):
        total = total + cnt_recv[k][0:1, 0:1]
    cnt_send[1] = jnp.broadcast_to(total, cnt_send.shape[1:])
    counts = [remote(cnt_send.at[1], cnt_recv.at[len(layer) + k], cnt_sems, len(layer) + k, dev)
              for k, dev in enumerate(layers)]
    for copy in counts:
        copy.start()
    send_pos(1)
    send_pos(2)
    acc_z[...] = jnp.zeros_like(acc_z)
    acc_s[...] = jnp.zeros_like(acc_s)
    acc_o[...] = jnp.zeros_like(acc_o)
    late_rows = pos_late_ref.shape[0]
    late_ref[0:late_rows, :] = pos_late_ref[...]
    steps = src_ref.shape[0] // STEP_ROWS

    def own_forward(i, carry):
        src = wide_row(src_ref, pl.multiple_of(i * STEP_ROWS, STEP_ROWS))
        vals[i] = pick_cols(ext_b[0:own_hi * CLASS_ROWS, :], src, lo_hot(src))
        return carry

    lax.fori_loop(0, steps, own_forward, 0)
    for copy in copies:
        copy.wait()
    for r in range(2):
        got = fwd_recv[r].astype(F32)
        for j in range(0, halo_hi, 2):
            two = jnp.concatenate([got[0:8, (j + k) * LANES:(j + k + 1) * LANES] for k in range(2)], axis=0)
            ext_b[pl.ds((own_hi + r * halo_hi + j) * CLASS_ROWS, 16), :] = two.astype(BF16)


    def forward(i, carry):
        first = pl.multiple_of(i * STEP_ROWS, STEP_ROWS)
        src, dst = wide_row(src_ref, first), wide_row(dst_ref, first)
        val = vals[i] + pick_cols(ext_b[own_hi * CLASS_ROWS:, :], src, lo_hot(src), own_hi)
        val = val * wide_row(w_ref, first)
        acc_z[...] += add_cols(val, dst, lo_hot(dst), own_hi)
        return carry

    lax.fori_loop(0, steps, forward, 0)

    logits = join_pieces(acc_z[...], own_hi)
    cls = lax.broadcasted_iota(jnp.int32, (CLASS_ROWS, LANES), 0)
    count = jnp.broadcast_to(total, (1, LANES))
    for k, copy in enumerate(counts):
        copy.wait()
        count = count + cnt_recv[len(layer) + k][0:1, :]
    count = jnp.maximum(count, 1.0)
    loss = jnp.zeros((1, LANES), F32)
    d_log = []
    for h in range(own_hi):
        z = jnp.where(cls < 7, logits[h], -jnp.inf)
        top = jnp.max(z, axis=0, keepdims=True)
        norm = jnp.log(jnp.sum(jnp.exp(z - top), axis=0, keepdims=True)) + top
        hot = cls == lab_ref[h:h + 1, :]
        mask = mask_ref[h:h + 1, :].astype(F32)
        picked = jnp.sum(jnp.where(hot, logits[h], 0.0), axis=0, keepdims=True)
        loss = loss + mask * (norm - picked)
        d_log.append((jnp.exp(z - norm) - hot.astype(F32)) * (mask / count))
    dz_b[...] = stack_pieces(jnp.concatenate(d_log, axis=0))

    def backward(i, carry):
        first = pl.multiple_of(i * STEP_ROWS, STEP_ROWS)
        src, dst = wide_row(src_ref, first), wide_row(dst_ref, first)
        val = pick_cols(dz_b[...], dst, lo_hot(dst)) * wide_row(w_ref, first)
        vals[i] = val
        acc_s[...] += add_cols(val, src, lo_hot(src), 2 * halo_hi, own_hi)
        return carry

    lax.fori_loop(0, steps, backward, 0)

    d_halo = join_pieces(acc_s[...], 2 * halo_hi)
    copies = []
    for r in range(2):
        for j in range(halo_hi):
            bwd_send[r, :, j * LANES:(j + 1) * LANES] = d_halo[r * halo_hi + j]
        copy = remote(bwd_send.at[r], bwd_recv.at[1 - r], sems, 2 + r, prv if r == 0 else nxt)
        copy.start()
        copies.append(copy)

    def own_backward(i, carry):
        src = wide_row(src_ref, pl.multiple_of(i * STEP_ROWS, STEP_ROWS))
        acc_o[...] += add_cols(vals[i], src, lo_hot(src), own_hi)
        return carry

    lax.fori_loop(0, steps, own_backward, 0)
    d_own = join_pieces(acc_o[...], own_hi)
    for copy in copies:
        copy.wait()
    for r in range(2):
        part = add_cols(bwd_recv[r], send_ref[r:r + 1, :], hot_send[r], own_hi)
        acc_r[...] = part if r == 0 else acc_r[...] + part
    back = join_pieces(acc_r[...], own_hi)
    d_tab = [d_own[h] + back[h] for h in range(own_hi)]
    half = own_hi // 2
    dt_ref[...] = jnp.concatenate(d_tab, axis=0).astype(BF16)
    late_ref[late_rows:, :] = jnp.concatenate(
        [jnp.concatenate(d_tab[:half], axis=0), jnp.concatenate(d_tab[half:], axis=0)], axis=1).astype(BF16)
    grad = jnp.zeros((CLASS_ROWS, hid_ref.shape[1]), F32)
    for h in range(own_hi):
        grad = grad + jnp.dot(d_tab[h].astype(BF16), hid_ref[pl.ds(h * LANES, LANES), :], preferred_element_type=F32)
    misc_ref[0:8, :] = grad
    total = jnp.sum(loss, axis=1, keepdims=True) / count[:, 0:1]
    misc_ref[8:16, :] = jnp.broadcast_to(total, (8, misc_ref.shape[1]))
    for copy in late:
        copy.wait()
    for s, (to_dst, to_put) in enumerate(((dst_prev_ref, put_prev_ref), (dst_next_ref, put_next_ref))):
        to_dst[...] = pairs[s] & 0xFFFF
        to_put[...] = lax.shift_right_logical(pairs[s], 16)
    row = lax.broadcasted_iota(jnp.int32, nums_ref.shape, 0)
    nums_ref[...] = jnp.where(row == 0, num_ref[0:1, :], jnp.where(row == 1, nums[0, 0:1, :], nums[1, 0:1, :]))
    names_ref[...] = 2 * jnp.concatenate(
        [send_ref[r:r + 1, j * LANES:(j + 1) * LANES] for r in (1, 0) for j in range(halo_hi)], axis=0)


def k5_body(num_dev, part_ref, full_ref, land_core, land_chip, land_z, by_core, by_chip, sems):
    me = lax.axis_index(GRAPH_AXIS)
    core, chip, z = me % 2, (me // 2) % 4, me // PLANE
    other = me + 1 - 2 * core
    chips = [me + 2 * ((chip + k) % 4 - chip) for k in range(1, 4)]
    layers = layer_peers(me, num_dev)
    num_z = num_dev // PLANE
    meet([other] + chips + layers)
    rows, width = part_ref.shape
    rows //= 2
    n1, n2, n3 = rows // 2, rows // 8, rows // 8 // num_z
    parts = [(p, pl.ds(c * LANES, LANES)) for p in range(2) for c in range(width // LANES)]
    used = [0]

    def send(pairs):
        out = []
        for src, dst, dev in pairs:
            out.append(remote(src, dst, sems, used[0], dev))
            used[0] += 1
        for copy in out:
            copy.start()
        return out

    def wait(copies):
        for copy in copies:
            copy.wait()

    def at(first, size):
        return pl.ds(pl.multiple_of(first, size), size)

    def run(p, size):
        return pl.ds(p * size, size)

    flying = [send([(part_ref.at[at(p * rows + (1 - core) * n1, n1), c], land_core.at[run(p, n1), c], other)]) for p, c in parts]
    for i, (p, c) in enumerate(parts):
        wait(flying[i])
        by_core[run(p, n1), c] = part_ref[at(p * rows + core * n1, n1), c] + land_core[run(p, n1), c]
        flying[i] = send([(by_core.at[at(p * n1 + (chip + k + 1) % 4 * n2, n2), c], land_chip.at[k, run(p, n2), c], dev)
                          for k, dev in enumerate(chips)])
    for i, (p, c) in enumerate(parts):
        wait(flying[i])
        total = by_core[at(p * n1 + chip * n2, n2), c]
        for k in range(len(chips)):
            total = total + land_chip[k, run(p, n2), c]
        by_chip[run(p, n2), c] = total
        flying[i] = send([(by_chip.at[at(p * n2 + (z + k + 1) % num_z * n3, n3), c], land_z.at[k, run(p, n3), c], dev)
                          for k, dev in enumerate(layers)])
    firsts = (core * n1 + chip * n2 + z * n3, core * n1 + chip * n2, core * n1)
    gathers = list(zip(firsts, (n3, n2, n1), (layers, chips, [other])))

    def gather(level, p, c):
        first, size, devs = gathers[level]
        own = full_ref.at[at(p * rows + first, size), c]
        return send([(own, own, dev) for dev in devs])

    for i, (p, c) in enumerate(parts):
        wait(flying[i])
        total = by_chip[at(p * n2 + z * n3, n3), c]
        for k in range(len(layers)):
            total = total + land_z[k, run(p, n3), c]
        full_ref[at(p * rows + firsts[0], n3), c] = total
        flying[i] = gather(0, p, c)
    for level in (1, 2):
        for i, (p, c) in enumerate(parts):
            wait(flying[i])
            flying[i] = gather(level, p, c)
    for copies in flying:
        wait(copies)


def k6_body(full_ref, loss_ref, one_ref, two_ref):
    feats, classes = one_ref.shape[0], two_ref.shape[0]
    one_ref[...] = full_ref[0:feats, :]
    two_ref[...] = full_ref[feats:feats + classes, :]
    loss_ref[...] = full_ref[feats + 8:feats + 9, 0:1]


def solution(mesh):
    num_dev = mesh.shape[GRAPH_AXIS]

    def params(cid=None):
        if cid is None:
            return pltpu.CompilerParams(vmem_limit_bytes=VMEM_BYTES)
        return pltpu.CompilerParams(vmem_limit_bytes=VMEM_BYTES, collective_id=cid, has_side_effects=True)

    def arr(dtype, *shape):
        return jax.ShapeDtypeStruct(shape, dtype)

    def scr(dtype, *shape):
        return pltpu.VMEM(shape, dtype)

    def dma(count):
        return pltpu.SemaphoreType.DMA((2, count))

    I32 = jnp.int32

    def device_step(node_feats, w_one, w_two, send_rows, edge_src, edge_dst, edge_w, labels, label_mask):
        rows, feats = node_feats.shape
        width = w_one.shape[1]
        halo = send_rows.shape[1]
        edges = edge_src.shape[0]
        own_hi, all_hi = rows // LANES, (rows + 2 * halo) // LANES
        feats_t, w2 = node_feats.T, w_two.T
        src2, dst2, ew2 = (a.reshape(edges // LANES, LANES) for a in (edge_src, edge_dst, edge_w))
        lab2, mask2 = labels.reshape(own_hi, LANES), label_mask.reshape(own_hi, LANES)
        listed = (LIST_ROWS, LANES)
        entries = LIST_ROWS * LANES
        fast_list = pltpu.SMEM(listed, I32)
        list_dma = dma(entries // CHUNK)

        late_rows = rows - EARLY_ROWS
        busy = pl.CostEstimate(flops=8 * 10**9, bytes_accessed=10**7, transcendentals=0)
        own_t, to_next, to_prev = pl.pallas_call(
            k1_body,
            out_shape=(arr(BF16, width, rows), arr(BF16, halo, width), arr(BF16, halo, width)),
            in_specs=[pl.BlockSpec(memory_space=pltpu.HBM)] * 3, out_specs=(vmem(),) * 3,
            scratch_shapes=[scr(BF16, feats, rows), scr(F32, feats, width), pltpu.VMEM((2, halo), I32),
                            scr(BF16, 2 * halo, rows), pltpu.SemaphoreType.DMA((3,))],
            compiler_params=pltpu.CompilerParams(vmem_limit_bytes=K1_VMEM), name="transform",
        )(feats_t, w_one, send_rows)
        from_prev = lax.ppermute(to_next, GRAPH_AXIS, [(g, (g + 1) % num_dev) for g in range(num_dev)])
        from_next = lax.ppermute(to_prev, GRAPH_AXIS, [(g, (g - 1) % num_dev) for g in range(num_dev)])

        bufs, own_bufs = ([scr(F32, 2 * rows, LANES)] * n for n in (NUM_BUFS, OWN_BUFS))
        fast_row = pltpu.SMEM((8, LANES), I32)
        lists_in = (arr(I32, *listed), arr(I32, *listed), arr(I32, *listed), arr(F32, *listed), arr(I32, 8, LANES))
        part_own, lsrc, ldst, lpair, lw, num = pl.pallas_call(
            k2a_body,
            out_shape=(arr(F32, rows, width),) + lists_in,
            in_specs=[vmem()] * 4, out_specs=(vmem(),) * 6,
            scratch_shapes=[scr(I32, edges // LANES, LANES), scr(F32, 6 * LIST_ROWS, LANES), scr(F32, 2 * rows, LANES),
                            scr(F32, entries, LANES), fast_row, fast_row, fast_row, fast_row,
                            dma(2)] + own_bufs,
            compiler_params=pltpu.CompilerParams(vmem_limit_bytes=OWN_VMEM), cost_estimate=busy, name="aggregate_own",
        )(own_t, src2, dst2, ew2)

        hid, pos_a, pos_b, tab = pl.pallas_call(
            k2b_body,
            out_shape=(arr(BF16, rows, width), arr(BF16, EARLY_ROWS, width), arr(BF16, late_rows, width),
                       arr(F32, own_hi * CLASS_ROWS, LANES)),
            in_specs=[vmem(), vmem(), vmem(), hbm(), hbm(), vmem(), vmem(), vmem()], out_specs=(vmem(),) * 4,
            scratch_shapes=[scr(F32, 4 * halo, LANES), scr(F32, entries, LANES), fast_list, fast_list, list_dma] + bufs,
            compiler_params=params(), name="aggregate_halo",
        )(part_own, from_prev, from_next, lsrc, ldst, num, lw, w2)

        num_z = num_dev // PLANE
        tab_b = arr(BF16, own_hi * CLASS_ROWS, LANES)
        pos_early = arr(BF16, EARLY_ROWS, width)
        list_i = arr(I32, *listed)
        (d_tab, misc, late, prev_a, next_a, dst_prev, dst_next, put_prev, put_next, w_prev, w_next,
         nums, names) = pl.pallas_call(
            functools.partial(k3_body, num_dev),
            out_shape=(tab_b, arr(F32, 16, width), arr(BF16, late_rows + own_hi * CLASS_ROWS * LANES // width, width), pos_early, pos_early, list_i, list_i, list_i, list_i,
                       arr(F32, *listed), arr(F32, *listed), arr(I32, 8, LANES), arr(I32, 2 * halo // LANES, LANES)),
            in_specs=[vmem()] * 13, out_specs=(vmem(),) * 13,
            scratch_shapes=[scr(I32, 2, *listed), scr(I32, 2, 8, LANES), scr(BF16, all_hi * CLASS_ROWS, LANES),
                            scr(BF16, 2, 16, halo), scr(BF16, 2, 16, halo), scr(F32, 2, CLASS_ROWS, halo),
                            scr(F32, 2, CLASS_ROWS, halo), scr(F32, edges // (STEP_ROWS * LANES), CLASS_ROWS, STEP_ROWS * LANES),
                            scr(F32, own_hi * 24, LANES), scr(F32, 2 * halo // LANES * 24, LANES),
                            scr(F32, own_hi * 24, LANES), scr(F32, own_hi * 24, LANES), scr(BF16, own_hi * CLASS_ROWS, 3 * LANES),
                            scr(F32, 2, 8, LANES), scr(F32, PLANE + num_z - 2, 8, LANES),
                            dma(4), dma(PLANE + num_z - 2), dma(6), dma(6)],
            compiler_params=params(1), name="layer_two",
        )(tab, send_rows, src2, dst2, ew2, lab2, mask2, hid, pos_a, pos_b, lpair, lw, num)

        prev_late = lax.ppermute(late, GRAPH_AXIS, [(g, (g + 1) % num_dev) for g in range(num_dev)])
        next_late = lax.ppermute(late, GRAPH_AXIS, [(g, (g - 1) % num_dev) for g in range(num_dev)])
        part_own = pl.pallas_call(
            k4a_body,
            out_shape=arr(F32, rows, width),
            in_specs=[hbm(), hbm()] + [vmem()] * 6, out_specs=vmem(),
            scratch_shapes=[scr(F32, 2 * rows, LANES), scr(F32, entries, LANES), fast_row, fast_row, fast_row, fast_row,
                            dma(2)] + own_bufs,
            compiler_params=pltpu.CompilerParams(vmem_limit_bytes=OWN_VMEM), cost_estimate=busy, name="scatter_own",
        )(ldst, lsrc, num, lw, pos_a, pos_b, d_tab, w2)

        sum_rows_pad = 512
        part = pl.pallas_call(
            k4b_body,
            out_shape=arr(F32, sum_rows_pad, width),
            in_specs=[vmem(), vmem(), vmem()] + [hbm(), hbm(), vmem()] * 2 + [vmem()] * 7, out_specs=vmem(),
            scratch_shapes=[scr(F32, 2 * rows, LANES), scr(F32, entries, LANES), scr(BF16, rows, width),
                            pltpu.SMEM((2 * halo,), I32), pltpu.SemaphoreType.DMA]
            + [fast_list] * 4 + [list_dma] * 2 + bufs,
            compiler_params=params(), name="scatter_peers",
        )(part_own, nums, names.reshape(2 * halo), dst_prev, put_prev, w_prev,
          dst_next, put_next, w_next,
          prev_a, prev_late, next_a, next_late, w2, feats_t, misc)

        n1, n2 = sum_rows_pad // 2, sum_rows_pad // 8
        n3 = n2 // num_z
        full = pl.pallas_call(
            functools.partial(k5_body, num_dev),
            out_shape=arr(F32, sum_rows_pad, width),
            in_specs=[vmem()], out_specs=vmem(),
            scratch_shapes=[scr(F32, n1, width), scr(F32, 3, n2, width), scr(F32, num_z - 1, n3, width),
                            scr(F32, n1, width), scr(F32, n2, width), dma(8 * (1 + 3 + num_z - 1))],
            compiler_params=params(2), name="sum_gradients",
        )(part)
        loss, grad_one, grad_two = pl.pallas_call(
            k6_body,
            out_shape=(arr(F32, 1, 1), arr(F32, feats, width), arr(F32, w2.shape[0], width)),
            in_specs=[vmem()], out_specs=(vmem(),) * 3, compiler_params=params(), name="outputs",
        )(full)
        return loss.reshape(()), grad_one, grad_two.T

    row_spec = P(GRAPH_AXIS)
    return jax.shard_map(device_step, mesh=mesh,
                         in_specs=(row_spec, P(), P(), row_spec, row_spec, row_spec, row_spec, row_spec, row_spec),
                         out_specs=(P(), P(), P()), check_vma=False)
```
